32 devices in a mesh: prompt: 4 (over y, x), resp: 8 (over z, core).
Axes of the slice: x: 2, y: 2, z: 4, core: 2. Of those that a mesh axis runs over, the one named last changes fastest.
Arguments:
- embeddings: bfloat16 [32, 256, 3584], P('prompt', 'resp'), parts along dimension 0, may hold values from -6 to 6
- head_weight: bfloat16 [3584, 3584], P('resp'), may hold values from -0.0017089844 to 0.0017089844
- valid_mask: int32 [32, 256], P('prompt', 'resp'), parts along dimension 0, may hold values from 0 to 1, as said below
Outputs:
- preferences: float32 [32, 256, 256], P('prompt', 'resp'), parts along dimension 0
- win_rates: float32 [32, 256], P('prompt', 'resp'), parts along dimension 0
The draws below stay inside these ranges and needn't reach their ends.
There are 4 independent parts, one for each index of `prompt`. The reference program is written for one: setup_inputs(seed, part) draws one part's arguments, and reference() takes and returns one part's arrays. A program takes and returns all parts, laid end to end along the dimension named above; an argument that names none is the same for every part. Nothing has to cross between parts.
Inputs may be any that keep to these rules, and one draw needn't show every extreme that they name: `valid_mask`: for each prompt the ones are its first response slots, between 64 and 256 of them; in every draw some prompt has all 256 slots filled.
All inputs are finite; a program needn't handle non-finite values.
Results may differ from the reference program's by a relative error of at most 0.003.
Values may be sent and summed in bfloat16 or wider, within the bound.
A program may use at most 128 MiB of HBM per device.

```python
import jax
import jax.numpy as jnp
from jax import lax

D = 3584
PROMPTS = 8
RESP = 256


def draw_valid_mask(key, part):
    first, second, third = jax.random.split(key, 3)
    lengths = jax.random.randint(first, (PROMPTS,), RESP // 4, RESP + 1)
    prompt_ids = jnp.arange(PROMPTS, dtype=jnp.int32)
    shortest = jax.random.randint(second, (), 0, PROMPTS)
    longest = jax.random.randint(third, (), 0, PROMPTS)
    lengths = jnp.where(prompt_ids == shortest, RESP // 4, lengths)
    lengths = jnp.where(prompt_ids == longest, RESP, lengths)
    slot_ids = jnp.arange(RESP, dtype=jnp.int32)
    return (slot_ids[None, :] < lengths[:, None]).astype(jnp.int32)


def block_levels(rng, shape, cuts, smallest, largest):
    loudness = 1.0
    for position, shards_of in cuts:
        steps = jax.random.uniform(jax.random.fold_in(jax.random.fold_in(rng, 6), position), (shards_of,), jnp.float32, smallest / len(cuts), largest / len(cuts))
        loudness = loudness * jnp.repeat(jnp.exp(steps), shape[position] // shards_of).reshape((-1,) + (1,) * (len(shape) - 1 - position))
    return loudness


def noise(stream_key, dims, deviation, most, pieces=(), held_as=jnp.bfloat16):
    drawn = deviation * jax.random.normal(stream_key, dims, jnp.float32)
    if pieces:
        drawn = drawn * block_levels(stream_key, dims, pieces, -0.22, 0.18)
    return jnp.clip(drawn, -most, most).astype(held_as)


def setup_inputs(seed: int = 0, part: int = 0) -> dict:
    keys = jax.random.split(jax.random.key(seed), 4)
    part_keys = jax.random.split(jax.random.fold_in(keys[3], part), 4)
    return {
        "embeddings": noise(part_keys[0], (PROMPTS, RESP, D), 1.0, 6.0, ((1, 8),)),
        "head_weight": noise(keys[1], (D, D), (D * D) ** -0.5, 0.0017089844, ((0, 8),)),
        "valid_mask": draw_valid_mask(jax.random.fold_in(jax.random.fold_in(keys[3], part), 71), part),
    }


def reference(embeddings, head_weight, valid_mask):
    flat_rows = embeddings.reshape(PROMPTS * RESP, D)
    direct = jnp.dot(flat_rows, head_weight, preferred_element_type=jnp.float32)
    mirror = lax.dot_general(flat_rows, head_weight, (((1,), (1,)), ((), ())), preferred_element_type=jnp.float32)
    projected = (direct - mirror).astype(jnp.bfloat16).reshape(PROMPTS, RESP, D)

    def one_prompt(pair):
        rows_in, proj_in = pair
        return -jnp.dot(rows_in, proj_in.T, preferred_element_type=jnp.float32)

    scores = lax.map(one_prompt, (embeddings, projected))
    valid = valid_mask.astype(jnp.float32)
    counts = jnp.sum(valid, axis=1)
    preferences = jax.nn.sigmoid(scores) * valid[:, :, None] * valid[:, None, :]
    totals = jnp.sum(preferences, axis=2) - 0.5 * valid
    win_rates = valid * totals / jnp.maximum(counts - 1.0, 1.0)[:, None]
    return preferences, win_rates
```

```python
import functools

import jax
import jax.numpy as jnp
from jax import lax
from jax.experimental import pallas as pl
from jax.experimental.pallas import tpu as pltpu
from jax.sharding import PartitionSpec as P

MESH = pl.DeviceIdType.MESH
CORES = 2
CHIPS = 4
PARTS = 4
NT = (((1,), (1,)), ((), ()))


def gathered_halves(embeddings, head_weight, own_index, group_size):
    prompts, block_rows, features = embeddings.shape
    held = head_weight.shape[0]
    slots = group_size * block_rows
    everyone = lax.all_gather(embeddings, "resp", axis=0, tiled=True)
    flat = everyone.reshape(group_size * prompts * block_rows, features)
    through = lax.dot_general(flat, head_weight, NT, preferred_element_type=jnp.float32)
    through = through.astype(jnp.bfloat16).reshape(group_size, prompts, block_rows, held)
    mine = lax.dynamic_slice_in_dim(
        everyone.reshape(group_size, prompts, block_rows, features), own_index * held, held, 3
    )
    partial = jnp.einsum("gpid,hpjd->gpihj", mine, through, preferred_element_type=jnp.float32)
    flipped = jnp.einsum("gpid,hpjd->gpihj", through, mine, preferred_element_type=jnp.float32)
    partial = (partial - flipped).astype(jnp.bfloat16)
    return partial.reshape(group_size, prompts, block_rows, slots)


def gathered_scores(embeddings, head_weight):
    group_size = lax.axis_size("resp")
    own_index = lax.axis_index("resp")
    prompts, block_rows, features = embeddings.shape
    slots = group_size * block_rows
    at_once = max(1, min(prompts, (1 << 11) // slots))

    def scores_of(some):
        partial = gathered_halves(some, head_weight, own_index, group_size)
        swapped = lax.all_to_all(partial, "resp", split_axis=0, concat_axis=0, tiled=True)
        return jnp.sum(swapped.astype(jnp.float32), axis=0)

    pieces = embeddings.reshape(prompts // at_once, at_once, block_rows, features)
    return lax.map(scores_of, pieces).reshape(prompts, block_rows, slots)


def kernel(e_ref, w_ref, m_ref, o_ref, r_ref,
           ebuf, wbuf, zt, sbuf, keep, pbuf, qbuf, fbuf, rbuf, mine, mbuf,
           m_send, m_recv, e_send, e_recv, n_send, h_send, el_sem,
           o_send, d_send, f_send, nw_send, wl_sem, x_send, y_send, u_send, v_send, w_recv,
           p_send, p_recv, r_send, r_recv):
    part = lax.axis_index("prompt")
    me = lax.axis_index("resp")
    z = me // CORES
    core = me % CORES
    half = z // 2
    prompts, block_rows, features = e_ref.shape
    held = w_ref.shape[0]
    group = CHIPS * CORES
    per_half = prompts // 2
    side = group // 2
    span = held * side
    rows = group * block_rows
    half_rows = rows // 2
    quarter = held // PARTS
    z_in = 1 + half
    z_out = 3 * half
    z_far = 2 - half
    z_end = 3 - z_out
    inner = z == z_in
    near = core == half
    other = 1 - core
    first = 2 * half
    second = 2 - first
    here = me % side
    x_part = part + 1 - 2 * (part % 2)
    y_part = lax.rem(part + 2, PARTS)
    d_part = PARTS - 1 - part
    step = quarter // 7
    pieces = ((0, step), (step, 2 * step), (3 * step, 2 * step), (5 * step, 2 * step))

    def copy(src, dst, send, recv, chip, c, q=None):
        return pltpu.make_async_remote_copy(
            src, dst, send, recv,
            device_id=(part if q is None else q, chip * CORES + c), device_id_type=MESH,
        )

    def arrived(dst, recv):
        copy(dst, dst, m_send.at[0], recv, z_far, core).wait_recv()

    valid = m_ref[...].astype(jnp.float32)
    mine[...] = jnp.broadcast_to(jnp.sum(m_ref[...], axis=1, keepdims=True), mine.shape)

    others = [lax.rem(me + d, group) for d in range(1, group)]
    barrier = pltpu.get_barrier_semaphore()
    for peer in others:
        pl.semaphore_signal(barrier, inc=1, device_id=(part, peer), device_id_type=MESH)
    for q in (x_part, y_part):
        pl.semaphore_signal(barrier, inc=1, device_id=(q, me), device_id_type=MESH)
    pl.semaphore_wait(barrier, len(others) + 2)

    def mask_copy(d):
        return pltpu.make_async_remote_copy(
            mine, mbuf.at[me], m_send.at[d], m_recv.at[me],
            device_id=(part, others[d]), device_id_type=MESH,
        )

    def w_rows(block, q, i):
        at, size = pieces[i]
        return wbuf.at[block, pl.ds(pl.multiple_of(q * quarter + at, 16), size)]

    def my_rows(q, i):
        at, size = pieces[i]
        return w_ref.at[pl.ds(pl.multiple_of(q * quarter + at, 16), size)]

    def outer_w(i):
        return copy(my_rows(part, i), w_rows(here, part, i), o_send.at[i], w_recv.at[here, part, i], z_in, half)

    def outer_diag(i):
        return copy(my_rows(d_part, i), w_rows(here, d_part, i), d_send.at[i], w_recv.at[here, d_part, i], z_in, half)

    def far_w(i):
        return copy(my_rows(part, i), w_rows(here, part, i), o_send.at[i], w_recv.at[here, part, i], z_far, half)

    def near_w(i):
        at = pl.ds(i * quarter, quarter)
        return copy(w_ref.at[at], wbuf.at[here, at], nw_send.at[i], w_recv.at[here, i, 0], z_in, half)

    def own_w():
        return pltpu.make_async_copy(w_ref, wbuf.at[here], wl_sem.at[0])

    def got_w(block, q, i):
        arrived(w_rows(block, q, i), w_recv.at[block, q, i])

    def along(block, q, i, sems, chip, q_to):
        spot = w_rows(block, q, i)
        return copy(spot, spot, sems.at[block, i], w_recv.at[block, q, i], chip, core, q_to)

    def to_x(block, i):
        return along(block, part, i, x_send, z_in, x_part)

    def to_y(block, i):
        return along(block, part, i, y_send, z_in, y_part)

    def to_far(block, i):
        return along(block, part, i, u_send, z_far, part)

    def x_to_y(block, i):
        return along(block, x_part, i, v_send, z_in, y_part)

    def y_to_x(block, i):
        return along(block, y_part, i, v_send, z_in, x_part)

    def relay(block, u, i):
        return x_to_y(block, i) if (i < 2) == (u == 0) else y_to_x(block, i)

    def e_copy(h, j):
        return copy(e_ref.at[h * per_half + j], ebuf.at[j, me], e_send.at[h, j], e_recv.at[j, me], 1 + h, core)

    def e_far(j):
        return copy(e_ref.at[(1 - half) * per_half + j], ebuf.at[j, me], e_send.at[1, j], e_recv.at[j, me], z_far, core)

    def e_near(j):
        return copy(e_ref.at[half * per_half + j], ebuf.at[j, me], e_send.at[0, j], e_recv.at[j, me], z_in, core)

    def near_e(j):
        return copy(e_ref.at[half * per_half + j], ebuf.at[j, me], n_send.at[j], e_recv.at[j, me], z_in, other)

    def own_e(j):
        return pltpu.make_async_copy(e_ref.at[half * per_half + j], ebuf.at[j, me], el_sem.at[j])

    away = (z_out, z_far, z_end)

    def pass_e(j, k):
        block = away[k] * CORES + core
        spot = ebuf.at[j, block]
        return copy(spot, spot, h_send.at[j, k], e_recv.at[j, block], z_in, other)

    def take_e(j):
        for k in range(3):
            block = away[k] * CORES + core
            arrived(ebuf.at[j, block], e_recv.at[j, block])
            pass_e(j, k).start()

    def have_e(j):
        own_e(j).wait()
        for chip in (z_in,) + away:
            block = chip * CORES + other
            arrived(ebuf.at[j, block], e_recv.at[j, block])

    def partial_copy(j):
        return copy(pbuf.at[j], qbuf.at[j], p_send.at[j], p_recv.at[j], z_in, other)

    def project(q, j):
        at = pl.ds(pl.multiple_of(q * quarter, 16), quarter)
        left = wbuf[:, at].reshape(side * quarter, features)
        right = ebuf[j].reshape(rows, features)
        zt[j, :, at] = lax.dot_general(
            left, right, NT, preferred_element_type=jnp.float32
        ).astype(jnp.bfloat16).reshape(side, quarter, rows)

    lanes = pl.ds(pl.multiple_of(core * span, 128), span)
    mine_at = pl.multiple_of(core * half_rows, half_rows)
    theirs_at = pl.multiple_of(other * half_rows, half_rows)

    def score(j):
        left = ebuf[j, :, :, lanes].reshape(rows, span)
        raw = jnp.dot(left, zt[j].reshape(span, rows), preferred_element_type=jnp.float32)
        sbuf[...] = raw - jnp.transpose(raw)
        pbuf[j] = sbuf[pl.ds(theirs_at, half_rows)]
        partial_copy(j).start()
        keep[j] = sbuf[pl.ds(mine_at, half_rows)]

    def final_copy(j, t):
        row = pl.multiple_of(t * block_rows, block_rows)
        return pltpu.make_async_remote_copy(
            fbuf.at[j, pl.ds(row, block_rows)], rbuf.at[half * per_half + j],
            r_send.at[j, t], r_recv.at[half * per_half + j],
            device_id=(part, core * side + t), device_id_type=MESH,
        )

    def each_target(j, act):
        for t in range(side):
            @pl.when(core * side + t != me)
            def _():
                act(final_copy(j, t))

    def finish(j):
        arrived(qbuf.at[j], p_recv.at[j])
        fbuf[j] = (keep[j] + qbuf[j]).astype(jnp.bfloat16)
        each_target(j, lambda c: c.start())

        @pl.when(near)
        def _():
            row = pl.multiple_of(here * block_rows, block_rows)
            rbuf[half * per_half + j] = fbuf[j, pl.ds(row, block_rows)]

    def each_mask():
        for d in range(group - 1):
            mask_copy(d).start()

    def settle():
        for j in range(per_half):
            e_far(j).wait_send()
            near_e(j).wait_send()
            for k in range(3):
                pass_e(j, k).wait_send()
            partial_copy(j).wait_send()
            each_target(j, lambda c: c.wait_send())
        for i in range(len(pieces)):
            far_w(i).wait_send()

    def loop(n, body):
        def run(j, carry):
            body(j)
            return carry
        lax.fori_loop(0, n, run, 0)

    def all_quarters(j):
        loop(PARTS, lambda q: project(q, j))

    @pl.when(jnp.logical_not(inner))
    def _():
        for i in range(len(pieces)):
            outer_w(i).start()
        for j in range(per_half):
            e_far(j).start()
            e_near(j).start()
            if j == 0:
                for i in range(len(pieces)):
                    outer_diag(i).start()
        each_mask()
        for i in range(len(pieces)):
            outer_w(i).wait_send()
            outer_diag(i).wait_send()
        for j in range(per_half):
            e_far(j).wait_send()
            e_near(j).wait_send()

    @pl.when(jnp.logical_and(inner, near))
    def _():
        for i in range(len(pieces)):
            far_w(i).start()
        e_far(0).start()
        own_w().start()
        for j in range(per_half):
            own_e(j).start()
            near_e(j).start()
        for i in range(len(pieces)):
            for u in range(2):
                got_w(first + u, part, i)
                to_x(first + u, i).start()
                to_y(first + u, i).start()
                to_far(first + u, i).start()
        for j in range(1, per_half):
            e_far(j).start()
        each_mask()
        take_e(0)
        own_w().wait()
        for q in range(PARTS):
            at = pl.ds(q * quarter, quarter)
            beside = second + other
            arrived(wbuf.at[beside, at], w_recv.at[beside, q, 0])
        for i in range(len(pieces)):
            for u in range(2):
                for q in (x_part, y_part, d_part):
                    got_w(first + u, q, i)
        take_e(1)

        def turn(j):
            @pl.when(j > 1)
            def _():
                take_e(j)
            have_e(j)
            all_quarters(j)
            score(j)

        loop(per_half, turn)
        loop(per_half, finish)
        settle()
        for i in range(len(pieces)):
            for u in range(2):
                to_x(first + u, i).wait_send()
                to_y(first + u, i).wait_send()
                to_far(first + u, i).wait_send()

    @pl.when(jnp.logical_and(inner, jnp.logical_not(near)))
    def _():
        for i in range(len(pieces)):
            far_w(i).start()
        for j in range(per_half):
            e_far(j).start()
        for i in range(PARTS):
            near_w(i).start()
        for j in range(per_half):
            own_e(j).start()
            near_e(j).start()
        each_mask()
        for base in (first, second):
            for i in range(len(pieces)):
                for u in range(2):
                    got_w(base + u, part, i)
                    to_x(base + u, i).start()
                    to_y(base + u, i).start()

        def relays(base):
            for i in range(len(pieces)):
                for u in range(2):
                    for q in (x_part, y_part):
                        got_w(base + u, q, i)
                    relay(base + u, u, i).start()

        relays(first)
        take_e(0)
        take_e(1)

        def early(j):
            have_e(j)
            project(part, j)

        loop(2, early)
        relays(second)

        def middle(j):
            @pl.when(j == 2)
            def _():
                take_e(2)
                early(2)
            project(x_part, j)
            project(y_part, j)

        loop(3, middle)
        for i in range(len(pieces)):
            for u in range(2):
                for base in (first, second):
                    got_w(base + u, d_part, i)

        def late(j):
            project(d_part, j)
            score(j)

        loop(3, late)
        take_e(3)
        have_e(3)
        all_quarters(3)
        score(3)
        loop(per_half, finish)
        settle()
        for i in range(PARTS):
            near_w(i).wait_send()
        for i in range(len(pieces)):
            for base in (first, second):
                for u in range(2):
                    to_x(base + u, i).wait_send()
                    to_y(base + u, i).wait_send()
                    relay(base + u, u, i).wait_send()

    for h in range(2):
        local = jnp.logical_and(jnp.logical_and(inner, near), half == h)

        @pl.when(jnp.logical_not(local))
        def _():
            for j in range(per_half):
                arrived(rbuf.at[h * per_half + j], r_recv.at[h * per_half + j])

    for d in range(group - 1):
        mask_copy(d).wait_send()
        arrived(mbuf.at[others[d]], m_recv.at[others[d]])
    mbuf[me] = mine[...]
    counts = mbuf[0]
    for g in range(1, group):
        counts = counts + mbuf[g]
    counts = counts[:, :1].astype(jnp.float32)
    slot = lax.broadcasted_iota(jnp.int32, (prompts, rows), 1).astype(jnp.float32)
    cols = (slot < counts).astype(jnp.float32)
    pairs = jnp.maximum(counts - 1.0, 1.0)
    same = lax.broadcasted_iota(jnp.int32, (block_rows, block_rows), 0)
    same = (same == lax.broadcasted_iota(jnp.int32, (block_rows, block_rows), 1)).astype(jnp.float32)
    down = lax.dot_general(same, valid, NT, preferred_element_type=jnp.float32)
    lane = lax.broadcasted_iota(jnp.int32, (block_rows, 128), 1)
    rates = jnp.zeros((block_rows, 128), jnp.float32)
    for p in range(prompts):
        given = down[:, p:p + 1]
        prefs = jax.nn.sigmoid(rbuf[p].astype(jnp.float32)) * given * cols[p:p + 1, :]
        o_ref[p] = prefs
        totals = jnp.sum(prefs, axis=1, keepdims=True) - 0.5 * given
        rates = jnp.where(lane == p, given * totals / pairs[p:p + 1, :], rates)
    r_ref[...] = jnp.transpose(rates)[:prompts]


def line_scores(embeddings, head_weight, mask):
    prompts, block_rows, features = embeddings.shape
    held = head_weight.shape[0]
    group = CHIPS * CORES
    side = group // 2
    per_half = prompts // 2
    rows = group * block_rows
    half_rows = rows // 2
    quarter = held // PARTS
    bf16, f32 = jnp.bfloat16, jnp.float32
    dma = pltpu.SemaphoreType.DMA
    anywhere = pl.BlockSpec(memory_space=pl.ANY)
    vmem = pl.BlockSpec(memory_space=pltpu.VMEM)
    return pl.pallas_call(
        kernel,
        out_shape=(
            jax.ShapeDtypeStruct((prompts, block_rows, rows), f32),
            jax.ShapeDtypeStruct((prompts, block_rows), f32),
        ),
        in_specs=[anywhere, anywhere, vmem],
        out_specs=(vmem, vmem),
        scratch_shapes=[
            pltpu.VMEM((per_half, group, block_rows, features), bf16),
            pltpu.VMEM((side, held, features), bf16),
            pltpu.VMEM((per_half, side, held, rows), bf16),
            pltpu.VMEM((rows, rows), f32),
            pltpu.VMEM((per_half, half_rows, rows), f32),
            pltpu.VMEM((per_half, half_rows, rows), f32),
            pltpu.VMEM((per_half, half_rows, rows), f32),
            pltpu.VMEM((per_half, half_rows, rows), bf16),
            pltpu.VMEM((prompts, block_rows, rows), bf16),
            pltpu.VMEM((prompts, 128), jnp.int32),
            pltpu.VMEM((group, prompts, 128), jnp.int32),
            dma((group - 1,)),
            dma((group,)),
            dma((2, per_half)),
            dma((per_half, group)),
            dma((per_half,)),
            dma((per_half, 3)),
            dma((per_half,)),
            dma((4,)),
            dma((4,)),
            dma((4,)),
            dma((PARTS,)),
            dma((1,)),
            dma((side, 4)),
            dma((side, 4)),
            dma((side, 4)),
            dma((side, 4)),
            dma((side, PARTS, 4)),
            dma((per_half,)),
            dma((per_half,)),
            dma((per_half, side)),
            dma((prompts,)),
        ],
        compiler_params=pltpu.CompilerParams(
            collective_id=0, has_side_effects=True, vmem_limit_bytes=56 << 20
        ),
    )(embeddings, head_weight, mask)


def shards(embeddings, head_weight, valid_mask):
    group_size = lax.axis_size("resp")
    slots = group_size * embeddings.shape[1]
    if (lax.axis_size("prompt"), group_size) == (PARTS, CHIPS * CORES):
        return line_scores(embeddings, head_weight, valid_mask)
    valid_rows = valid_mask.astype(jnp.float32)
    counts = lax.psum(jnp.sum(valid_rows, axis=1), "resp")
    scores = gathered_scores(embeddings, head_weight)
    column_ids = jnp.arange(slots, dtype=jnp.float32)
    valid_cols = (column_ids[None, :] < counts[:, None]).astype(jnp.float32)
    preferences = jax.nn.sigmoid(scores) * valid_rows[:, :, None] * valid_cols[:, None, :]
    totals = jnp.sum(preferences, axis=2) - 0.5 * valid_rows
    win_rates = valid_rows * totals / jnp.maximum(counts - 1.0, 1.0)[:, None]
    return (preferences, win_rates)


def solution(mesh):
    return jax.shard_map(
        shards,
        mesh=mesh,
        in_specs=(P("prompt", "resp", None), P("resp", None), P("prompt", "resp")),
        out_specs=(P("prompt", "resp", None), P("prompt", "resp")),
        check_vma=False,
    )
```

```python
import functools

import jax
import jax.numpy as jnp
from jax import lax
from jax.experimental import pallas as pl
from jax.experimental.pallas import tpu as pltpu
from jax.sharding import PartitionSpec as P

MESH = pl.DeviceIdType.MESH
CORES = 2
CHIPS = 4
PARTS = 4
NT = (((1,), (1,)), ((), ()))


def gathered_halves(embeddings, head_weight, own_index, group_size):
    prompts, block_rows, features = embeddings.shape
    held = head_weight.shape[0]
    slots = group_size * block_rows
    everyone = lax.all_gather(embeddings, "resp", axis=0, tiled=True)
    flat = everyone.reshape(group_size * prompts * block_rows, features)
    through = lax.dot_general(flat, head_weight, NT, preferred_element_type=jnp.float32)
    through = through.astype(jnp.bfloat16).reshape(group_size, prompts, block_rows, held)
    mine = lax.dynamic_slice_in_dim(
        everyone.reshape(group_size, prompts, block_rows, features), own_index * held, held, 3
    )
    partial = jnp.einsum("gpid,hpjd->gpihj", mine, through, preferred_element_type=jnp.float32)
    flipped = jnp.einsum("gpid,hpjd->gpihj", through, mine, preferred_element_type=jnp.float32)
    partial = (partial - flipped).astype(jnp.bfloat16)
    return partial.reshape(group_size, prompts, block_rows, slots)


def gathered_scores(embeddings, head_weight):
    group_size = lax.axis_size("resp")
    own_index = lax.axis_index("resp")
    prompts, block_rows, features = embeddings.shape
    slots = group_size * block_rows
    at_once = max(1, min(prompts, (1 << 11) // slots))

    def scores_of(some):
        partial = gathered_halves(some, head_weight, own_index, group_size)
        swapped = lax.all_to_all(partial, "resp", split_axis=0, concat_axis=0, tiled=True)
        return jnp.sum(swapped.astype(jnp.float32), axis=0)

    pieces = embeddings.reshape(prompts // at_once, at_once, block_rows, features)
    return lax.map(scores_of, pieces).reshape(prompts, block_rows, slots)


def kernel(e_ref, w_ref, m_ref, o_ref, r_ref,
           ebuf, wbuf, gbuf, zt, sbuf, keep, pbuf, qbuf, fbuf, rbuf, mine, mbuf,
           m_send, m_recv, e_send, e_recv, n_send, h_send, el_sem,
           o_send, d_send, nw_send, wl_sem, g_recv, x_send, y_send, u_send, v_send, w_recv,
           p_send, p_recv, r_send, r_recv):
    part = lax.axis_index("prompt")
    me = lax.axis_index("resp")
    z = me // CORES
    core = me % CORES
    half = z // 2
    prompts, block_rows, features = e_ref.shape
    held = w_ref.shape[0]
    group = CHIPS * CORES
    per_half = prompts // 2
    side = group // 2
    span = held * side
    rows = group * block_rows
    half_rows = rows // 2
    quarter = held // PARTS
    z_in = 1 + half
    z_out = 3 * half
    z_far = 2 - half
    z_end = 3 - z_out
    inner = z == z_in
    near = core == half
    other = 1 - core
    first = 2 * half
    second = 2 - first
    here = me % side
    x_part = part + 1 - 2 * (part % 2)
    y_part = lax.rem(part + 2, PARTS)
    d_part = PARTS - 1 - part
    chip_width = features // CHIPS
    step = quarter // 7
    pieces = ((0, step), (step, 2 * step), (3 * step, 2 * step), (5 * step, 2 * step))

    def copy(src, dst, send, recv, chip, c, q=None):
        return pltpu.make_async_remote_copy(
            src, dst, send, recv,
            device_id=(part if q is None else q, chip * CORES + c), device_id_type=MESH,
        )

    def arrived(dst, recv):
        copy(dst, dst, m_send.at[0], recv, z_far, core).wait_recv()

    valid = m_ref[...].astype(jnp.float32)
    mine[...] = jnp.broadcast_to(jnp.sum(m_ref[...], axis=1, keepdims=True), mine.shape)

    folded = pl.ds(jnp.where(near, second, first), 2)
    away_cols = pl.ds(pl.multiple_of(jnp.where(near, z_out, 3 - z_out) * chip_width, 128), chip_width)
    wbuf[folded, :, away_cols] = jnp.zeros((2, held, chip_width), jnp.bfloat16)

    others = [lax.rem(me + d, group) for d in range(1, group)]
    barrier = pltpu.get_barrier_semaphore()
    for peer in others:
        pl.semaphore_signal(barrier, inc=1, device_id=(part, peer), device_id_type=MESH)
    for q in (x_part, y_part):
        pl.semaphore_signal(barrier, inc=1, device_id=(q, me), device_id_type=MESH)
    pl.semaphore_wait(barrier, len(others) + 2)

    def mask_copy(d):
        return pltpu.make_async_remote_copy(
            mine, mbuf.at[me], m_send.at[d], m_recv.at[me],
            device_id=(part, others[d]), device_id_type=MESH,
        )

    def chip_cols(chip):
        return pl.ds(pl.multiple_of(chip * chip_width, 128), chip_width)

    def kept_cols(h):
        return pl.ds(pl.multiple_of((1 - h) * chip_width, 128), features - chip_width)

    every = pl.ds(0, features)

    def w_rows(block, q, i, cols=every):
        at, size = pieces[i]
        return wbuf.at[block, pl.ds(pl.multiple_of(q * quarter + at, 16), size), cols]

    def my_rows(q, i, cols=every):
        at, size = pieces[i]
        return w_ref.at[pl.ds(pl.multiple_of(q * quarter + at, 16), size), cols]

    def outer_w(i):
        return copy(my_rows(part, i), w_rows(here, part, i), o_send.at[i], w_recv.at[here, part, i], z_in, half)

    def outer_diag(i):
        return copy(my_rows(d_part, i), w_rows(here, d_part, i), d_send.at[i], w_recv.at[here, d_part, i], z_in, half)

    def far_w(i):
        cols = kept_cols(half)
        return copy(my_rows(part, i, cols), w_rows(here, part, i, cols), o_send.at[i],
                    w_recv.at[here, part, i], z_far, half)

    def near_w(i):
        at = pl.ds(i * quarter, quarter)
        cols = kept_cols(half)
        return copy(w_ref.at[at, cols], wbuf.at[here, at, cols], nw_send.at[i], w_recv.at[here, i, 0], z_in, half)

    def near_g():
        return copy(w_ref.at[:, chip_cols(z_out)], gbuf.at[core], nw_send.at[PARTS], g_recv.at[0], z_in, half)

    def own_w():
        cols = kept_cols(half)
        return pltpu.make_async_copy(w_ref.at[:, cols], wbuf.at[here, :, cols], wl_sem.at[0])

    def own_g():
        return pltpu.make_async_copy(w_ref.at[:, chip_cols(z_out)], gbuf.at[core], wl_sem.at[1])

    def fold(q, at, size):
        start = q * quarter + at
        row = lax.broadcasted_iota(jnp.int32, (2 * size, chip_width), 0)
        col = lax.broadcasted_iota(jnp.int32, (2 * size, chip_width), 1)
        pick = (start + jnp.where(row < size, row, row + held - size) == col).astype(jnp.bfloat16)
        turned = lax.dot_general(
            pick, gbuf[...].reshape(chip_width, chip_width), NT, preferred_element_type=jnp.float32
        ).reshape(2, size, chip_width)
        pair, where, cols = pl.ds(first, 2), pl.ds(pl.multiple_of(start, 16), size), chip_cols(z_in)
        wbuf[pair, where, cols] = (wbuf[pair, where, cols].astype(jnp.float32) - turned).astype(jnp.bfloat16)

    def got_w(block, q, i, cols=every):
        arrived(w_rows(block, q, i, cols), w_recv.at[block, q, i])

    def along(block, q, i, sems, chip, q_to, cols):
        spot = w_rows(block, q, i, cols)
        return copy(spot, spot, sems.at[block, i], w_recv.at[block, q, i], chip, core, q_to)

    def to_x(block, i, cols=every):
        return along(block, part, i, x_send, z_in, x_part, cols)

    def to_y(block, i, cols=every):
        return along(block, part, i, y_send, z_in, y_part, cols)

    def to_far(block, i):
        return along(block, part, i, u_send, z_far, part, every)

    def relay(block, u, i, cols=every):
        if (i < 2) == (u == 0):
            return along(block, x_part, i, v_send, z_in, y_part, cols)
        return along(block, y_part, i, v_send, z_in, x_part, cols)

    passed = ((first, kept_cols(1 - half)), (second, every))

    def e_far(j):
        return copy(e_ref.at[(1 - half) * per_half + j], ebuf.at[j, me], e_send.at[1, j], e_recv.at[j, me], z_far, core)

    def e_near(j):
        return copy(e_ref.at[half * per_half + j], ebuf.at[j, me], e_send.at[0, j], e_recv.at[j, me], z_in, core)

    def near_e(j):
        return copy(e_ref.at[half * per_half + j], ebuf.at[j, me], n_send.at[j], e_recv.at[j, me], z_in, other)

    def own_e(j):
        return pltpu.make_async_copy(e_ref.at[half * per_half + j], ebuf.at[j, me], el_sem.at[j])

    away = (z_out, z_far, z_end)

    def pass_e(j, k):
        block = away[k] * CORES + core
        spot = ebuf.at[j, block]
        return copy(spot, spot, h_send.at[j, k], e_recv.at[j, block], z_in, other)

    def take_e(j):
        for k in range(3):
            block = away[k] * CORES + core
            arrived(ebuf.at[j, block], e_recv.at[j, block])
            pass_e(j, k).start()

    def have_e(j):
        own_e(j).wait()
        for chip in (z_in,) + away:
            block = chip * CORES + other
            arrived(ebuf.at[j, block], e_recv.at[j, block])

    def partial_copy(j):
        return copy(pbuf.at[j], qbuf.at[j], p_send.at[j], p_recv.at[j], z_in, other)

    def project(q, j):
        at = pl.ds(pl.multiple_of(q * quarter, 16), quarter)
        left = wbuf[:, at].reshape(side * quarter, features)
        right = ebuf[j].reshape(rows, features)
        zt[j, :, at] = lax.dot_general(
            left, right, NT, preferred_element_type=jnp.float32
        ).astype(jnp.bfloat16).reshape(side, quarter, rows)

    lanes = pl.ds(pl.multiple_of(core * span, 128), span)
    mine_at = pl.multiple_of(core * half_rows, half_rows)
    theirs_at = pl.multiple_of(other * half_rows, half_rows)

    def score(j):
        left = ebuf[j, :, :, lanes].reshape(rows, span)
        raw = jnp.dot(left, zt[j].reshape(span, rows), preferred_element_type=jnp.float32)
        sbuf[...] = raw - jnp.transpose(raw)
        pbuf[j] = sbuf[pl.ds(theirs_at, half_rows)]
        partial_copy(j).start()
        keep[j] = sbuf[pl.ds(mine_at, half_rows)]

    def final_copy(j, t):
        row = pl.multiple_of(t * block_rows, block_rows)
        return pltpu.make_async_remote_copy(
            fbuf.at[j, pl.ds(row, block_rows)], rbuf.at[half * per_half + j],
            r_send.at[j, t], r_recv.at[half * per_half + j],
            device_id=(part, core * side + t), device_id_type=MESH,
        )

    def each_target(j, act):
        for t in range(side):
            @pl.when(core * side + t != me)
            def _():
                act(final_copy(j, t))

    def finish(j):
        arrived(qbuf.at[j], p_recv.at[j])
        fbuf[j] = (keep[j] + qbuf[j]).astype(jnp.bfloat16)
        each_target(j, lambda c: c.start())

        @pl.when(near)
        def _():
            row = pl.multiple_of(here * block_rows, block_rows)
            rbuf[half * per_half + j] = fbuf[j, pl.ds(row, block_rows)]

    def each_mask():
        for d in range(group - 1):
            mask_copy(d).start()

    def settle():
        for j in range(per_half):
            e_far(j).wait_send()
            near_e(j).wait_send()
            for k in range(3):
                pass_e(j, k).wait_send()
            partial_copy(j).wait_send()
            each_target(j, lambda c: c.wait_send())
        for i in range(len(pieces)):
            far_w(i).wait_send()

    def loop(n, body):
        def run(j, carry):
            body(j)
            return carry
        lax.fori_loop(0, n, run, 0)

    def all_quarters(j):
        loop(PARTS, lambda q: project(q, j))

    @pl.when(jnp.logical_not(inner))
    def _():
        for i in range(len(pieces)):
            outer_w(i).start()
        each_mask()
        for i in range(len(pieces)):
            outer_diag(i).start()
        for j in range(per_half):
            e_far(j).start()
            e_near(j).start()

    @pl.when(jnp.logical_and(inner, near))
    def _():
        for i in range(len(pieces)):
            far_w(i).start()
        each_mask()
        own_g().start()
        own_w().start()
        for j in range(per_half):
            own_e(j).start()
            near_e(j).start()
        own_g().wait()
        arrived(gbuf.at[other], g_recv.at[0])
        for i in range(len(pieces)):
            for u in range(2):
                got_w(first + u, part, i)
            fold(part, *pieces[i])
            for u in range(2):
                to_far(first + u, i).start()
                to_x(first + u, i).start()
                to_y(first + u, i).start()
        for j in range(per_half):
            e_far(j).start()
        own_w().wait()
        for q in range(PARTS):
            at = pl.ds(q * quarter, quarter)
            beside = second + other
            arrived(wbuf.at[beside, at, kept_cols(half)], w_recv.at[beside, q, 0])
        for i in range(len(pieces)):
            for u in range(2):
                for q in (x_part, y_part, d_part):
                    got_w(first + u, q, i)
        fold(d_part, 0, quarter)

        def turn(j):
            take_e(j)
            have_e(j)
            all_quarters(j)

            @pl.when(j == per_half - 1)
            def _():
                loop(per_half - 1, finish)
            score(j)

        loop(per_half, turn)
        finish(per_half - 1)

    @pl.when(jnp.logical_and(inner, jnp.logical_not(near)))
    def _():
        near_g().start()
        for i in range(len(pieces)):
            far_w(i).start()
        each_mask()
        for i in range(PARTS):
            near_w(i).start()
        for j in range(per_half):
            own_e(j).start()
            near_e(j).start()
        for base, cols in passed:
            for i in range(len(pieces)):
                for u in range(2):
                    got_w(base + u, part, i, cols)
                    to_x(base + u, i, cols).start()
                    to_y(base + u, i, cols).start()
        for j in range(per_half):
            e_far(j).start()

        def relays(base, cols, i):
            for u in range(2):
                for q in (x_part, y_part):
                    got_w(base + u, q, i, cols)
                relay(base + u, u, i, cols).start()

        for i in range(len(pieces)):
            relays(*passed[0], i)
        take_e(0)
        have_e(0)
        project(part, 0)
        for i in range(len(pieces)):
            if i == len(pieces) - 1:
                take_e(1)
            relays(*passed[1], i)

        def middle(j):
            @pl.when(j > 0)
            def _():
                @pl.when(j > 1)
                def _():
                    take_e(j)
                have_e(j)
                project(part, j)
            project(x_part, j)
            project(y_part, j)

        loop(3, middle)
        for base, cols in passed:
            for i in range(len(pieces)):
                for u in range(2):
                    got_w(base + u, d_part, i, cols)

        def late(j):
            @pl.when(j == 2)
            def _():
                take_e(3)
            project(d_part, j)
            score(j)

        loop(3, late)
        loop(3, finish)
        have_e(3)
        all_quarters(3)
        score(3)
        finish(3)

    for d in range(group - 1):
        arrived(mbuf.at[others[d]], m_recv.at[others[d]])
    mbuf[me] = mine[...]
    counts = mbuf[0]
    for g in range(1, group):
        counts = counts + mbuf[g]
    counts = counts[:, :1].astype(jnp.float32)
    slot = lax.broadcasted_iota(jnp.int32, (prompts, rows), 1).astype(jnp.float32)
    cols = (slot < counts).astype(jnp.float32)
    pairs = jnp.maximum(counts - 1.0, 1.0)
    same = lax.broadcasted_iota(jnp.int32, (block_rows, block_rows), 0)
    same = (same == lax.broadcasted_iota(jnp.int32, (block_rows, block_rows), 1)).astype(jnp.float32)
    down = lax.dot_general(same, valid, NT, preferred_element_type=jnp.float32)
    lane = lax.broadcasted_iota(jnp.int32, (block_rows, 128), 1)
    rates = jnp.zeros((block_rows, 128), jnp.float32)
    for j in range(per_half):
        for h in range(2):
            p = h * per_half + j

            @pl.when(jnp.logical_not(jnp.logical_and(jnp.logical_and(inner, near), half == h)))
            def _():
                arrived(rbuf.at[p], r_recv.at[p])
            given = down[:, p:p + 1]
            prefs = jax.nn.sigmoid(rbuf[p].astype(jnp.float32)) * given * cols[p:p + 1, :]
            o_ref[p] = prefs
            totals = jnp.sum(prefs, axis=1, keepdims=True) - 0.5 * given
            rates = jnp.where(lane == p, given * totals / pairs[p:p + 1, :], rates)
    r_ref[...] = jnp.transpose(rates)[:prompts]

    for d in range(group - 1):
        mask_copy(d).wait_send()

    @pl.when(jnp.logical_not(inner))
    def _():
        for i in range(len(pieces)):
            outer_w(i).wait_send()
            outer_diag(i).wait_send()
        for j in range(per_half):
            e_far(j).wait_send()
            e_near(j).wait_send()

    @pl.when(inner)
    def _():
        settle()

    @pl.when(jnp.logical_and(inner, near))
    def _():
        for i in range(len(pieces)):
            for u in range(2):
                to_x(first + u, i).wait_send()
                to_y(first + u, i).wait_send()
                to_far(first + u, i).wait_send()

    @pl.when(jnp.logical_and(inner, jnp.logical_not(near)))
    def _():
        near_g().wait_send()
        for i in range(PARTS):
            near_w(i).wait_send()
        for i in range(len(pieces)):
            for base, cols in passed:
                for u in range(2):
                    to_x(base + u, i, cols).wait_send()
                    to_y(base + u, i, cols).wait_send()
                    relay(base + u, u, i, cols).wait_send()


def line_scores(embeddings, head_weight, mask):
    prompts, block_rows, features = embeddings.shape
    held = head_weight.shape[0]
    group = CHIPS * CORES
    side = group // 2
    per_half = prompts // 2
    rows = group * block_rows
    half_rows = rows // 2
    quarter = held // PARTS
    bf16, f32 = jnp.bfloat16, jnp.float32
    dma = pltpu.SemaphoreType.DMA
    anywhere = pl.BlockSpec(memory_space=pl.ANY)
    vmem = pl.BlockSpec(memory_space=pltpu.VMEM)
    return pl.pallas_call(
        kernel,
        out_shape=(
            jax.ShapeDtypeStruct((prompts, block_rows, rows), f32),
            jax.ShapeDtypeStruct((prompts, block_rows), f32),
        ),
        in_specs=[anywhere, anywhere, vmem],
        out_specs=(vmem, vmem),
        scratch_shapes=[
            pltpu.VMEM((per_half, group, block_rows, features), bf16),
            pltpu.VMEM((side, held, features), bf16),
            pltpu.VMEM((CORES, held, features // CHIPS), bf16),
            pltpu.VMEM((per_half, side, held, rows), bf16),
            pltpu.VMEM((rows, rows), f32),
            pltpu.VMEM((per_half, half_rows, rows), f32),
            pltpu.VMEM((per_half, half_rows, rows), f32),
            pltpu.VMEM((per_half, half_rows, rows), f32),
            pltpu.VMEM((per_half, half_rows, rows), bf16),
            pltpu.VMEM((prompts, block_rows, rows), bf16),
            pltpu.VMEM((prompts, 128), jnp.int32),
            pltpu.VMEM((group, prompts, 128), jnp.int32),
            dma((group - 1,)),
            dma((group,)),
            dma((2, per_half)),
            dma((per_half, group)),
            dma((per_half,)),
            dma((per_half, 3)),
            dma((per_half,)),
            dma((4,)),
            dma((4,)),
            dma((PARTS + 1,)),
            dma((2,)),
            dma((1,)),
            dma((side, 4)),
            dma((side, 4)),
            dma((side, 4)),
            dma((side, 4)),
            dma((side, PARTS, 4)),
            dma((per_half,)),
            dma((per_half,)),
            dma((per_half, side)),
            dma((prompts,)),
        ],
        compiler_params=pltpu.CompilerParams(
            collective_id=0, has_side_effects=True, vmem_limit_bytes=56 << 20
        ),
    )(embeddings, head_weight, mask)


def shards(embeddings, head_weight, valid_mask):
    group_size = lax.axis_size("resp")
    slots = group_size * embeddings.shape[1]
    if (lax.axis_size("prompt"), group_size) == (PARTS, CHIPS * CORES):
        return line_scores(embeddings, head_weight, valid_mask)
    valid_rows = valid_mask.astype(jnp.float32)
    counts = lax.psum(jnp.sum(valid_rows, axis=1), "resp")
    scores = gathered_scores(embeddings, head_weight)
    column_ids = jnp.arange(slots, dtype=jnp.float32)
    valid_cols = (column_ids[None, :] < counts[:, None]).astype(jnp.float32)
    preferences = jax.nn.sigmoid(scores) * valid_rows[:, :, None] * valid_cols[:, None, :]
    totals = jnp.sum(preferences, axis=2) - 0.5 * valid_rows
    win_rates = valid_rows * totals / jnp.maximum(counts - 1.0, 1.0)[:, None]
    return (preferences, win_rates)


def solution(mesh):
    return jax.shard_map(
        shards,
        mesh=mesh,
        in_specs=(P("prompt", "resp", None), P("resp", None), P("prompt", "resp")),
        out_specs=(P("prompt", "resp", None), P("prompt", "resp")),
        check_vma=False,
    )
```

```python
import functools

import jax
import jax.numpy as jnp
from jax import lax
from jax.experimental import pallas as pl
from jax.experimental.pallas import tpu as pltpu
from jax.sharding import PartitionSpec as P

MESH = pl.DeviceIdType.MESH
CORES = 2
CHIPS = 4
PARTS = 4
CHUNKS = 2
DIRECT = 3
NT = (((1,), (1,)), ((), ()))


def gathered_halves(embeddings, head_weight, own_index, group_size):
    prompts, block_rows, features = embeddings.shape
    held = head_weight.shape[0]
    slots = group_size * block_rows
    everyone = lax.all_gather(embeddings, "resp", axis=0, tiled=True)
    flat = everyone.reshape(group_size * prompts * block_rows, features)
    through = lax.dot_general(flat, head_weight, NT, preferred_element_type=jnp.float32)
    through = through.astype(jnp.bfloat16).reshape(group_size, prompts, block_rows, held)
    mine = lax.dynamic_slice_in_dim(
        everyone.reshape(group_size, prompts, block_rows, features), own_index * held, held, 3
    )
    partial = jnp.einsum("gpid,hpjd->gpihj", mine, through, preferred_element_type=jnp.float32)
    flipped = jnp.einsum("gpid,hpjd->gpihj", through, mine, preferred_element_type=jnp.float32)
    partial = (partial - flipped).astype(jnp.bfloat16)
    return partial.reshape(group_size, prompts, block_rows, slots)


def gathered_scores(embeddings, head_weight):
    group_size = lax.axis_size("resp")
    own_index = lax.axis_index("resp")
    prompts, block_rows, features = embeddings.shape
    slots = group_size * block_rows
    at_once = max(1, min(prompts, (1 << 11) // slots))

    def scores_of(some):
        partial = gathered_halves(some, head_weight, own_index, group_size)
        swapped = lax.all_to_all(partial, "resp", split_axis=0, concat_axis=0, tiled=True)
        return jnp.sum(swapped.astype(jnp.float32), axis=0)

    pieces = embeddings.reshape(prompts // at_once, at_once, block_rows, features)
    return lax.map(scores_of, pieces).reshape(prompts, block_rows, slots)


def kernel(e_ref, w_ref, m_hbm, o_ref, r_ref,
           m_ref, ebuf, wbuf, gbuf, zt, zsum, sbuf, keep, pbuf, qbuf, fbuf, rbuf, mine, mbuf,
           m_sem, m_send, m_recv, e_send, e_recv, n_send, h_send, el_sem,
           o_send, d_send, nw_send, wl_sem, g_recv, x_send, y_send, u_send, v_send, w_recv,
           p_send, p_recv, r_send, r_recv):
    part = lax.axis_index("prompt")
    me = lax.axis_index("resp")
    z = me // CORES
    core = me % CORES
    half = z // 2
    prompts, block_rows, features = e_ref.shape
    held = w_ref.shape[0]
    group = CHIPS * CORES
    per_half = prompts // 2
    side = group // 2
    span = held * side
    rows = group * block_rows
    half_rows = rows // 2
    quarter = held // PARTS
    z_in = 1 + half
    z_out = 3 * half
    z_far = 2 - half
    z_end = 3 - z_out
    inner = z == z_in
    near = core == half
    other = 1 - core
    first = 2 * half
    second = 2 - first
    here = me % side
    x_part = part + 1 - 2 * (part % 2)
    y_part = lax.rem(part + 2, PARTS)
    d_part = PARTS - 1 - part
    chip_width = features // CHIPS
    step = quarter // 7
    last = per_half - 1
    pieces = ((0, step), (step, 2 * step), (3 * step, 2 * step), (5 * step, 2 * step))

    chunk_width = features // CHUNKS

    def copy(src, dst, send, recv, chip, c, q=None):
        return pltpu.make_async_remote_copy(
            src, dst, send, recv,
            device_id=(part if q is None else q, chip * CORES + c), device_id_type=MESH,
        )

    def arrived(dst, recv):
        copy(dst, dst, m_send.at[0], recv, z_far, core).wait_recv()

    m_copy = pltpu.make_async_copy(m_hbm, m_ref, m_sem.at[0])
    m_copy.start()
    others = [lax.rem(me + d, group) for d in range(1, group)]
    barrier = pltpu.get_barrier_semaphore()
    for peer in others:
        pl.semaphore_signal(barrier, inc=1, device_id=(part, peer), device_id_type=MESH)
    for q in (x_part, y_part):
        pl.semaphore_signal(barrier, inc=1, device_id=(q, me), device_id_type=MESH)

    def mask_copy(d):
        return pltpu.make_async_remote_copy(
            mine, mbuf.at[me], m_send.at[d], m_recv.at[me],
            device_id=(part, others[d]), device_id_type=MESH,
        )

    def chip_cols(chip):
        return pl.ds(pl.multiple_of(chip * chip_width, 128), chip_width)

    def kept_cols(h):
        return pl.ds(pl.multiple_of((1 - h) * chip_width, 128), features - chip_width)

    every = pl.ds(0, features)

    def w_rows(block, q, i, cols=every):
        at, size = pieces[i]
        return wbuf.at[block, pl.ds(pl.multiple_of(q * quarter + at, 16), size), cols]

    def my_rows(q, i, cols=every):
        at, size = pieces[i]
        return w_ref.at[pl.ds(pl.multiple_of(q * quarter + at, 16), size), cols]

    def outer_w(i):
        return copy(my_rows(part, i), w_rows(here, part, i), o_send.at[i], w_recv.at[here, part, i], z_in, half)

    def outer_diag(i):
        return copy(my_rows(d_part, i), w_rows(here, d_part, i), d_send.at[i], w_recv.at[here, d_part, i], z_in, half)

    def far_w(i):
        cols = kept_cols(half)
        return copy(my_rows(part, i, cols), w_rows(here, part, i, cols), o_send.at[i],
                    w_recv.at[here, part, i], z_far, half)

    def near_w(i):
        at = pl.ds(i * quarter, quarter)
        cols = kept_cols(half)
        return copy(w_ref.at[at, cols], wbuf.at[here, at, cols], nw_send.at[i], w_recv.at[here, i, 0], z_in, half)

    def near_g():
        return copy(w_ref.at[:, chip_cols(z_out)], gbuf.at[core], nw_send.at[PARTS], g_recv.at[0], z_in, half)

    def own_w():
        cols = kept_cols(half)
        return pltpu.make_async_copy(w_ref.at[:, cols], wbuf.at[here, :, cols], wl_sem.at[0])

    def own_g():
        return pltpu.make_async_copy(w_ref.at[:, chip_cols(z_out)], gbuf.at[core], wl_sem.at[1])

    def fold(q, at, size):
        start = q * quarter + at
        row = lax.broadcasted_iota(jnp.int32, (2 * size, chip_width), 0)
        col = lax.broadcasted_iota(jnp.int32, (2 * size, chip_width), 1)
        pick = (start + jnp.where(row < size, row, row + held - size) == col).astype(jnp.bfloat16)
        turned = lax.dot_general(
            pick, gbuf[...].reshape(chip_width, chip_width), NT, preferred_element_type=jnp.float32
        ).reshape(2, size, chip_width)
        pair, where, cols = pl.ds(first, 2), pl.ds(pl.multiple_of(start, 16), size), chip_cols(z_in)
        wbuf[pair, where, cols] = (wbuf[pair, where, cols].astype(jnp.float32) - turned).astype(jnp.bfloat16)

    def got_w(block, q, i, cols=every):
        arrived(w_rows(block, q, i, cols), w_recv.at[block, q, i])

    def along(block, q, i, sems, chip, q_to, cols):
        spot = w_rows(block, q, i, cols)
        return copy(spot, spot, sems.at[block, i], w_recv.at[block, q, i], chip, core, q_to)

    def to_x(block, i, cols=every):
        return along(block, part, i, x_send, z_in, x_part, cols)

    def to_y(block, i, cols=every):
        return along(block, part, i, y_send, z_in, y_part, cols)

    def to_far(block, i):
        return along(block, part, i, u_send, z_far, part, every)

    def relay(block, u, i, cols=every):
        if (i < 2) == (u == 0):
            return along(block, x_part, i, v_send, z_in, y_part, cols)
        return along(block, y_part, i, v_send, z_in, x_part, cols)

    passed = ((first, kept_cols(1 - half)), (second, every))

    def chunk_cols(k):
        return pl.ds(pl.multiple_of(k * chunk_width, 128), chunk_width)

    def e_part(j, block, k):
        if k is None:
            return ebuf.at[j, block]
        return ebuf.at[j, block, :, chunk_cols(k)]

    def e_mine(h, j, k):
        if k is None:
            return e_ref.at[h * per_half + j]
        return e_ref.at[h * per_half + j, :, chunk_cols(k)]

    def e_far(j, k=None):
        unit = j if k is None else j + k
        return copy(e_mine(1 - half, j, k), e_part(j, me, k), e_send.at[1, unit], e_recv.at[unit, me], z_far, core)

    def e_near(j, k=None):
        unit = j if k is None else j + k
        return copy(e_mine(half, j, k), e_part(j, me, k), e_send.at[0, unit], e_recv.at[unit, me], z_in, core)

    def near_e(j):
        return copy(e_mine(half, j, None), ebuf.at[j, me], n_send.at[j], e_recv.at[j, me], z_in, other)

    def own_e(j):
        return pltpu.make_async_copy(e_mine(half, j, None), ebuf.at[j, me], el_sem.at[j])

    away = (z_out, z_far, z_end)

    def pass_e(j, n, k=None):
        unit = j if k is None else j + k
        block = away[n] * CORES + core
        spot = e_part(j, block, k)
        return copy(spot, spot, h_send.at[unit, n], e_recv.at[unit, block], z_in, other)

    def take_e(j, k=None):
        unit = j if k is None else j + k
        for n in range(3):
            block = away[n] * CORES + core
            arrived(e_part(j, block, k), e_recv.at[unit, block])
            pass_e(j, n, k).start()

    def have_own(j):
        own_e(j).wait()
        beside = z_in * CORES + other
        arrived(ebuf.at[j, beside], e_recv.at[j, beside])

    def have_e(j, k=None):
        unit = j if k is None else j + k
        for chip in away:
            block = chip * CORES + other
            arrived(e_part(j, block, k), e_recv.at[unit, block])

    def all_units(act):
        for j in range(last):
            act(j, None)
        for k in range(CHUNKS):
            act(last, k)

    def partial_copy(j):
        return copy(pbuf.at[j], qbuf.at[j], p_send.at[j], p_recv.at[j], z_in, other)

    def project(q, j, base, many):
        at = pl.ds(pl.multiple_of(q * quarter, 16), quarter)
        blocks = pl.ds(base, many)
        left = wbuf[blocks, at].reshape(many * quarter, features)
        right = ebuf[j].reshape(rows, features)
        zt[j, blocks, at] = lax.dot_general(
            left, right, NT, preferred_element_type=jnp.float32
        ).astype(jnp.bfloat16).reshape(many, quarter, rows)

    def project_last(k):
        cols = chunk_cols(k)
        left = wbuf[:, :, cols].reshape(side * held, chunk_width)
        right = ebuf[last, :, :, cols].reshape(rows, chunk_width)
        total = lax.dot_general(
            left, right, NT, preferred_element_type=jnp.float32
        ).reshape(side, held, rows)
        zsum[...] = jnp.where(k > 0, zsum[...], 0.0) + total

    def settle_last():
        zt[last] = zsum[...].astype(jnp.bfloat16)

    lanes = pl.ds(pl.multiple_of(core * span, 128), span)
    mine_at = pl.multiple_of(core * half_rows, half_rows)
    theirs_at = pl.multiple_of(other * half_rows, half_rows)

    def score(j):
        left = ebuf[j, :, :, lanes].reshape(rows, span)
        raw = jnp.dot(left, zt[j].reshape(span, rows), preferred_element_type=jnp.float32)
        sbuf[...] = raw - jnp.transpose(raw)
        pbuf[j] = sbuf[pl.ds(theirs_at, half_rows)]
        partial_copy(j).start()
        keep[j] = sbuf[pl.ds(mine_at, half_rows)]

    def final_copy(j, t):
        row = pl.multiple_of(t * block_rows, block_rows)
        return pltpu.make_async_remote_copy(
            fbuf.at[j, pl.ds(row, block_rows)], rbuf.at[half * per_half + j],
            r_send.at[j, t], r_recv.at[half * per_half + j],
            device_id=(part, core * side + t), device_id_type=MESH,
        )

    def each_target(j, act):
        for t in range(side):
            @pl.when(core * side + t != me)
            def _():
                act(final_copy(j, t))

    def finish(j):
        arrived(qbuf.at[j], p_recv.at[j])
        fbuf[j] = (keep[j] + qbuf[j]).astype(jnp.bfloat16)
        each_target(j, lambda c: c.start())

        @pl.when(near)
        def _():
            row = pl.multiple_of(here * block_rows, block_rows)
            rbuf[half * per_half + j] = fbuf[j, pl.ds(row, block_rows)]

    def each_mask():
        for d in range(group - 1):
            mask_copy(d).start()

    def settle():
        def sent(j, k):
            e_far(j, k).wait_send()
            for n in range(3):
                pass_e(j, n, k).wait_send()

        all_units(sent)
        for j in range(per_half):
            near_e(j).wait_send()
            partial_copy(j).wait_send()
            each_target(j, lambda c: c.wait_send())
        for i in range(len(pieces)):
            far_w(i).wait_send()

    def loop(n, body):
        def run(j, carry):
            body(j)
            return carry
        lax.fori_loop(0, n, run, 0)

    def choose(index, values):
        picked = values[0]
        for n in range(1, len(values)):
            picked = jnp.where(index == n, values[n], picked)
        return picked

    @pl.when(inner)
    def _():
        @pl.when(near)
        def _():
            own_g().start()
            own_w().start()
        for j in range(per_half):
            own_e(j).start()

    folded = pl.ds(jnp.where(near, second, first), 2)
    away_cols = pl.ds(pl.multiple_of(jnp.where(near, z_out, 3 - z_out) * chip_width, 128), chip_width)
    wbuf[folded, :, away_cols] = jnp.zeros((2, held, chip_width), jnp.bfloat16)
    m_copy.wait()
    valid = m_ref[...].astype(jnp.float32)
    mine[...] = jnp.broadcast_to(jnp.sum(m_ref[...], axis=1, keepdims=True), mine.shape)
    pl.semaphore_wait(barrier, len(others) + 2)

    @pl.when(jnp.logical_not(inner))
    def _():
        for i in range(len(pieces)):
            outer_w(i).start()
        each_mask()
        for i in range(DIRECT):
            outer_diag(i).start()

        def send(j, k):
            e_near(j, k).start()
            e_far(j, k).start()

        all_units(send)

    def relays(base, cols, i):
        for u in range(2):
            for q in (x_part, y_part):
                got_w(base + u, q, i, cols)
            relay(base + u, u, i, cols).start()

    @pl.when(jnp.logical_and(inner, near))
    def _():
        for i in range(len(pieces)):
            far_w(i).start()
        each_mask()
        for j in range(per_half):
            near_e(j).start()
        own_g().wait()
        arrived(gbuf.at[other], g_recv.at[0])
        for i in range(len(pieces)):
            for u in range(2):
                got_w(first + u, part, i)
            fold(part, *pieces[i])
            for u in range(2):
                to_far(first + u, i).start()
                to_x(first + u, i).start()
                to_y(first + u, i).start()
        all_units(lambda j, k: e_far(j, k).start())
        own_w().wait()
        for q in range(PARTS):
            at = pl.ds(q * quarter, quarter)
            beside = second + other
            arrived(wbuf.at[beside, at, kept_cols(half)], w_recv.at[beside, q, 0])
        for i in range(len(pieces)):
            if i >= DIRECT:
                relays(first, every, i)
            for u in range(2):
                if i < DIRECT:
                    got_w(first + u, x_part, i)
                    got_w(first + u, y_part, i)

        def turn(t):
            j = t // PARTS
            s = t % PARTS

            @pl.when(s == 0)
            def _():
                take_e(j)
                have_own(j)
                have_e(j)

            @pl.when(t == PARTS - 1)
            def _():
                for i in range(len(pieces)):
                    for u in range(2):
                        got_w(first + u, d_part, i)
                fold(d_part, 0, pieces[DIRECT][0])

            @pl.when(t == last * PARTS - 1)
            def _():
                take_e(last, 0)
            project(choose(s, (part, x_part, y_part, d_part)), j, 0, side)

            @pl.when(s == PARTS - 1)
            def _():
                score(j)

        loop(last * PARTS, turn)
        have_own(last)

        def final_turn(k):
            @pl.when(k < CHUNKS - 1)
            def _():
                take_e(last, k + 1)

            @pl.when(k == CHUNKS - 1)
            def _():
                loop(last, finish)
            have_e(last, k)
            project_last(k)

        loop(CHUNKS, final_turn)
        settle_last()
        score(last)
        finish(last)

    @pl.when(jnp.logical_and(inner, jnp.logical_not(near)))
    def _():
        near_g().start()
        for i in range(len(pieces)):
            far_w(i).start()
        each_mask()
        for i in range(PARTS):
            near_w(i).start()
        for j in range(per_half):
            near_e(j).start()
        for base, cols in passed:
            for i in range(len(pieces)):
                for u in range(2):
                    got_w(base + u, part, i, cols)
                    to_x(base + u, i, cols).start()
                    to_y(base + u, i, cols).start()
        all_units(lambda j, k: e_far(j, k).start())

        def got_diag(base, cols):
            for i in range(len(pieces)):
                for u in range(2):
                    got_w(base + u, d_part, i, cols)

        for i in range(len(pieces)):
            relays(*passed[0], i)
        take_e(0)
        have_own(0)
        have_e(0)
        order = ((0, 0), (1, 0), (2, 0), (0, 1), (1, 1), (2, 1), (0, 2), (1, 2), (2, 2), (3, 0), (3, 1), (3, 2))

        def turn(t):
            what = choose(t, [q * PARTS + j for q, j in order])
            j = what % PARTS

            @pl.when(t == 1)
            def _():
                for i in range(len(pieces)):
                    if i == len(pieces) - 1:
                        take_e(1)
                    relays(*passed[1], i)

            @pl.when(t == 3)
            def _():
                have_own(1)
                have_e(1)

            @pl.when(t == 6)
            def _():
                take_e(2)
                have_own(2)
                have_e(2)

            @pl.when(t == 9)
            def _():
                take_e(last, 0)
                for base, cols in passed:
                    got_diag(base, cols)
            project(choose(what // PARTS, (part, x_part, y_part, d_part)), j, 0, side)

        loop(len(order), turn)
        have_own(last)
        have_e(last, 0)
        loop(last, score)
        take_e(last, 1)
        loop(last, finish)

        def final_turn(k):
            @pl.when(k > 0)
            def _():
                have_e(last, k)
            project_last(k)

        loop(CHUNKS, final_turn)
        settle_last()
        score(last)
        finish(last)

    for d in range(group - 1):
        arrived(mbuf.at[others[d]], m_recv.at[others[d]])
    mbuf[me] = mine[...]
    counts = mbuf[0]
    for g in range(1, group):
        counts = counts + mbuf[g]
    counts = counts[:, :1].astype(jnp.float32)
    slot = lax.broadcasted_iota(jnp.int32, (prompts, rows), 1).astype(jnp.float32)
    cols = (slot < counts).astype(jnp.float32)
    pairs = jnp.maximum(counts - 1.0, 1.0)
    same = lax.broadcasted_iota(jnp.int32, (block_rows, block_rows), 0)
    same = (same == lax.broadcasted_iota(jnp.int32, (block_rows, block_rows), 1)).astype(jnp.float32)
    down = lax.dot_general(same, valid, NT, preferred_element_type=jnp.float32)
    lane = lax.broadcasted_iota(jnp.int32, (block_rows, 128), 1)
    rates = jnp.zeros((block_rows, 128), jnp.float32)
    for batch in (range(last), range(last, per_half)):
        for j in batch:
            for h in range(2):
                @pl.when(jnp.logical_not(jnp.logical_and(jnp.logical_and(inner, near), half == h)))
                def _():
                    arrived(rbuf.at[h * per_half + j], r_recv.at[h * per_half + j])
        for j in batch:
            for h in range(2):
                p = h * per_half + j
                given = down[:, p:p + 1]
                prefs = jax.nn.sigmoid(rbuf[p].astype(jnp.float32)) * given * cols[p:p + 1, :]
                o_ref[p] = prefs
                totals = jnp.sum(prefs, axis=1, keepdims=True) - 0.5 * given
                rates = jnp.where(lane == p, given * totals / pairs[p:p + 1, :], rates)
    r_ref[...] = jnp.transpose(rates)[:prompts]

    for d in range(group - 1):
        mask_copy(d).wait_send()

    @pl.when(jnp.logical_not(inner))
    def _():
        for i in range(len(pieces)):
            outer_w(i).wait_send()
        for i in range(DIRECT):
            outer_diag(i).wait_send()

        def left(j, k):
            e_far(j, k).wait_send()
            e_near(j, k).wait_send()

        all_units(left)

    @pl.when(inner)
    def _():
        settle()

    @pl.when(jnp.logical_and(inner, near))
    def _():
        for i in range(len(pieces)):
            for u in range(2):
                to_x(first + u, i).wait_send()
                to_y(first + u, i).wait_send()
                to_far(first + u, i).wait_send()
                if i >= DIRECT:
                    relay(first + u, u, i).wait_send()

    @pl.when(jnp.logical_and(inner, jnp.logical_not(near)))
    def _():
        near_g().wait_send()
        for i in range(PARTS):
            near_w(i).wait_send()
        for i in range(len(pieces)):
            for base, cols in passed:
                for u in range(2):
                    to_x(base + u, i, cols).wait_send()
                    to_y(base + u, i, cols).wait_send()
                    relay(base + u, u, i, cols).wait_send()


def line_scores(embeddings, head_weight, mask):
    prompts, block_rows, features = embeddings.shape
    held = head_weight.shape[0]
    group = CHIPS * CORES
    side = group // 2
    per_half = prompts // 2
    rows = group * block_rows
    half_rows = rows // 2
    quarter = held // PARTS
    units = per_half - 1 + CHUNKS
    bf16, f32 = jnp.bfloat16, jnp.float32
    dma = pltpu.SemaphoreType.DMA
    held_in = pl.BlockSpec(memory_space=pltpu.HBM)
    vmem = pl.BlockSpec(memory_space=pltpu.VMEM)
    return pl.pallas_call(
        kernel,
        out_shape=(
            jax.ShapeDtypeStruct((prompts, block_rows, rows), f32),
            jax.ShapeDtypeStruct((prompts, block_rows), f32),
        ),
        in_specs=[held_in, held_in, held_in],
        out_specs=(vmem, vmem),
        scratch_shapes=[
            pltpu.VMEM((prompts, block_rows), jnp.int32),
            pltpu.VMEM((per_half, group, block_rows, features), bf16),
            pltpu.VMEM((side, held, features), bf16),
            pltpu.VMEM((CORES, held, features // CHIPS), bf16),
            pltpu.VMEM((per_half, side, held, rows), bf16),
            pltpu.VMEM((side, held, rows), f32),
            pltpu.VMEM((rows, rows), f32),
            pltpu.VMEM((per_half, half_rows, rows), f32),
            pltpu.VMEM((per_half, half_rows, rows), f32),
            pltpu.VMEM((per_half, half_rows, rows), f32),
            pltpu.VMEM((per_half, half_rows, rows), bf16),
            pltpu.VMEM((prompts, block_rows, rows), bf16),
            pltpu.VMEM((prompts, 128), jnp.int32),
            pltpu.VMEM((group, prompts, 128), jnp.int32),
            dma((1,)),
            dma((group - 1,)),
            dma((group,)),
            dma((2, units)),
            dma((units, group)),
            dma((per_half,)),
            dma((units, 3)),
            dma((per_half,)),
            dma((4,)),
            dma((4,)),
            dma((PARTS + 1,)),
            dma((2,)),
            dma((1,)),
            dma((side, 4)),
            dma((side, 4)),
            dma((side, 4)),
            dma((side, 4)),
            dma((side, PARTS, 4)),
            dma((per_half,)),
            dma((per_half,)),
            dma((per_half, side)),
            dma((prompts,)),
        ],
        compiler_params=pltpu.CompilerParams(
            collective_id=0, has_side_effects=True, vmem_limit_bytes=53 << 20
        ),
    )(embeddings, head_weight, mask)


def shards(embeddings, head_weight, valid_mask):
    group_size = lax.axis_size("resp")
    slots = group_size * embeddings.shape[1]
    if (lax.axis_size("prompt"), group_size) == (PARTS, CHIPS * CORES):
        return line_scores(embeddings, head_weight, valid_mask)
    valid_rows = valid_mask.astype(jnp.float32)
    counts = lax.psum(jnp.sum(valid_rows, axis=1), "resp")
    scores = gathered_scores(embeddings, head_weight)
    column_ids = jnp.arange(slots, dtype=jnp.float32)
    valid_cols = (column_ids[None, :] < counts[:, None]).astype(jnp.float32)
    preferences = jax.nn.sigmoid(scores) * valid_rows[:, :, None] * valid_cols[:, None, :]
    totals = jnp.sum(preferences, axis=2) - 0.5 * valid_rows
    win_rates = valid_rows * totals / jnp.maximum(counts - 1.0, 1.0)[:, None]
    return (preferences, win_rates)


def solution(mesh):
    return jax.shard_map(
        shards,
        mesh=mesh,
        in_specs=(P("prompt", "resp", None), P("resp", None), P("prompt", "resp")),
        out_specs=(P("prompt", "resp", None), P("prompt", "resp")),
        check_vma=False,
    )
```

```python
import functools

import jax
import jax.numpy as jnp
from jax import lax
from jax.experimental import pallas as pl
from jax.experimental.pallas import tpu as pltpu
from jax.sharding import PartitionSpec as P

MESH = pl.DeviceIdType.MESH
CORES = 2
CHIPS = 4
PARTS = 4
CHUNKS = 2
DIRECT = 3
NT = (((1,), (1,)), ((), ()))


def gathered_halves(embeddings, head_weight, own_index, group_size):
    prompts, block_rows, features = embeddings.shape
    held = head_weight.shape[0]
    slots = group_size * block_rows
    everyone = lax.all_gather(embeddings, "resp", axis=0, tiled=True)
    flat = everyone.reshape(group_size * prompts * block_rows, features)
    through = lax.dot_general(flat, head_weight, NT, preferred_element_type=jnp.float32)
    through = through.astype(jnp.bfloat16).reshape(group_size, prompts, block_rows, held)
    mine = lax.dynamic_slice_in_dim(
        everyone.reshape(group_size, prompts, block_rows, features), own_index * held, held, 3
    )
    partial = jnp.einsum("gpid,hpjd->gpihj", mine, through, preferred_element_type=jnp.float32)
    flipped = jnp.einsum("gpid,hpjd->gpihj", through, mine, preferred_element_type=jnp.float32)
    partial = (partial - flipped).astype(jnp.bfloat16)
    return partial.reshape(group_size, prompts, block_rows, slots)


def gathered_scores(embeddings, head_weight):
    group_size = lax.axis_size("resp")
    own_index = lax.axis_index("resp")
    prompts, block_rows, features = embeddings.shape
    slots = group_size * block_rows
    at_once = max(1, min(prompts, (1 << 11) // slots))

    def scores_of(some):
        partial = gathered_halves(some, head_weight, own_index, group_size)
        swapped = lax.all_to_all(partial, "resp", split_axis=0, concat_axis=0, tiled=True)
        return jnp.sum(swapped.astype(jnp.float32), axis=0)

    pieces = embeddings.reshape(prompts // at_once, at_once, block_rows, features)
    return lax.map(scores_of, pieces).reshape(prompts, block_rows, slots)


def kernel(e_ref, w_ref, m_hbm, o_ref, r_ref,
           m_ref, ebuf, wbuf, gbuf, cbuf, zt, zsum, sbuf, keep, pbuf, qbuf, fbuf, rbuf, mine, mbuf,
           m_sems, e_send, e_recv, h_recv, n_sems, h_send, o_send, l_sems, g_send, g_recv,
           x_send, y_send, u_send, v_send, a_recv, b_recv, d_recv, p_send, p_recv, r_send, r_recv):
    part = lax.axis_index("prompt")
    me = lax.axis_index("resp")
    z = me // CORES
    core = me % CORES
    half = z // 2
    prompts, block_rows, features = e_ref.shape
    held = w_ref.shape[0]
    group = CHIPS * CORES
    per_half = prompts // 2
    side = group // 2
    span = held * side
    rows = group * block_rows
    half_rows = rows // 2
    quarter = held // PARTS
    z_in = 1 + half
    z_out = 3 * half
    z_far = 2 - half
    z_end = 3 - z_out
    inner = z == z_in
    near = core == half
    other = 1 - core
    here = me % side
    x_part = part + 1 - 2 * (part % 2)
    y_part = lax.rem(part + 2, PARTS)
    d_part = PARTS - 1 - part
    chip_width = features // CHIPS
    chunk_width = features // CHUNKS
    cut = held // 128 * 128
    spare = held - cut
    wide = chip_width - cut
    step = quarter // 7
    last = per_half - 1
    pieces = ((0, step), (step, 2 * step), (3 * step, 2 * step), (5 * step, 2 * step))
    count = len(pieces)
    direct = pieces[DIRECT][0]

    def copy(src, dst, send, recv, chip, c, q=None):
        return pltpu.make_async_remote_copy(
            src, dst, send, recv,
            device_id=(part if q is None else q, chip * CORES + c), device_id_type=MESH,
        )

    def arrived(dst, recv):
        copy(dst, dst, m_sems.at[0], recv, z_far, core).wait_recv()

    def departed(src, send):
        copy(src, src, send, m_sems.at[1], z_far, core).wait_send()

    m_copy = pltpu.make_async_copy(m_hbm, m_ref, m_sems.at[2])
    m_copy.start()
    others = [lax.rem(me + d, group) for d in range(1, group)]
    barrier = pltpu.get_barrier_semaphore()
    for peer in others:
        pl.semaphore_signal(barrier, inc=1, device_id=(part, peer), device_id_type=MESH)
    for q in (x_part, y_part):
        pl.semaphore_signal(barrier, inc=1, device_id=(q, me), device_id_type=MESH)

    def mask_copy(d):
        return pltpu.make_async_remote_copy(
            mine, mbuf.at[me], m_sems.at[0], m_sems.at[1],
            device_id=(part, others[d]), device_id_type=MESH,
        )

    def chip_cols(chip):
        return pl.ds(pl.multiple_of(chip * chip_width, 128), chip_width)

    def cut_cols(chip, h):
        return pl.ds(pl.multiple_of(chip * chip_width + h * wide, 128), cut)

    def weights(h, within, v):
        size = features - (chip_width if within else 0) - (cut if v else 0)
        block = 2 * ((1 - h) if within else h) + ((1 - h) if v else h)
        return block, pl.ds(pl.multiple_of((1 - h) * (features - size), 128), size)

    outer_set = tuple(weights(core, False, v) for v in range(2))
    inner_set = tuple(weights(core, True, v) for v in range(2))
    first = 2 * half
    every = pl.ds(0, features)

    def span_rows(q, i):
        at, size = pieces[i]
        return pl.ds(pl.multiple_of(q * quarter + at, 16), size)

    def outer_w(i, v):
        block, cols = weights(half, False, v)
        at = span_rows(part, i)
        dst = wbuf.at[block, at, cols]
        return copy(w_ref.at[at, cols] if v else dst, dst, o_send.at[0], a_recv.at[block, i], z_in, half)

    def outer_diag(v):
        block, cols = weights(half, False, v)
        at = pl.ds(pl.multiple_of(d_part * quarter, 16), direct)
        dst = wbuf.at[block, at, cols]
        return copy(w_ref.at[at, cols] if v else dst, dst, o_send.at[1], d_recv.at[block], z_in, half)

    def far_w(i, v):
        block, cols = weights(half, True, v)
        at = span_rows(part, i)
        dst = wbuf.at[block, at, cols]
        return copy(w_ref.at[at, cols] if v else dst, dst, o_send.at[0], a_recv.at[block, i], z_far, half)

    def near_w():
        block, cols = weights(half, True, 1)
        return copy(w_ref.at[:, cols], wbuf.at[block, :, cols], g_send.at[0], g_recv.at[2], z_in, half)

    def near_g():
        return copy(w_ref.at[:, chip_cols(z_out)], gbuf.at[core], g_send.at[1], g_recv.at[0], z_in, half)

    def near_c():
        at = pl.ds(pl.multiple_of((1 - half) * spare, 16), held)
        return copy(w_ref.at[:, cut_cols(z, half)], cbuf.at[at], g_send.at[2], g_recv.at[1], z, half)

    def own_w(within):
        block, cols = weights(half, within, 0)
        return pltpu.make_async_copy(w_ref.at[:, cols], wbuf.at[block, :, cols], l_sems.at[0])

    def own_g():
        return pltpu.make_async_copy(w_ref.at[:, chip_cols(z_out)], gbuf.at[core], l_sems.at[1])

    def fold_core():
        arrived(cbuf.at[pl.ds(0, held)], g_recv.at[1])
        row = lax.broadcasted_iota(jnp.int32, (held, cut), 0)
        col = lax.broadcasted_iota(jnp.int32, (held, cut), 1)
        pick = (row - half * spare == col).astype(jnp.bfloat16)
        turned = lax.dot_general(pick, cbuf[...], NT, preferred_element_type=jnp.float32)
        cols = pl.ds(pl.multiple_of(z * chip_width + (1 - half) * cut, 128), wide)
        wbuf[here, :, cols] = (wbuf[here, :, cols].astype(jnp.float32) - turned).astype(jnp.bfloat16)

    def fold(q, at, size):
        start = q * quarter + at
        row = lax.broadcasted_iota(jnp.int32, (2 * size, chip_width), 0)
        col = lax.broadcasted_iota(jnp.int32, (2 * size, chip_width), 1)
        pick = (start + jnp.where(row < size, row, row + held - size) == col).astype(jnp.bfloat16)
        turned = lax.dot_general(
            pick, gbuf[...].reshape(chip_width, chip_width), NT, preferred_element_type=jnp.float32
        ).reshape(2, size, chip_width)
        pair, where, cols = pl.ds(first, 2), pl.ds(pl.multiple_of(start, 16), size), chip_cols(z_in)
        wbuf[pair, where, cols] = (wbuf[pair, where, cols].astype(jnp.float32) - turned).astype(jnp.bfloat16)

    def got_mine(w, i):
        block, cols = w
        arrived(wbuf.at[block, span_rows(part, i), cols], a_recv.at[block, i])

    def got_sides(w, i):
        block, cols = w
        arrived(wbuf.at[block, pl.ds(0, 2 * pieces[i][1]), cols], b_recv.at[block, i])

    def got_diag(w):
        block, cols = w
        arrived(wbuf.at[block, pl.ds(0, quarter), cols], d_recv.at[block])

    def along(w, q, i, send, recv, chip, q_to):
        block, cols = w
        spot = wbuf.at[block, span_rows(q, i), cols]
        return copy(spot, spot, send, recv, chip, core, q_to)

    def spread(w, i):
        along(w, part, i, x_send.at[w[0]], b_recv.at[w[0], i], z_in, x_part).start()
        along(w, part, i, y_send.at[w[0]], b_recv.at[w[0], i], z_in, y_part).start()

    def to_far(w, i):
        along(w, part, i, u_send.at[w[0]], a_recv.at[w[0], i], z_far, part).start()

    def relay(w, v, i):
        got_sides(w, i)
        if (i < 2) == (v == 0):
            along(w, x_part, i, v_send.at[w[0]], d_recv.at[w[0]], z_in, y_part).start()
        else:
            along(w, y_part, i, v_send.at[w[0]], d_recv.at[w[0]], z_in, x_part).start()

    def sent_rows(w, send, many):
        block, cols = w
        departed(wbuf.at[block, pl.ds(0, many), cols], send.at[block])

    def chunk_cols(k):
        return pl.ds(pl.multiple_of(k * chunk_width, 128), chunk_width)

    def e_part(j, block, k):
        if k is None:
            return ebuf.at[j, block]
        return ebuf.at[j, block, :, chunk_cols(k)]

    def e_mine(h, j, k):
        if k is None:
            return e_ref.at[h * per_half + j]
        return e_ref.at[h * per_half + j, :, chunk_cols(k)]

    def unit(j, k):
        return j if k is None else j + k

    def e_far(j, k=None):
        return copy(e_mine(1 - half, j, k), e_part(j, me, k), e_send.at[1], e_recv.at[unit(j, k)], z_far, core)

    def e_near(j, k=None):
        return copy(e_mine(half, j, k), e_part(j, me, k), e_send.at[0], e_recv.at[unit(j, k)], z_in, core)

    def near_e(j):
        return copy(e_mine(half, j, None), ebuf.at[j, me], n_sems.at[0], n_sems.at[1], z_in, other)

    def own_e(j):
        return pltpu.make_async_copy(e_mine(half, j, None), ebuf.at[j, me], n_sems.at[2])

    away = (z_out, z_far, z_end)

    def three(j, k):
        if k is None:
            return ebuf.at[j, pl.ds(0, 3)]
        return ebuf.at[j, pl.ds(0, 3), :, chunk_cols(k)]

    def take_e(j, k=None):
        arrived(three(j, k), e_recv.at[unit(j, k)])
        for chip in away:
            spot = e_part(j, chip * CORES + core, k)
            copy(spot, spot, h_send.at[0], h_recv.at[unit(j, k)], z_in, other).start()

    def have_e(j, k=None):
        arrived(three(j, k), h_recv.at[unit(j, k)])

    def have_own():
        pltpu.make_async_copy(ebuf.at[:, me], ebuf.at[:, me], n_sems.at[2]).wait()
        arrived(ebuf.at[:, z_in * CORES + other], n_sems.at[1])

    def all_units(act):
        for j in range(last):
            act(j, None)
        for k in range(CHUNKS):
            act(last, k)

    def partial_copy(j):
        return copy(pbuf.at[j], qbuf.at[j], p_send.at[0], p_recv.at[j], z_in, other)

    def project(q, j):
        at = pl.ds(pl.multiple_of(q * quarter, 16), quarter)
        left = wbuf[:, at].reshape(side * quarter, features)
        right = ebuf[j].reshape(rows, features)
        zt[j, :, at] = lax.dot_general(
            left, right, NT, preferred_element_type=jnp.float32
        ).astype(jnp.bfloat16).reshape(side, quarter, rows)

    def project_last(q, k):
        at = pl.ds(pl.multiple_of(q * quarter, 16), quarter)
        cols = chunk_cols(k)
        left = wbuf[:, at, cols].reshape(side * quarter, chunk_width)
        right = ebuf[last, :, :, cols].reshape(rows, chunk_width)
        total = lax.dot_general(
            left, right, NT, preferred_element_type=jnp.float32
        ).reshape(side, quarter, rows)
        total = jnp.where(k > 0, zsum[:, at], 0.0) + total
        zsum[:, at] = total
        zt[last, :, at] = total.astype(jnp.bfloat16)

    lanes = pl.ds(pl.multiple_of(core * span, 128), span)
    mine_at = pl.multiple_of(core * half_rows, half_rows)
    theirs_at = pl.multiple_of(other * half_rows, half_rows)

    def score(j):
        left = ebuf[j, :, :, lanes].reshape(rows, span)
        raw = jnp.dot(left, zt[j].reshape(span, rows), preferred_element_type=jnp.float32)
        sbuf[...] = raw - jnp.transpose(raw)
        pbuf[j] = sbuf[pl.ds(theirs_at, half_rows)]
        partial_copy(j).start()
        keep[j] = sbuf[pl.ds(mine_at, half_rows)]

    def final_copy(j, t):
        row = pl.multiple_of(t * block_rows, block_rows)
        return pltpu.make_async_remote_copy(
            fbuf.at[j, pl.ds(row, block_rows)], rbuf.at[half * per_half + j],
            r_send.at[0], r_recv.at[half, j // last],
            device_id=(part, core * side + t), device_id_type=MESH,
        )

    def finish(j):
        arrived(qbuf.at[j], p_recv.at[j])
        fbuf[j] = (keep[j] + qbuf[j]).astype(jnp.bfloat16)
        for t in range(side):
            @pl.when(core * side + t != me)
            def _():
                final_copy(j, t).start()

        @pl.when(near)
        def _():
            row = pl.multiple_of(here * block_rows, block_rows)
            rbuf[half * per_half + j] = fbuf[j, pl.ds(row, block_rows)]

    def each_mask():
        for d in range(group - 1):
            mask_copy(d).start()

    def loop(n, body):
        def run(j, carry):
            body(j)
            return carry
        lax.fori_loop(0, n, run, 0)

    def choose(index, values):
        picked = values[0]
        for n in range(1, len(values)):
            picked = jnp.where(index == n, values[n], picked)
        return picked

    quarters = (part, x_part, y_part, d_part)

    @pl.when(near)
    def _():
        @pl.when(inner)
        def _():
            own_w(True).start()
            own_g().start()

        @pl.when(jnp.logical_not(inner))
        def _():
            own_w(False).start()

    @pl.when(inner)
    def _():
        for j in range(per_half):
            own_e(j).start()

    wbuf[pl.ds(inner_set[0][0] // 2 * 2, 2), :, chip_cols(3 * core)] = jnp.zeros((2, held, chip_width), jnp.bfloat16)
    wbuf[inner_set[1][0], :, cut_cols(1 + core, core)] = jnp.zeros((held, cut), jnp.bfloat16)
    wbuf[outer_set[1][0], :, cut_cols(3 * core, core)] = jnp.zeros((held, cut), jnp.bfloat16)
    cbuf[pl.ds(pl.multiple_of(half * held, 16), spare)] = jnp.zeros((spare, cut), jnp.bfloat16)
    m_copy.wait()
    valid = m_ref[...].astype(jnp.float32)
    mine[...] = jnp.broadcast_to(jnp.sum(m_ref[...], axis=1, keepdims=True), mine.shape)
    pl.semaphore_wait(barrier, len(others) + 2)

    for v in range(2):
        @pl.when(jnp.logical_and(jnp.logical_not(inner), near == (v == 0)))
        def _():
            if v:
                near_c().start()
            else:
                own_w(False).wait()
                fold_core()
            for i in range(count):
                outer_w(i, v).start()
            each_mask()
            outer_diag(v).start()

            def send(j, k):
                e_near(j, k).start()
                e_far(j, k).start()

            all_units(send)

    @pl.when(jnp.logical_and(inner, near))
    def _():
        own_w(True).wait()
        fold_core()
        for i in range(count):
            far_w(i, 0).start()
        each_mask()
        for j in range(per_half):
            near_e(j).start()
        own_g().wait()
        arrived(gbuf.at[other], g_recv.at[0])
        for i in range(count):
            for w in outer_set:
                got_mine(w, i)
            fold(part, *pieces[i])
            for w in outer_set:
                to_far(w, i)
                spread(w, i)
        all_units(lambda j, k: e_far(j, k).start())
        block, cols = weights(half, True, 1)
        arrived(wbuf.at[block, :, cols], g_recv.at[2])
        have_own()
        for i in range(count):
            for v in range(2):
                if i < DIRECT:
                    got_sides(outer_set[v], i)
                else:
                    relay(outer_set[v], v, i)

        def turn(t):
            j = t // PARTS
            s = t % PARTS

            @pl.when(s == 0)
            def _():
                take_e(j)
                have_e(j)

            @pl.when(t == PARTS - 1)
            def _():
                for w in outer_set:
                    got_diag(w)
                fold(d_part, 0, direct)

            @pl.when(t == last * PARTS - 3)
            def _():
                take_e(last, 0)
            project(choose(s, quarters), j)

            @pl.when(s == PARTS - 1)
            def _():
                score(j)

        loop(last * PARTS, turn)

        def final_turn(n):
            k = n // PARTS
            s = n % PARTS

            @pl.when(s == 0)
            def _():
                @pl.when(k < CHUNKS - 1)
                def _():
                    take_e(last, k + 1)

                have_e(last, k)
            project_last(choose(s, quarters), k)

        loop(CHUNKS * PARTS, final_turn)
        loop(last, finish)
        score(last)
        finish(last)

    @pl.when(jnp.logical_and(inner, jnp.logical_not(near)))
    def _():
        near_c().start()
        near_g().start()
        for i in range(count):
            far_w(i, 1).start()
        each_mask()
        near_w().start()
        for j in range(per_half):
            near_e(j).start()
        for pair in (inner_set, outer_set):
            for i in range(count):
                for w in pair:
                    got_mine(w, i)
                    spread(w, i)
        all_units(lambda j, k: e_far(j, k).start())
        for i in range(count):
            for v in range(2):
                relay(inner_set[v], v, i)
        have_own()
        take_e(0)
        have_e(0)
        order = ((0, 0), (1, 0), (2, 0), (0, 1), (1, 1), (2, 1), (0, 2), (1, 2), (2, 2), (3, 0), (3, 1), (3, 2))

        def turn(t):
            what = choose(t, [q * PARTS + j for q, j in order])

            @pl.when(t == 1)
            def _():
                for i in range(count):
                    if i == count - 1:
                        take_e(1)
                    for v in range(2):
                        relay(outer_set[v], v, i)

            @pl.when(t == 3)
            def _():
                have_e(1)

            @pl.when(t == 6)
            def _():
                take_e(2)
                have_e(2)

            @pl.when(t == 9)
            def _():
                take_e(last, 0)
                for w in inner_set + outer_set:
                    got_diag(w)
            project(choose(what // PARTS, quarters), what % PARTS)

        loop(len(order), turn)
        have_e(last, 0)

        def final_turn(n):
            @pl.when(n == PARTS)
            def _():
                take_e(last, 1)
                loop(last, score)
                loop(last, finish)
                have_e(last, 1)
            project_last(choose(n % PARTS, quarters), n // PARTS)

        loop(CHUNKS * PARTS, final_turn)
        score(last)
        finish(last)

    arrived(mbuf.at[pl.ds(0, group - 1)], m_sems.at[1])
    mbuf[me] = mine[...]
    counts = mbuf[0]
    for g in range(1, group):
        counts = counts + mbuf[g]
    counts = counts[:, :1].astype(jnp.float32)
    slot = lax.broadcasted_iota(jnp.int32, (prompts, rows), 1).astype(jnp.float32)
    cols = (slot < counts).astype(jnp.float32)
    pairs = jnp.maximum(counts - 1.0, 1.0)
    same = lax.broadcasted_iota(jnp.int32, (block_rows, block_rows), 0)
    same = (same == lax.broadcasted_iota(jnp.int32, (block_rows, block_rows), 1)).astype(jnp.float32)
    down = lax.dot_general(same, valid, NT, preferred_element_type=jnp.float32)
    lane = lax.broadcasted_iota(jnp.int32, (block_rows, 128), 1)
    rates = jnp.zeros((block_rows, 128), jnp.float32)
    for batch in (range(last), range(last, per_half)):
        for h in range(2):
            @pl.when(jnp.logical_not(jnp.logical_and(jnp.logical_and(inner, near), half == h)))
            def _():
                arrived(rbuf.at[pl.ds(h * per_half + batch[0], len(batch))], r_recv.at[h, batch[0] // last])
        for j in batch:
            for h in range(2):
                p = h * per_half + j
                given = down[:, p:p + 1]
                prefs = jax.nn.sigmoid(rbuf[p].astype(jnp.float32)) * given * cols[p:p + 1, :]
                o_ref[p] = prefs
                totals = jnp.sum(prefs, axis=1, keepdims=True) - 0.5 * given
                rates = jnp.where(lane == p, given * totals / pairs[p:p + 1, :], rates)
    r_ref[...] = jnp.transpose(rates)[:prompts]

    departed(mbuf.at[pl.ds(0, group - 1)], m_sems.at[0])
    departed(ebuf.at[:, 0], e_send.at[1])
    for v in range(2):
        @pl.when(near == (v == 0))
        def _():
            @pl.when(inner)
            def _():
                block, cols = weights(half, True, v)
                departed(wbuf.at[block, pl.ds(0, quarter), cols], o_send.at[0])

            @pl.when(jnp.logical_not(inner))
            def _():
                block, cols = weights(half, False, v)
                departed(wbuf.at[block, pl.ds(0, quarter), cols], o_send.at[0])
                departed(wbuf.at[block, pl.ds(0, direct), cols], o_send.at[1])

    @pl.when(jnp.logical_not(near))
    def _():
        near_c().wait_send()

    @pl.when(jnp.logical_not(inner))
    def _():
        departed(ebuf.at[:, 0], e_send.at[0])

    @pl.when(inner)
    def _():
        departed(ebuf.at[:, 0], n_sems.at[0])
        departed(ebuf.at[:, pl.ds(0, 3)], h_send.at[0])
        departed(pbuf, p_send.at[0])

    @pl.when(jnp.logical_and(inner, near))
    def _():
        for w in outer_set:
            for sems in (x_send, y_send, u_send):
                sent_rows(w, sems, quarter)
            sent_rows(w, v_send, quarter - direct)
        departed(fbuf.at[:, pl.ds(0, half_rows - block_rows)], r_send.at[0])

    @pl.when(jnp.logical_and(inner, jnp.logical_not(near)))
    def _():
        near_g().wait_send()
        near_w().wait_send()
        for w in inner_set + outer_set:
            for sems in (x_send, y_send, v_send):
                sent_rows(w, sems, quarter)
        departed(fbuf, r_send.at[0])


def line_scores(embeddings, head_weight, mask):
    prompts, block_rows, features = embeddings.shape
    held = head_weight.shape[0]
    group = CHIPS * CORES
    side = group // 2
    per_half = prompts // 2
    rows = group * block_rows
    half_rows = rows // 2
    units = per_half - 1 + CHUNKS
    chip_width = features // CHIPS
    cut = held // 128 * 128
    bf16, f32 = jnp.bfloat16, jnp.float32
    dma = pltpu.SemaphoreType.DMA
    held_in = pl.BlockSpec(memory_space=pltpu.HBM)
    vmem = pl.BlockSpec(memory_space=pltpu.VMEM)
    return pl.pallas_call(
        kernel,
        out_shape=(
            jax.ShapeDtypeStruct((prompts, block_rows, rows), f32),
            jax.ShapeDtypeStruct((prompts, block_rows), f32),
        ),
        in_specs=[held_in, held_in, held_in],
        out_specs=(vmem, vmem),
        scratch_shapes=[
            pltpu.VMEM((prompts, block_rows), jnp.int32),
            pltpu.VMEM((per_half, group, block_rows, features), bf16),
            pltpu.VMEM((side, held, features), bf16),
            pltpu.VMEM((CORES, held, chip_width), bf16),
            pltpu.VMEM((chip_width - cut, cut), bf16),
            pltpu.VMEM((per_half, side, held, rows), bf16),
            pltpu.VMEM((side, held, rows), f32),
            pltpu.VMEM((rows, rows), f32),
            pltpu.VMEM((per_half, half_rows, rows), f32),
            pltpu.VMEM((per_half, half_rows, rows), f32),
            pltpu.VMEM((per_half, half_rows, rows), f32),
            pltpu.VMEM((per_half, half_rows, rows), bf16),
            pltpu.VMEM((prompts, block_rows, rows), bf16),
            pltpu.VMEM((prompts, 128), jnp.int32),
            pltpu.VMEM((group, prompts, 128), jnp.int32),
            dma((3,)),
            dma((2,)),
            dma((units,)),
            dma((units,)),
            dma((3,)),
            dma((1,)),
            dma((2,)),
            dma((2,)),
            dma((3,)),
            dma((3,)),
            dma((side,)),
            dma((side,)),
            dma((side,)),
            dma((side,)),
            dma((side, 4)),
            dma((side, 4)),
            dma((side,)),
            dma((1,)),
            dma((per_half,)),
            dma((1,)),
            dma((2, 2)),
        ],
        compiler_params=pltpu.CompilerParams(
            collective_id=0, has_side_effects=True, vmem_limit_bytes=53 << 20
        ),
    )(embeddings, head_weight, mask)


def shards(embeddings, head_weight, valid_mask):
    group_size = lax.axis_size("resp")
    slots = group_size * embeddings.shape[1]
    if (lax.axis_size("prompt"), group_size) == (PARTS, CHIPS * CORES):
        return line_scores(embeddings, head_weight, valid_mask)
    valid_rows = valid_mask.astype(jnp.float32)
    counts = lax.psum(jnp.sum(valid_rows, axis=1), "resp")
    scores = gathered_scores(embeddings, head_weight)
    column_ids = jnp.arange(slots, dtype=jnp.float32)
    valid_cols = (column_ids[None, :] < counts[:, None]).astype(jnp.float32)
    preferences = jax.nn.sigmoid(scores) * valid_rows[:, :, None] * valid_cols[:, None, :]
    totals = jnp.sum(preferences, axis=2) - 0.5 * valid_rows
    win_rates = valid_rows * totals / jnp.maximum(counts - 1.0, 1.0)[:, None]
    return (preferences, win_rates)


def solution(mesh):
    return jax.shard_map(
        shards,
        mesh=mesh,
        in_specs=(P("prompt", "resp", None), P("resp", None), P("prompt", "resp")),
        out_specs=(P("prompt", "resp", None), P("prompt", "resp")),
        check_vma=False,
    )
```

```python
import functools

import jax
import jax.numpy as jnp
from jax import lax
from jax.experimental import pallas as pl
from jax.experimental.pallas import tpu as pltpu
from jax.sharding import PartitionSpec as P

MESH = pl.DeviceIdType.MESH
CORES = 2
CHIPS = 4
PARTS = 4
CHUNKS = 2
DIRECT = 3
NT = (((1,), (1,)), ((), ()))


def gathered_halves(embeddings, head_weight, own_index, group_size):
    prompts, block_rows, features = embeddings.shape
    held = head_weight.shape[0]
    slots = group_size * block_rows
    everyone = lax.all_gather(embeddings, "resp", axis=0, tiled=True)
    flat = everyone.reshape(group_size * prompts * block_rows, features)
    through = lax.dot_general(flat, head_weight, NT, preferred_element_type=jnp.float32)
    through = through.astype(jnp.bfloat16).reshape(group_size, prompts, block_rows, held)
    mine = lax.dynamic_slice_in_dim(
        everyone.reshape(group_size, prompts, block_rows, features), own_index * held, held, 3
    )
    partial = jnp.einsum("gpid,hpjd->gpihj", mine, through, preferred_element_type=jnp.float32)
    flipped = jnp.einsum("gpid,hpjd->gpihj", through, mine, preferred_element_type=jnp.float32)
    partial = (partial - flipped).astype(jnp.bfloat16)
    return partial.reshape(group_size, prompts, block_rows, slots)


def gathered_scores(embeddings, head_weight):
    group_size = lax.axis_size("resp")
    own_index = lax.axis_index("resp")
    prompts, block_rows, features = embeddings.shape
    slots = group_size * block_rows
    at_once = max(1, min(prompts, (1 << 11) // slots))

    def scores_of(some):
        partial = gathered_halves(some, head_weight, own_index, group_size)
        swapped = lax.all_to_all(partial, "resp", split_axis=0, concat_axis=0, tiled=True)
        return jnp.sum(swapped.astype(jnp.float32), axis=0)

    pieces = embeddings.reshape(prompts // at_once, at_once, block_rows, features)
    return lax.map(scores_of, pieces).reshape(prompts, block_rows, slots)


def kernel(e_ref, w_ref, m_hbm, o_ref, r_ref,
           m_ref, ebuf, wbuf, gbuf, cbuf, zt, zfar, zsum, held_raw, sbuf, keep, pbuf, qbuf, fbuf, tbuf, rbuf, mine, mbuf,
           m_sems, e_send, e_recv, h_recv, n_sems, h_send, o_send, l_sems, g_send, g_recv,
           x_send, y_send, u_send, v_send, a_recv, b_recv, d_recv, z_send, z_recv, p_send, p_recv, r_send, r_recv):
    part = lax.axis_index("prompt")
    me = lax.axis_index("resp")
    z = me // CORES
    core = me % CORES
    half = z // 2
    prompts, block_rows, features = e_ref.shape
    held = w_ref.shape[0]
    group = CHIPS * CORES
    per_half = prompts // 2
    side = group // 2
    span = held * side
    rows = group * block_rows
    half_rows = rows // 2
    quarter = held // PARTS
    z_in = 1 + half
    z_out = 3 * half
    z_far = 2 - half
    z_end = 3 - z_out
    inner = z == z_in
    near = core == half
    other = 1 - core
    here = me % side
    x_part = part + 1 - 2 * (part % 2)
    y_part = lax.rem(part + 2, PARTS)
    d_part = PARTS - 1 - part
    chip_width = features // CHIPS
    tiles = features // 256
    ends = [tiles * (CHUNKS - k) // CHUNKS * 256 for k in range(CHUNKS)]
    chunks = [(features - end, end - after) for end, after in zip(ends, ends[1:] + [0])]
    cut = held // 128 * 128
    spare = held - cut
    wide = chip_width - cut
    step = quarter // 7
    last = per_half - 1
    pieces = ((0, step), (step, 2 * step), (3 * step, 2 * step), (5 * step, 2 * step))
    count = len(pieces)
    direct = pieces[DIRECT][0]

    def copy(src, dst, send, recv, chip, c, q=None):
        return pltpu.make_async_remote_copy(
            src, dst, send, recv,
            device_id=(part if q is None else q, chip * CORES + c), device_id_type=MESH,
        )

    def arrived(dst, recv):
        copy(dst, dst, m_sems.at[0], recv, z_far, core).wait_recv()

    def departed(src, send):
        copy(src, src, send, m_sems.at[1], z_far, core).wait_send()

    m_copy = pltpu.make_async_copy(m_hbm, m_ref, m_sems.at[2])
    m_copy.start()
    others = [lax.rem(me + d, group) for d in range(1, group)]
    barrier = pltpu.get_barrier_semaphore()
    for peer in others:
        pl.semaphore_signal(barrier, inc=1, device_id=(part, peer), device_id_type=MESH)
    for q in (x_part, y_part):
        pl.semaphore_signal(barrier, inc=1, device_id=(q, me), device_id_type=MESH)

    def mask_copy(d):
        return pltpu.make_async_remote_copy(
            mine, mbuf.at[me], m_sems.at[0], m_sems.at[1],
            device_id=(part, others[d]), device_id_type=MESH,
        )

    def chip_cols(chip):
        return pl.ds(pl.multiple_of(chip * chip_width, 128), chip_width)

    def cut_cols(chip, h):
        return pl.ds(pl.multiple_of(chip * chip_width + h * wide, 128), cut)

    def weights(h, within, v):
        size = features - (chip_width if within else 0) - (cut if v else 0)
        block = 2 * ((1 - h) if within else h) + ((1 - h) if v else h)
        return block, pl.ds(pl.multiple_of((1 - h) * (features - size), 128), size)

    outer_set = tuple(weights(core, False, v) for v in range(2))
    inner_set = tuple(weights(core, True, v) for v in range(2))
    first = 2 * half
    every = pl.ds(0, features)

    def span_rows(q, i):
        at, size = pieces[i]
        return pl.ds(pl.multiple_of(q * quarter + at, 16), size)

    def outer_w(i, v):
        block, cols = weights(half, False, v)
        at = span_rows(part, i)
        dst = wbuf.at[block, at, cols]
        return copy(w_ref.at[at, cols] if v else dst, dst, o_send.at[0], a_recv.at[block, i], z_in, half)

    def outer_diag(v):
        block, cols = weights(half, False, v)
        at = pl.ds(pl.multiple_of(d_part * quarter, 16), direct)
        dst = wbuf.at[block, at, cols]
        return copy(w_ref.at[at, cols] if v else dst, dst, o_send.at[1], d_recv.at[block], z_in, half)

    def far_w(i, v):
        block, cols = weights(half, True, v)
        at = span_rows(part, i)
        dst = wbuf.at[block, at, cols]
        return copy(w_ref.at[at, cols] if v else dst, dst, o_send.at[0], a_recv.at[block, i], z_far, half)

    def near_w():
        block, cols = weights(half, True, 1)
        return copy(w_ref.at[:, cols], wbuf.at[block, :, cols], g_send.at[0], g_recv.at[2], z_in, half)

    def near_g():
        return copy(w_ref.at[:, chip_cols(z_out)], gbuf.at[core], g_send.at[1], g_recv.at[0], z_in, half)

    def near_c():
        at = pl.ds(pl.multiple_of((1 - half) * spare, 16), held)
        return copy(w_ref.at[:, cut_cols(z, half)], cbuf.at[at], g_send.at[2], g_recv.at[1], z, half)

    def own_w(within):
        block, cols = weights(half, within, 0)
        return pltpu.make_async_copy(w_ref.at[:, cols], wbuf.at[block, :, cols], l_sems.at[0])

    def own_g():
        return pltpu.make_async_copy(w_ref.at[:, chip_cols(z_out)], gbuf.at[core], l_sems.at[1])

    def fold_core():
        arrived(cbuf.at[pl.ds(0, held)], g_recv.at[1])
        row = lax.broadcasted_iota(jnp.int32, (held, cut), 0)
        col = lax.broadcasted_iota(jnp.int32, (held, cut), 1)
        pick = (row - half * spare == col).astype(jnp.bfloat16)
        turned = lax.dot_general(pick, cbuf[...], NT, preferred_element_type=jnp.float32)
        cols = pl.ds(pl.multiple_of(z * chip_width + (1 - half) * cut, 128), wide)
        wbuf[here, :, cols] = (wbuf[here, :, cols].astype(jnp.float32) - turned).astype(jnp.bfloat16)

    def fold(q, at, size):
        start = q * quarter + at
        row = lax.broadcasted_iota(jnp.int32, (2 * size, chip_width), 0)
        col = lax.broadcasted_iota(jnp.int32, (2 * size, chip_width), 1)
        pick = (start + jnp.where(row < size, row, row + held - size) == col).astype(jnp.bfloat16)
        turned = lax.dot_general(
            pick, gbuf[...].reshape(chip_width, chip_width), NT, preferred_element_type=jnp.float32
        ).reshape(2, size, chip_width)
        pair, where, cols = pl.ds(first, 2), pl.ds(pl.multiple_of(start, 16), size), chip_cols(z_in)
        wbuf[pair, where, cols] = (wbuf[pair, where, cols].astype(jnp.float32) - turned).astype(jnp.bfloat16)

    def got_mine(w, i):
        block, cols = w
        arrived(wbuf.at[block, span_rows(part, i), cols], a_recv.at[block, i])

    def got_sides(w, i):
        block, cols = w
        arrived(wbuf.at[block, pl.ds(0, 2 * pieces[i][1]), cols], b_recv.at[block, i])

    def got_diag(w):
        block, cols = w
        arrived(wbuf.at[block, pl.ds(0, quarter), cols], d_recv.at[block])

    def along(w, q, i, send, recv, chip, q_to):
        block, cols = w
        spot = wbuf.at[block, span_rows(q, i), cols]
        return copy(spot, spot, send, recv, chip, core, q_to)

    def spread(w, i):
        along(w, part, i, x_send.at[w[0]], b_recv.at[w[0], i], z_in, x_part).start()
        along(w, part, i, y_send.at[w[0]], b_recv.at[w[0], i], z_in, y_part).start()

    def to_far(w, i):
        along(w, part, i, u_send.at[w[0]], a_recv.at[w[0], i], z_far, part).start()

    def relay(w, v, i):
        got_sides(w, i)
        if (i < 2) == (v == 0):
            along(w, x_part, i, v_send.at[w[0]], d_recv.at[w[0]], z_in, y_part).start()
        else:
            along(w, y_part, i, v_send.at[w[0]], d_recv.at[w[0]], z_in, x_part).start()

    def sent_rows(w, send, many):
        block, cols = w
        departed(wbuf.at[block, pl.ds(0, many), cols], send.at[block])

    def chunk_cols(k):
        return pl.ds(*chunks[k])

    def e_part(j, block, k):
        if k is None:
            return ebuf.at[j, block]
        return ebuf.at[j, block, :, chunk_cols(k)]

    def e_mine(h, j, k):
        if k is None:
            return e_ref.at[h * per_half + j]
        return e_ref.at[h * per_half + j, :, chunk_cols(k)]

    def unit(j, k):
        return j if k is None else j + k

    def e_far(j, k=None):
        recv = e_recv.at[unit(j, k), z]
        return copy(e_mine(1 - half, j, k), e_part(j, me, k), e_send.at[1], recv, z_far, core)

    def e_near(j, k=None):
        return copy(e_mine(half, j, k), e_part(j, me, k), e_send.at[0], e_recv.at[unit(j, k), z], z_in, core)

    def near_e(j):
        return copy(e_mine(half, j, None), ebuf.at[j, me], n_sems.at[0], n_sems.at[1], z_in, other)

    def own_e(j):
        return pltpu.make_async_copy(e_mine(half, j, None), ebuf.at[j, me], n_sems.at[2])

    away = (z_out, z_far, z_end)

    def three(j, k):
        if k is None:
            return ebuf.at[j, pl.ds(0, 3)]
        return ebuf.at[j, pl.ds(0, 3), :, chunk_cols(k)]

    def take_e(j, k=None):
        for chip in away:
            spot = e_part(j, chip * CORES + core, k)
            arrived(spot, e_recv.at[unit(j, k), chip])
            copy(spot, spot, h_send.at[0], h_recv.at[unit(j, k)], z_in, other).start()

    def have_e(j, k=None):
        arrived(three(j, k), h_recv.at[unit(j, k)])

    def have_own():
        pltpu.make_async_copy(ebuf.at[:, me], ebuf.at[:, me], n_sems.at[2]).wait()
        arrived(ebuf.at[:, z_in * CORES + other], n_sems.at[1])

    def all_units(act):
        for j in range(last):
            act(j, None)
        for k in range(CHUNKS):
            act(last, k)

    def partial_copy():
        return copy(pbuf, qbuf, p_send.at[0], p_recv.at[0], z_in, other)

    def far_copy(j):
        return copy(zt.at[j], zfar.at[j], z_send.at[0], z_recv.at[j], z_in, other)

    def project(q, j):
        at = pl.ds(pl.multiple_of(q * quarter, 16), quarter)
        left = wbuf[:, at].reshape(side * quarter, features)
        right = ebuf[j].reshape(rows, features)
        zt[j, :, at] = lax.dot_general(
            left, right, NT, preferred_element_type=jnp.float32
        ).astype(jnp.bfloat16).reshape(side, quarter, rows)

    def project_last(q, k):
        at = pl.ds(pl.multiple_of(q * quarter, 16), quarter)
        cols, width = chunk_cols(k), chunks[k][1]
        left = wbuf[:, at, cols].reshape(side * quarter, width)
        right = ebuf[last, :, :, cols].reshape(rows, width)
        total = lax.dot_general(
            left, right, NT, preferred_element_type=jnp.float32
        ).reshape(side, quarter, rows)
        if k > 0:
            total = zsum[:, at] + total
        if k < CHUNKS - 1:
            zsum[:, at] = total
        else:
            zt[last, :, at] = total.astype(jnp.bfloat16)

    mine_at = pl.multiple_of(core * half_rows, half_rows)
    theirs_at = pl.multiple_of(other * half_rows, half_rows)

    def raw_scores(j, c, held_zt):
        lanes = pl.ds(pl.multiple_of(c * span, 128), span)
        left = ebuf[j, :, :, lanes].reshape(rows, span)
        return jnp.dot(left, held_zt[j].reshape(span, rows), preferred_element_type=jnp.float32)

    def score_last():
        raw = raw_scores(last, core, zt)
        sbuf[...] = raw - jnp.transpose(raw)
        pbuf[...] = sbuf[pl.ds(theirs_at, half_rows)]
        partial_copy().start()
        keep[...] = sbuf[pl.ds(mine_at, half_rows)]

    def block_at(t):
        return pl.ds(pl.multiple_of(t * block_rows, block_rows), block_rows)

    def final_copy(src, j, t):
        return pltpu.make_async_remote_copy(
            src, rbuf.at[half * per_half + j], r_send.at[0], r_recv.at[half, j // last],
            device_id=(part, t), device_id_type=MESH,
        )

    def score_all(j):
        arrived(zfar.at[j], z_recv.at[j])
        raw = held_raw[j] + raw_scores(j, other, zfar)
        fbuf[j] = (raw - jnp.transpose(raw)).astype(jnp.bfloat16)
        for d in range(group - 1):
            final_copy(fbuf.at[j, block_at(others[d])], j, others[d]).start()
        rbuf[half * per_half + j] = fbuf[j, block_at(me)]

    def finish_last():
        arrived(qbuf, p_recv.at[0])
        tbuf[...] = (keep[...] + qbuf[...]).astype(jnp.bfloat16)
        for t in range(side):
            @pl.when(core * side + t != me)
            def _():
                final_copy(tbuf.at[block_at(t)], last, core * side + t).start()

        @pl.when(near)
        def _():
            rbuf[half * per_half + last] = tbuf[block_at(here)]

    def each_mask():
        for d in range(group - 1):
            mask_copy(d).start()

    def loop(n, body):
        def run(j, carry):
            body(j)
            return carry
        lax.fori_loop(0, n, run, 0)

    def choose(index, values):
        picked = values[0]
        for n in range(1, len(values)):
            picked = jnp.where(index == n, values[n], picked)
        return picked

    quarters = (part, x_part, y_part, d_part)

    @pl.when(near)
    def _():
        @pl.when(inner)
        def _():
            own_w(True).start()
            own_g().start()

        @pl.when(jnp.logical_not(inner))
        def _():
            own_w(False).start()

    @pl.when(inner)
    def _():
        for j in range(per_half):
            own_e(j).start()

    wbuf[pl.ds(inner_set[0][0] // 2 * 2, 2), :, chip_cols(3 * core)] = jnp.zeros((2, held, chip_width), jnp.bfloat16)
    wbuf[inner_set[1][0], :, cut_cols(1 + core, core)] = jnp.zeros((held, cut), jnp.bfloat16)
    wbuf[outer_set[1][0], :, cut_cols(3 * core, core)] = jnp.zeros((held, cut), jnp.bfloat16)
    cbuf[pl.ds(pl.multiple_of(half * held, 16), spare)] = jnp.zeros((spare, cut), jnp.bfloat16)
    m_copy.wait()
    valid = m_ref[...].astype(jnp.float32)
    mine[...] = jnp.broadcast_to(jnp.sum(m_ref[...], axis=1, keepdims=True), mine.shape)
    pl.semaphore_wait(barrier, len(others) + 2)

    for v in range(2):
        @pl.when(jnp.logical_and(jnp.logical_not(inner), near == (v == 0)))
        def _():
            if v:
                near_c().start()
            else:
                own_w(False).wait()
                fold_core()
            for i in range(count):
                outer_w(i, v).start()
            each_mask()
            outer_diag(v).start()

            def send(j, k):
                e_near(j, k).start()
                e_far(j, k).start()

            all_units(send)

    @pl.when(jnp.logical_and(inner, near))
    def _():
        own_w(True).wait()
        fold_core()
        for i in range(count):
            far_w(i, 0).start()
        each_mask()
        for j in range(per_half):
            near_e(j).start()
        own_g().wait()
        arrived(gbuf.at[other], g_recv.at[0])
        for i in range(count):
            for w in outer_set:
                got_mine(w, i)
            fold(part, *pieces[i])
            for w in outer_set:
                to_far(w, i)
                spread(w, i)
        all_units(lambda j, k: e_far(j, k).start())
        block, cols = weights(half, True, 1)
        arrived(wbuf.at[block, :, cols], g_recv.at[2])
        have_own()
        for i in range(count):
            for v in range(2):
                if i < DIRECT:
                    got_sides(outer_set[v], i)
                else:
                    relay(outer_set[v], v, i)

        def turn(t):
            j = t // PARTS
            s = t % PARTS

            @pl.when(s == 0)
            def _():
                take_e(j)
                have_e(j)

            @pl.when(t == PARTS - 1)
            def _():
                for w in outer_set:
                    got_diag(w)
                fold(d_part, 0, direct)

            @pl.when(t == last * PARTS - 3)
            def _():
                take_e(last, 0)
            project(choose(s, quarters), j)

            @pl.when(s == PARTS - 1)
            def _():
                held_raw[j] = raw_scores(j, core, zt)

        loop(last * PARTS, turn)

        for k in range(CHUNKS):
            if k + 1 < CHUNKS:
                take_e(last, k + 1)
            have_e(last, k)
            loop(PARTS, lambda s: project_last(choose(s, quarters), k))
        loop(last, score_all)
        score_last()
        finish_last()

    @pl.when(jnp.logical_and(inner, jnp.logical_not(near)))
    def _():
        near_c().start()
        near_g().start()
        for i in range(count):
            far_w(i, 1).start()
        each_mask()
        near_w().start()
        for j in range(per_half):
            near_e(j).start()
        for pair in (inner_set, outer_set):
            for i in range(count):
                for w in pair:
                    got_mine(w, i)
                    spread(w, i)
        all_units(lambda j, k: e_far(j, k).start())
        for i in range(count):
            for v in range(2):
                relay(inner_set[v], v, i)
        have_own()
        take_e(0)
        have_e(0)
        order = ((0, 0), (1, 0), (2, 0), (0, 1), (1, 1), (2, 1), (0, 2), (1, 2), (2, 2), (3, 0), (3, 1), (3, 2))

        def turn(t):
            what = choose(t, [q * PARTS + j for q, j in order])

            @pl.when(t == 1)
            def _():
                for i in range(count):
                    if i == count - 1:
                        take_e(1)
                    for v in range(2):
                        relay(outer_set[v], v, i)

            @pl.when(t == 3)
            def _():
                have_e(1)

            @pl.when(t == 6)
            def _():
                take_e(2)
                have_e(2)

            @pl.when(t == 9)
            def _():
                take_e(last, 0)
                have_e(last, 0)
                loop(PARTS - 1, lambda s: project_last(choose(s, quarters), 0))
                for w in inner_set + outer_set:
                    got_diag(w)
                take_e(last, 1)
            project(choose(what // PARTS, quarters), what % PARTS)

            @pl.when(t >= 9)
            def _():
                far_copy(t - 9).start()

        loop(len(order), turn)
        project_last(d_part, 0)
        have_e(last, 1)
        loop(PARTS, lambda s: project_last(choose(s, quarters), 1))
        score_last()
        finish_last()

    arrived(mbuf.at[pl.ds(0, group - 1)], m_sems.at[1])
    mbuf[me] = mine[...]
    counts = mbuf[0]
    for g in range(1, group):
        counts = counts + mbuf[g]
    counts = counts[:, :1].astype(jnp.float32)
    slot = lax.broadcasted_iota(jnp.int32, (prompts, rows), 1).astype(jnp.float32)
    cols = (slot < counts).astype(jnp.float32)
    pairs = jnp.maximum(counts - 1.0, 1.0)
    same = lax.broadcasted_iota(jnp.int32, (block_rows, block_rows), 0)
    same = (same == lax.broadcasted_iota(jnp.int32, (block_rows, block_rows), 1)).astype(jnp.float32)
    down = lax.dot_general(same, valid, NT, preferred_element_type=jnp.float32)
    lane = lax.broadcasted_iota(jnp.int32, (block_rows, 128), 1)
    rates = jnp.zeros((block_rows, 128), jnp.float32)
    for batch in (range(last), range(last, per_half)):
        for h in range(2):
            @pl.when(jnp.logical_not(jnp.logical_and(jnp.logical_and(inner, near), half == h)))
            def _():
                arrived(rbuf.at[pl.ds(h * per_half + batch[0], len(batch))], r_recv.at[h, batch[0] // last])
        for j in batch:
            for h in range(2):
                p = h * per_half + j
                given = down[:, p:p + 1]
                prefs = jax.nn.sigmoid(rbuf[p].astype(jnp.float32)) * given * cols[p:p + 1, :]
                o_ref[p] = prefs
                totals = jnp.sum(prefs, axis=1, keepdims=True) - 0.5 * given
                rates = jnp.where(lane == p, given * totals / pairs[p:p + 1, :], rates)
    r_ref[...] = jnp.transpose(rates)[:prompts]

    departed(mbuf.at[pl.ds(0, group - 1)], m_sems.at[0])
    departed(ebuf.at[:, 0], e_send.at[1])
    for v in range(2):
        @pl.when(near == (v == 0))
        def _():
            @pl.when(inner)
            def _():
                block, cols = weights(half, True, v)
                departed(wbuf.at[block, pl.ds(0, quarter), cols], o_send.at[0])

            @pl.when(jnp.logical_not(inner))
            def _():
                block, cols = weights(half, False, v)
                departed(wbuf.at[block, pl.ds(0, quarter), cols], o_send.at[0])
                departed(wbuf.at[block, pl.ds(0, direct), cols], o_send.at[1])

    @pl.when(jnp.logical_not(near))
    def _():
        near_c().wait_send()

    @pl.when(jnp.logical_not(inner))
    def _():
        departed(ebuf.at[:, 0], e_send.at[0])

    @pl.when(inner)
    def _():
        departed(ebuf.at[:, 0], n_sems.at[0])
        departed(ebuf.at[:, pl.ds(0, 3)], h_send.at[0])
        departed(pbuf, p_send.at[0])

    @pl.when(jnp.logical_and(inner, near))
    def _():
        for w in outer_set:
            for sems in (x_send, y_send, u_send):
                sent_rows(w, sems, quarter)
            sent_rows(w, v_send, quarter - direct)
        departed(fbuf, r_send.at[0])

    @pl.when(jnp.logical_and(inner, jnp.logical_not(near)))
    def _():
        near_g().wait_send()
        near_w().wait_send()
        for w in inner_set + outer_set:
            for sems in (x_send, y_send, v_send):
                sent_rows(w, sems, quarter)
        departed(zt.at[pl.ds(0, last)], z_send.at[0])
        departed(tbuf, r_send.at[0])


def line_scores(embeddings, head_weight, mask):
    prompts, block_rows, features = embeddings.shape
    held = head_weight.shape[0]
    group = CHIPS * CORES
    side = group // 2
    per_half = prompts // 2
    rows = group * block_rows
    half_rows = rows // 2
    units = per_half - 1 + CHUNKS
    chip_width = features // CHIPS
    cut = held // 128 * 128
    bf16, f32 = jnp.bfloat16, jnp.float32
    dma = pltpu.SemaphoreType.DMA
    held_in = pl.BlockSpec(memory_space=pltpu.HBM)
    vmem = pl.BlockSpec(memory_space=pltpu.VMEM)
    return pl.pallas_call(
        kernel,
        out_shape=(
            jax.ShapeDtypeStruct((prompts, block_rows, rows), f32),
            jax.ShapeDtypeStruct((prompts, block_rows), f32),
        ),
        in_specs=[held_in, held_in, held_in],
        out_specs=(vmem, vmem),
        scratch_shapes=[
            pltpu.VMEM((prompts, block_rows), jnp.int32),
            pltpu.VMEM((per_half, group, block_rows, features), bf16),
            pltpu.VMEM((side, held, features), bf16),
            pltpu.VMEM((CORES, held, chip_width), bf16),
            pltpu.VMEM((chip_width - cut, cut), bf16),
            pltpu.VMEM((per_half, side, held, rows), bf16),
            pltpu.VMEM((per_half - 1, side, held, rows), bf16),
            pltpu.VMEM((side, held, rows), f32),
            pltpu.VMEM((per_half - 1, rows, rows), f32),
            pltpu.VMEM((rows, rows), f32),
            pltpu.VMEM((half_rows, rows), f32),
            pltpu.VMEM((half_rows, rows), f32),
            pltpu.VMEM((half_rows, rows), f32),
            pltpu.VMEM((per_half - 1, rows, rows), bf16),
            pltpu.VMEM((half_rows, rows), bf16),
            pltpu.VMEM((prompts, block_rows, rows), bf16),
            pltpu.VMEM((prompts, 128), jnp.int32),
            pltpu.VMEM((group, prompts, 128), jnp.int32),
            dma((3,)),
            dma((2,)),
            dma((units, CHIPS)),
            dma((units,)),
            dma((3,)),
            dma((1,)),
            dma((2,)),
            dma((2,)),
            dma((3,)),
            dma((3,)),
            dma((side,)),
            dma((side,)),
            dma((side,)),
            dma((side,)),
            dma((side, 4)),
            dma((side, 4)),
            dma((side,)),
            dma((1,)),
            dma((per_half - 1,)),
            dma((1,)),
            dma((1,)),
            dma((1,)),
            dma((2, 2)),
        ],
        compiler_params=pltpu.CompilerParams(
            collective_id=0, has_side_effects=True, vmem_limit_bytes=53 << 20
        ),
    )(embeddings, head_weight, mask)


def shards(embeddings, head_weight, valid_mask):
    group_size = lax.axis_size("resp")
    slots = group_size * embeddings.shape[1]
    if (lax.axis_size("prompt"), group_size) == (PARTS, CHIPS * CORES):
        return line_scores(embeddings, head_weight, valid_mask)
    valid_rows = valid_mask.astype(jnp.float32)
    counts = lax.psum(jnp.sum(valid_rows, axis=1), "resp")
    scores = gathered_scores(embeddings, head_weight)
    column_ids = jnp.arange(slots, dtype=jnp.float32)
    valid_cols = (column_ids[None, :] < counts[:, None]).astype(jnp.float32)
    preferences = jax.nn.sigmoid(scores) * valid_rows[:, :, None] * valid_cols[:, None, :]
    totals = jnp.sum(preferences, axis=2) - 0.5 * valid_rows
    win_rates = valid_rows * totals / jnp.maximum(counts - 1.0, 1.0)[:, None]
    return (preferences, win_rates)


def solution(mesh):
    return jax.shard_map(
        shards,
        mesh=mesh,
        in_specs=(P("prompt", "resp", None), P("resp", None), P("prompt", "resp")),
        out_specs=(P("prompt", "resp", None), P("prompt", "resp")),
        check_vma=False,
    )
```

```python
import functools

import jax
import jax.numpy as jnp
from jax import lax
from jax.experimental import pallas as pl
from jax.experimental.pallas import tpu as pltpu
from jax.sharding import PartitionSpec as P

MESH = pl.DeviceIdType.MESH
CORES = 2
CHIPS = 4
PARTS = 4
CHUNKS = 2
DIRECT = 3
NT = (((1,), (1,)), ((), ()))


def gathered_halves(embeddings, head_weight, own_index, group_size):
    prompts, block_rows, features = embeddings.shape
    held = head_weight.shape[0]
    slots = group_size * block_rows
    everyone = lax.all_gather(embeddings, "resp", axis=0, tiled=True)
    flat = everyone.reshape(group_size * prompts * block_rows, features)
    through = lax.dot_general(flat, head_weight, NT, preferred_element_type=jnp.float32)
    through = through.astype(jnp.bfloat16).reshape(group_size, prompts, block_rows, held)
    mine = lax.dynamic_slice_in_dim(
        everyone.reshape(group_size, prompts, block_rows, features), own_index * held, held, 3
    )
    partial = jnp.einsum("gpid,hpjd->gpihj", mine, through, preferred_element_type=jnp.float32)
    flipped = jnp.einsum("gpid,hpjd->gpihj", through, mine, preferred_element_type=jnp.float32)
    partial = (partial - flipped).astype(jnp.bfloat16)
    return partial.reshape(group_size, prompts, block_rows, slots)


def gathered_scores(embeddings, head_weight):
    group_size = lax.axis_size("resp")
    own_index = lax.axis_index("resp")
    prompts, block_rows, features = embeddings.shape
    slots = group_size * block_rows
    at_once = max(1, min(prompts, (1 << 11) // slots))

    def scores_of(some):
        partial = gathered_halves(some, head_weight, own_index, group_size)
        swapped = lax.all_to_all(partial, "resp", split_axis=0, concat_axis=0, tiled=True)
        return jnp.sum(swapped.astype(jnp.float32), axis=0)

    pieces = embeddings.reshape(prompts // at_once, at_once, block_rows, features)
    return lax.map(scores_of, pieces).reshape(prompts, block_rows, slots)


def kernel(e_ref, w_ref, m_hbm, o_ref, r_ref,
           m_ref, ebuf, wbuf, gbuf, cbuf, zt, zfar, zsum, held_raw, sbuf, keep, pbuf, qbuf, fbuf, tbuf, rbuf, mine, mbuf,
           m_sems, e_send, e_recv, h_recv, n_sems, h_send, o_send, l_sems, g_send, g_recv,
           x_send, y_send, u_send, v_send, a_recv, b_recv, d_recv, z_send, z_recv, p_send, p_recv, r_send, r_recv):
    part = lax.axis_index("prompt")
    me = lax.axis_index("resp")
    z = me // CORES
    core = me % CORES
    half = z // 2
    prompts, block_rows, features = e_ref.shape
    held = w_ref.shape[0]
    group = CHIPS * CORES
    per_half = prompts // 2
    side = group // 2
    span = held * side
    rows = group * block_rows
    half_rows = rows // 2
    quarter = held // PARTS
    z_in = 1 + half
    z_out = 3 * half
    z_far = 2 - half
    z_end = 3 - z_out
    inner = z == z_in
    near = core == half
    other = 1 - core
    here = me % side
    x_part = part + 1 - 2 * (part % 2)
    y_part = lax.rem(part + 2, PARTS)
    d_part = PARTS - 1 - part
    chip_width = features // CHIPS
    tiles = features // 256
    ends = [tiles * (CHUNKS - k) // CHUNKS * 256 for k in range(CHUNKS)]
    chunks = [(features - end, end - after) for end, after in zip(ends, ends[1:] + [0])]
    cut = held // 128 * 128
    spare = held - cut
    wide = chip_width - cut
    step = quarter // 7
    last = per_half - 1
    whole = per_half - 2
    pieces = ((0, step), (step, 2 * step), (3 * step, 2 * step), (5 * step, 2 * step))
    count = len(pieces)
    direct = pieces[DIRECT][0]

    def copy(src, dst, send, recv, chip, c, q=None):
        return pltpu.make_async_remote_copy(
            src, dst, send, recv,
            device_id=(part if q is None else q, chip * CORES + c), device_id_type=MESH,
        )

    def arrived(dst, recv):
        copy(dst, dst, m_sems.at[0], recv, z_far, core).wait_recv()

    def departed(src, send):
        copy(src, src, send, m_sems.at[1], z_far, core).wait_send()

    m_copy = pltpu.make_async_copy(m_hbm, m_ref, m_sems.at[2])
    m_copy.start()
    others = [lax.rem(me + d, group) for d in range(1, group)]
    barrier = pltpu.get_barrier_semaphore()
    for peer in others:
        pl.semaphore_signal(barrier, inc=1, device_id=(part, peer), device_id_type=MESH)
    for q in (x_part, y_part):
        pl.semaphore_signal(barrier, inc=1, device_id=(q, me), device_id_type=MESH)

    def mask_copy(d):
        return pltpu.make_async_remote_copy(
            mine, mbuf.at[me], m_sems.at[0], m_sems.at[1],
            device_id=(part, others[d]), device_id_type=MESH,
        )

    def chip_cols(chip):
        return pl.ds(pl.multiple_of(chip * chip_width, 128), chip_width)

    def cut_cols(chip, h):
        return pl.ds(pl.multiple_of(chip * chip_width + h * wide, 128), cut)

    def weights(h, within, v):
        size = features - (chip_width if within else 0) - (cut if v else 0)
        block = 2 * ((1 - h) if within else h) + ((1 - h) if v else h)
        return block, pl.ds(pl.multiple_of((1 - h) * (features - size), 128), size)

    outer_set = tuple(weights(core, False, v) for v in range(2))
    inner_set = tuple(weights(core, True, v) for v in range(2))
    first = 2 * half
    every = pl.ds(0, features)

    def span_rows(q, i):
        at, size = pieces[i]
        return pl.ds(pl.multiple_of(q * quarter + at, 16), size)

    def outer_w(i, v):
        block, cols = weights(half, False, v)
        at = span_rows(part, i)
        dst = wbuf.at[block, at, cols]
        return copy(w_ref.at[at, cols] if v else dst, dst, o_send.at[0], a_recv.at[block, i], z_in, half)

    def outer_diag(v):
        block, cols = weights(half, False, v)
        at = pl.ds(pl.multiple_of(d_part * quarter, 16), direct)
        dst = wbuf.at[block, at, cols]
        return copy(w_ref.at[at, cols] if v else dst, dst, o_send.at[1], d_recv.at[block], z_in, half)

    def far_w(i, v):
        block, cols = weights(half, True, v)
        at = span_rows(part, i)
        dst = wbuf.at[block, at, cols]
        return copy(w_ref.at[at, cols] if v else dst, dst, o_send.at[0], a_recv.at[block, i], z_far, half)

    def near_w():
        block, cols = weights(half, True, 1)
        return copy(w_ref.at[:, cols], wbuf.at[block, :, cols], g_send.at[0], g_recv.at[2], z_in, half)

    def near_g():
        return copy(w_ref.at[:, chip_cols(z_out)], gbuf.at[core], g_send.at[1], g_recv.at[0], z_in, half)

    def near_c():
        at = pl.ds(pl.multiple_of((1 - half) * spare, 16), held)
        return copy(w_ref.at[:, cut_cols(z, half)], cbuf.at[at], g_send.at[2], g_recv.at[1], z, half)

    def own_w(within):
        block, cols = weights(half, within, 0)
        return pltpu.make_async_copy(w_ref.at[:, cols], wbuf.at[block, :, cols], l_sems.at[0])

    def own_g():
        return pltpu.make_async_copy(w_ref.at[:, chip_cols(z_out)], gbuf.at[core], l_sems.at[1])

    def fold_core():
        arrived(cbuf.at[pl.ds(0, held)], g_recv.at[1])
        row = lax.broadcasted_iota(jnp.int32, (held, cut), 0)
        col = lax.broadcasted_iota(jnp.int32, (held, cut), 1)
        pick = (row - half * spare == col).astype(jnp.bfloat16)
        turned = lax.dot_general(pick, cbuf[...], NT, preferred_element_type=jnp.float32)
        cols = pl.ds(pl.multiple_of(z * chip_width + (1 - half) * cut, 128), wide)
        wbuf[here, :, cols] = (wbuf[here, :, cols].astype(jnp.float32) - turned).astype(jnp.bfloat16)

    def fold(q, at, size):
        start = q * quarter + at
        row = lax.broadcasted_iota(jnp.int32, (2 * size, chip_width), 0)
        col = lax.broadcasted_iota(jnp.int32, (2 * size, chip_width), 1)
        pick = (start + jnp.where(row < size, row, row + held - size) == col).astype(jnp.bfloat16)
        turned = lax.dot_general(
            pick, gbuf[...].reshape(chip_width, chip_width), NT, preferred_element_type=jnp.float32
        ).reshape(2, size, chip_width)
        pair, where, cols = pl.ds(first, 2), pl.ds(pl.multiple_of(start, 16), size), chip_cols(z_in)
        wbuf[pair, where, cols] = (wbuf[pair, where, cols].astype(jnp.float32) - turned).astype(jnp.bfloat16)

    def got_mine(w, i):
        block, cols = w
        arrived(wbuf.at[block, span_rows(part, i), cols], a_recv.at[block, i])

    def got_sides(w, i):
        block, cols = w
        arrived(wbuf.at[block, pl.ds(0, 2 * pieces[i][1]), cols], b_recv.at[block, i])

    def got_diag(w):
        block, cols = w
        arrived(wbuf.at[block, pl.ds(0, quarter), cols], d_recv.at[block])

    def along(w, q, i, send, recv, chip, q_to):
        block, cols = w
        spot = wbuf.at[block, span_rows(q, i), cols]
        return copy(spot, spot, send, recv, chip, core, q_to)

    def spread(w, i):
        along(w, part, i, x_send.at[w[0]], b_recv.at[w[0], i], z_in, x_part).start()
        along(w, part, i, y_send.at[w[0]], b_recv.at[w[0], i], z_in, y_part).start()

    def to_far(w, i):
        along(w, part, i, u_send.at[w[0]], a_recv.at[w[0], i], z_far, part).start()

    def relay(w, v, i):
        got_sides(w, i)
        if (i < 2) == (v == 0):
            along(w, x_part, i, v_send.at[w[0]], d_recv.at[w[0]], z_in, y_part).start()
        else:
            along(w, y_part, i, v_send.at[w[0]], d_recv.at[w[0]], z_in, x_part).start()

    def sent_rows(w, send, many):
        block, cols = w
        departed(wbuf.at[block, pl.ds(0, many), cols], send.at[block])

    def chunk_cols(k):
        return pl.ds(*chunks[k])

    def e_part(j, block, k):
        if k is None:
            return ebuf.at[j, block]
        return ebuf.at[j, block, :, chunk_cols(k)]

    def e_mine(h, j, k):
        if k is None:
            return e_ref.at[h * per_half + j]
        return e_ref.at[h * per_half + j, :, chunk_cols(k)]

    def unit(j, k):
        return j if k is None else whole + (j - whole) * CHUNKS + k

    def e_far(j, k=None):
        recv = e_recv.at[unit(j, k), z]
        return copy(e_mine(1 - half, j, k), e_part(j, me, k), e_send.at[1], recv, z_far, core)

    def e_near(j, k=None):
        return copy(e_mine(half, j, k), e_part(j, me, k), e_send.at[0], e_recv.at[unit(j, k), z], z_in, core)

    def near_e(j):
        return copy(e_mine(half, j, None), ebuf.at[j, me], n_sems.at[0], n_sems.at[1], z_in, other)

    def own_e(j):
        return pltpu.make_async_copy(e_mine(half, j, None), ebuf.at[j, me], n_sems.at[2])

    away = (z_out, z_far, z_end)

    def three(j, k):
        if k is None:
            return ebuf.at[j, pl.ds(0, 3)]
        return ebuf.at[j, pl.ds(0, 3), :, chunk_cols(k)]

    def take_e(j, k=None):
        for chip in away:
            spot = e_part(j, chip * CORES + core, k)
            arrived(spot, e_recv.at[unit(j, k), chip])
            copy(spot, spot, h_send.at[0], h_recv.at[unit(j, k)], z_in, other).start()

    def have_e(j, k=None):
        arrived(three(j, k), h_recv.at[unit(j, k)])

    def have_own():
        pltpu.make_async_copy(ebuf.at[:, me], ebuf.at[:, me], n_sems.at[2]).wait()
        arrived(ebuf.at[:, z_in * CORES + other], n_sems.at[1])

    def all_units(act):
        for j in range(whole):
            act(j, None)
        for j in range(whole, per_half):
            for k in range(CHUNKS):
                act(j, k)

    def partial_copy():
        return copy(pbuf, qbuf, p_send.at[0], p_recv.at[0], z_in, other)

    def far_copy(j):
        return copy(zt.at[j], zfar.at[j], z_send.at[0], z_recv.at[j], z_in, other)

    def project(q, j):
        at = pl.ds(pl.multiple_of(q * quarter, 16), quarter)
        left = wbuf[:, at].reshape(side * quarter, features)
        right = ebuf[j].reshape(rows, features)
        zt[j, :, at] = lax.dot_general(
            left, right, NT, preferred_element_type=jnp.float32
        ).astype(jnp.bfloat16).reshape(side, quarter, rows)

    def project_part(j, q, k):
        at = pl.ds(pl.multiple_of(q * quarter, 16), quarter)
        cols, width = chunk_cols(k), chunks[k][1]
        left = wbuf[:, at, cols].reshape(side * quarter, width)
        right = ebuf[j, :, :, cols].reshape(rows, width)
        total = lax.dot_general(
            left, right, NT, preferred_element_type=jnp.float32
        ).reshape(side, quarter, rows)
        if k > 0:
            total = zsum[j - whole, :, at] + total
        if k < CHUNKS - 1:
            zsum[j - whole, :, at] = total
        else:
            zt[j, :, at] = total.astype(jnp.bfloat16)

    mine_at = pl.multiple_of(core * half_rows, half_rows)
    theirs_at = pl.multiple_of(other * half_rows, half_rows)

    def raw_scores(j, c, held_zt):
        lanes = pl.ds(pl.multiple_of(c * span, 128), span)
        left = ebuf[j, :, :, lanes].reshape(rows, span)
        return jnp.dot(left, held_zt[j].reshape(span, rows), preferred_element_type=jnp.float32)

    def score_last():
        raw = raw_scores(last, core, zt)
        sbuf[...] = raw - jnp.transpose(raw)
        pbuf[...] = sbuf[pl.ds(theirs_at, half_rows)]
        partial_copy().start()
        keep[...] = sbuf[pl.ds(mine_at, half_rows)]

    def block_at(t):
        return pl.ds(pl.multiple_of(t * block_rows, block_rows), block_rows)

    def final_copy(src, j, t):
        return pltpu.make_async_remote_copy(
            src, rbuf.at[half * per_half + j], r_send.at[0], r_recv.at[half, j // last],
            device_id=(part, t), device_id_type=MESH,
        )

    def score_all(j):
        arrived(zfar.at[j], z_recv.at[j])
        raw = held_raw[j] + raw_scores(j, other, zfar)
        fbuf[j] = (raw - jnp.transpose(raw)).astype(jnp.bfloat16)
        for d in range(group - 1):
            final_copy(fbuf.at[j, block_at(others[d])], j, others[d]).start()
        rbuf[half * per_half + j] = fbuf[j, block_at(me)]

    def finish_last():
        arrived(qbuf, p_recv.at[0])
        tbuf[...] = (keep[...] + qbuf[...]).astype(jnp.bfloat16)
        for t in range(side):
            @pl.when(core * side + t != me)
            def _():
                final_copy(tbuf.at[block_at(t)], last, core * side + t).start()

        @pl.when(near)
        def _():
            rbuf[half * per_half + last] = tbuf[block_at(here)]

    def each_mask():
        for d in range(group - 1):
            mask_copy(d).start()

    def loop(n, body):
        def run(j, carry):
            body(j)
            return carry
        lax.fori_loop(0, n, run, 0)

    def choose(index, values):
        picked = values[0]
        for n in range(1, len(values)):
            picked = jnp.where(index == n, values[n], picked)
        return picked

    quarters = (part, x_part, y_part, d_part)

    @pl.when(near)
    def _():
        @pl.when(inner)
        def _():
            own_w(True).start()
            own_g().start()

        @pl.when(jnp.logical_not(inner))
        def _():
            own_w(False).start()

    @pl.when(inner)
    def _():
        for j in range(per_half):
            own_e(j).start()

    wbuf[pl.ds(inner_set[0][0] // 2 * 2, 2), :, chip_cols(3 * core)] = jnp.zeros((2, held, chip_width), jnp.bfloat16)
    wbuf[inner_set[1][0], :, cut_cols(1 + core, core)] = jnp.zeros((held, cut), jnp.bfloat16)
    wbuf[outer_set[1][0], :, cut_cols(3 * core, core)] = jnp.zeros((held, cut), jnp.bfloat16)
    cbuf[pl.ds(pl.multiple_of(half * held, 16), spare)] = jnp.zeros((spare, cut), jnp.bfloat16)
    m_copy.wait()
    valid = m_ref[...].astype(jnp.float32)
    mine[...] = jnp.broadcast_to(jnp.sum(m_ref[...], axis=1, keepdims=True), mine.shape)
    pl.semaphore_wait(barrier, len(others) + 2)

    for v in range(2):
        @pl.when(jnp.logical_and(jnp.logical_not(inner), near == (v == 0)))
        def _():
            if v:
                near_c().start()
            else:
                own_w(False).wait()
                fold_core()
            for i in range(count):
                outer_w(i, v).start()
            outer_diag(v).start()

            def send(j, k):
                e_near(j, k).start()
                e_far(j, k).start()

            all_units(send)
            each_mask()

    @pl.when(jnp.logical_and(inner, near))
    def _():
        own_w(True).wait()
        fold_core()
        for i in range(count):
            far_w(i, 0).start()
        for j in range(per_half):
            near_e(j).start()
        own_g().wait()
        arrived(gbuf.at[other], g_recv.at[0])
        for i in range(count):
            for w in outer_set:
                got_mine(w, i)
            fold(part, *pieces[i])
            for w in outer_set:
                to_far(w, i)
                spread(w, i)
        all_units(lambda j, k: e_far(j, k).start())
        each_mask()
        block, cols = weights(half, True, 1)
        arrived(wbuf.at[block, :, cols], g_recv.at[2])
        have_own()
        for i in range(count):
            for v in range(2):
                if i < DIRECT:
                    got_sides(outer_set[v], i)
                else:
                    relay(outer_set[v], v, i)

        def turn(t):
            j = t // PARTS
            s = t % PARTS

            @pl.when(s == 0)
            def _():
                take_e(j)
                have_e(j)

            @pl.when(t == PARTS - 1)
            def _():
                for w in outer_set:
                    got_diag(w)
                fold(d_part, 0, direct)

            project(choose(s, quarters), j)

            @pl.when(s == PARTS - 1)
            def _():
                held_raw[j] = raw_scores(j, core, zt)

        loop(whole * PARTS, turn)
        take_e(whole, 0)
        have_e(whole, 0)

        def with_take(j, k, at):
            def run(s):
                @pl.when(s == at)
                def _():
                    take_e(whole + (k + 1) // CHUNKS, (k + 1) % CHUNKS)
                project_part(j, choose(s, quarters), k)

            loop(PARTS, run)

        with_take(whole, 0, 3)
        have_e(whole, 1)
        with_take(whole, 1, 2)
        held_raw[whole] = raw_scores(whole, core, zt)
        take_e(last, 1)
        for k in range(CHUNKS):
            have_e(last, k)
            loop(PARTS, lambda s: project_part(last, choose(s, quarters), k))
        loop(last, score_all)
        score_last()
        finish_last()

    @pl.when(jnp.logical_and(inner, jnp.logical_not(near)))
    def _():
        near_c().start()
        near_g().start()
        for i in range(count):
            far_w(i, 1).start()
        near_w().start()
        for j in range(per_half):
            near_e(j).start()
        for pair in (inner_set, outer_set):
            for i in range(count):
                for w in pair:
                    got_mine(w, i)
                    spread(w, i)
        all_units(lambda j, k: e_far(j, k).start())
        each_mask()
        for i in range(count):
            for v in range(2):
                relay(inner_set[v], v, i)
        have_own()
        take_e(0)
        have_e(0)
        order = ((0, 0), (1, 0), (2, 0), (0, 1), (1, 1), (2, 1), (3, 0), (3, 1))

        def three_parts(j, k):
            loop(PARTS - 1, lambda s: project_part(j, choose(s, quarters), k))

        def turn(t):
            what = choose(t, [q * PARTS + j for q, j in order])

            @pl.when(t == 1)
            def _():
                for i in range(count):
                    if i == count - 1:
                        take_e(1)
                    for v in range(2):
                        relay(outer_set[v], v, i)

            @pl.when(t == 3)
            def _():
                have_e(1)

            @pl.when(t == 5)
            def _():
                take_e(whole, 0)

            @pl.when(t == 6)
            def _():
                have_e(whole, 0)
                three_parts(whole, 0)
                take_e(whole, 1)
                have_e(whole, 1)
                three_parts(whole, 1)
                take_e(last, 0)
                have_e(last, 0)
                three_parts(last, 0)
                for w in inner_set + outer_set:
                    got_diag(w)
                take_e(last, 1)
            project(choose(what // PARTS, quarters), what % PARTS)

            @pl.when(t >= 6)
            def _():
                far_copy(t - 6).start()

        loop(len(order), turn)
        for k in range(CHUNKS):
            project_part(whole, d_part, k)
        far_copy(whole).start()
        project_part(last, d_part, 0)
        have_e(last, 1)
        loop(PARTS, lambda s: project_part(last, choose(s, quarters), 1))
        score_last()
        finish_last()

    arrived(mbuf.at[pl.ds(0, group - 1)], m_sems.at[1])
    mbuf[me] = mine[...]
    counts = mbuf[0]
    for g in range(1, group):
        counts = counts + mbuf[g]
    counts = counts[:, :1].astype(jnp.float32)
    slot = lax.broadcasted_iota(jnp.int32, (prompts, rows), 1).astype(jnp.float32)
    cols = (slot < counts).astype(jnp.float32)
    pairs = jnp.maximum(counts - 1.0, 1.0)
    same = lax.broadcasted_iota(jnp.int32, (block_rows, block_rows), 0)
    same = (same == lax.broadcasted_iota(jnp.int32, (block_rows, block_rows), 1)).astype(jnp.float32)
    down = lax.dot_general(same, valid, NT, preferred_element_type=jnp.float32)
    lane = lax.broadcasted_iota(jnp.int32, (block_rows, 128), 1)
    rates = jnp.zeros((block_rows, 128), jnp.float32)
    for batch in (range(last), range(last, per_half)):
        for h in range(2):
            @pl.when(jnp.logical_not(jnp.logical_and(jnp.logical_and(inner, near), half == h)))
            def _():
                arrived(rbuf.at[pl.ds(h * per_half + batch[0], len(batch))], r_recv.at[h, batch[0] // last])
        for j in batch:
            for h in range(2):
                p = h * per_half + j
                given = down[:, p:p + 1]
                prefs = jax.nn.sigmoid(rbuf[p].astype(jnp.float32)) * given * cols[p:p + 1, :]
                o_ref[p] = prefs
                totals = jnp.sum(prefs, axis=1, keepdims=True) - 0.5 * given
                rates = jnp.where(lane == p, given * totals / pairs[p:p + 1, :], rates)
    r_ref[...] = jnp.transpose(rates)[:prompts]

    departed(mbuf.at[pl.ds(0, group - 1)], m_sems.at[0])
    departed(ebuf.at[:, 0], e_send.at[1])
    for v in range(2):
        @pl.when(near == (v == 0))
        def _():
            @pl.when(inner)
            def _():
                block, cols = weights(half, True, v)
                departed(wbuf.at[block, pl.ds(0, quarter), cols], o_send.at[0])

            @pl.when(jnp.logical_not(inner))
            def _():
                block, cols = weights(half, False, v)
                departed(wbuf.at[block, pl.ds(0, quarter), cols], o_send.at[0])
                departed(wbuf.at[block, pl.ds(0, direct), cols], o_send.at[1])

    @pl.when(jnp.logical_not(near))
    def _():
        near_c().wait_send()

    @pl.when(jnp.logical_not(inner))
    def _():
        departed(ebuf.at[:, 0], e_send.at[0])

    @pl.when(inner)
    def _():
        departed(ebuf.at[:, 0], n_sems.at[0])
        departed(ebuf.at[:, pl.ds(0, 3)], h_send.at[0])
        departed(pbuf, p_send.at[0])

    @pl.when(jnp.logical_and(inner, near))
    def _():
        for w in outer_set:
            for sems in (x_send, y_send, u_send):
                sent_rows(w, sems, quarter)
            sent_rows(w, v_send, quarter - direct)
        departed(fbuf, r_send.at[0])

    @pl.when(jnp.logical_and(inner, jnp.logical_not(near)))
    def _():
        near_g().wait_send()
        near_w().wait_send()
        for w in inner_set + outer_set:
            for sems in (x_send, y_send, v_send):
                sent_rows(w, sems, quarter)
        departed(zt.at[pl.ds(0, last)], z_send.at[0])
        departed(tbuf, r_send.at[0])


def line_scores(embeddings, head_weight, mask):
    prompts, block_rows, features = embeddings.shape
    held = head_weight.shape[0]
    group = CHIPS * CORES
    side = group // 2
    per_half = prompts // 2
    rows = group * block_rows
    half_rows = rows // 2
    units = per_half - 2 + 2 * CHUNKS
    chip_width = features // CHIPS
    cut = held // 128 * 128
    bf16, f32 = jnp.bfloat16, jnp.float32
    dma = pltpu.SemaphoreType.DMA
    held_in = pl.BlockSpec(memory_space=pltpu.HBM)
    vmem = pl.BlockSpec(memory_space=pltpu.VMEM)
    return pl.pallas_call(
        kernel,
        out_shape=(
            jax.ShapeDtypeStruct((prompts, block_rows, rows), f32),
            jax.ShapeDtypeStruct((prompts, block_rows), f32),
        ),
        in_specs=[held_in, held_in, held_in],
        out_specs=(vmem, vmem),
        scratch_shapes=[
            pltpu.VMEM((prompts, block_rows), jnp.int32),
            pltpu.VMEM((per_half, group, block_rows, features), bf16),
            pltpu.VMEM((side, held, features), bf16),
            pltpu.VMEM((CORES, held, chip_width), bf16),
            pltpu.VMEM((chip_width - cut, cut), bf16),
            pltpu.VMEM((per_half, side, held, rows), bf16),
            pltpu.VMEM((per_half - 1, side, held, rows), bf16),
            pltpu.VMEM((2, side, held, rows), f32),
            pltpu.VMEM((per_half - 1, rows, rows), f32),
            pltpu.VMEM((rows, rows), f32),
            pltpu.VMEM((half_rows, rows), f32),
            pltpu.VMEM((half_rows, rows), f32),
            pltpu.VMEM((half_rows, rows), f32),
            pltpu.VMEM((per_half - 1, rows, rows), bf16),
            pltpu.VMEM((half_rows, rows), bf16),
            pltpu.VMEM((prompts, block_rows, rows), bf16),
            pltpu.VMEM((prompts, 128), jnp.int32),
            pltpu.VMEM((group, prompts, 128), jnp.int32),
            dma((3,)),
            dma((2,)),
            dma((units, CHIPS)),
            dma((units,)),
            dma((3,)),
            dma((1,)),
            dma((2,)),
            dma((2,)),
            dma((3,)),
            dma((3,)),
            dma((side,)),
            dma((side,)),
            dma((side,)),
            dma((side,)),
            dma((side, 4)),
            dma((side, 4)),
            dma((side,)),
            dma((1,)),
            dma((per_half - 1,)),
            dma((1,)),
            dma((1,)),
            dma((1,)),
            dma((2, 2)),
        ],
        compiler_params=pltpu.CompilerParams(
            collective_id=0, has_side_effects=True, vmem_limit_bytes=53 << 20
        ),
    )(embeddings, head_weight, pltpu.with_memory_space_constraint(mask, pltpu.HBM))


def shards(embeddings, head_weight, valid_mask):
    group_size = lax.axis_size("resp")
    slots = group_size * embeddings.shape[1]
    if (lax.axis_size("prompt"), group_size) == (PARTS, CHIPS * CORES):
        return line_scores(embeddings, head_weight, valid_mask)
    valid_rows = valid_mask.astype(jnp.float32)
    counts = lax.psum(jnp.sum(valid_rows, axis=1), "resp")
    scores = gathered_scores(embeddings, head_weight)
    column_ids = jnp.arange(slots, dtype=jnp.float32)
    valid_cols = (column_ids[None, :] < counts[:, None]).astype(jnp.float32)
    preferences = jax.nn.sigmoid(scores) * valid_rows[:, :, None] * valid_cols[:, None, :]
    totals = jnp.sum(preferences, axis=2) - 0.5 * valid_rows
    win_rates = valid_rows * totals / jnp.maximum(counts - 1.0, 1.0)[:, None]
    return (preferences, win_rates)


def solution(mesh):
    return jax.shard_map(
        shards,
        mesh=mesh,
        in_specs=(P("prompt", "resp", None), P("resp", None), P("prompt", "resp")),
        out_specs=(P("prompt", "resp", None), P("prompt", "resp")),
        check_vma=False,
    )
```

```python
import functools

import jax
import jax.numpy as jnp
from jax import lax
from jax.experimental import pallas as pl
from jax.experimental.pallas import tpu as pltpu
from jax.sharding import PartitionSpec as P

MESH = pl.DeviceIdType.MESH
CORES = 2
CHIPS = 4
PARTS = 4
CHUNKS = 2
DIRECT = 3
NT = (((1,), (1,)), ((), ()))


def gathered_halves(embeddings, head_weight, own_index, group_size):
    prompts, block_rows, features = embeddings.shape
    held = head_weight.shape[0]
    slots = group_size * block_rows
    everyone = lax.all_gather(embeddings, "resp", axis=0, tiled=True)
    flat = everyone.reshape(group_size * prompts * block_rows, features)
    through = lax.dot_general(flat, head_weight, NT, preferred_element_type=jnp.float32)
    through = through.astype(jnp.bfloat16).reshape(group_size, prompts, block_rows, held)
    mine = lax.dynamic_slice_in_dim(
        everyone.reshape(group_size, prompts, block_rows, features), own_index * held, held, 3
    )
    partial = jnp.einsum("gpid,hpjd->gpihj", mine, through, preferred_element_type=jnp.float32)
    flipped = jnp.einsum("gpid,hpjd->gpihj", through, mine, preferred_element_type=jnp.float32)
    partial = (partial - flipped).astype(jnp.bfloat16)
    return partial.reshape(group_size, prompts, block_rows, slots)


def gathered_scores(embeddings, head_weight):
    group_size = lax.axis_size("resp")
    own_index = lax.axis_index("resp")
    prompts, block_rows, features = embeddings.shape
    slots = group_size * block_rows
    at_once = max(1, min(prompts, (1 << 11) // slots))

    def scores_of(some):
        partial = gathered_halves(some, head_weight, own_index, group_size)
        swapped = lax.all_to_all(partial, "resp", split_axis=0, concat_axis=0, tiled=True)
        return jnp.sum(swapped.astype(jnp.float32), axis=0)

    pieces = embeddings.reshape(prompts // at_once, at_once, block_rows, features)
    return lax.map(scores_of, pieces).reshape(prompts, block_rows, slots)


def kernel(e_ref, w_ref, m_hbm, o_ref, r_ref,
           m_ref, ebuf, wbuf, gbuf, cbuf, zt, zfar, zsum, held_raw, fbuf, tbuf, rbuf, lbuf, mine, mbuf,
           m_sems, e_send, e_recv, h_recv, n_sems, h_send, o_send, l_sems, g_send, g_recv,
           x_send, y_send, u_send, v_send, a_recv, b_recv, d_recv, z_send, z_recv, r_send, r_recv, s_recv):
    part = lax.axis_index("prompt")
    me = lax.axis_index("resp")
    z = me // CORES
    core = me % CORES
    half = z // 2
    prompts, block_rows, features = e_ref.shape
    held = w_ref.shape[0]
    group = CHIPS * CORES
    per_half = prompts // 2
    side = group // 2
    span = held * side
    rows = group * block_rows
    quarter = held // PARTS
    z_in = 1 + half
    z_out = 3 * half
    z_far = 2 - half
    z_end = 3 - z_out
    inner = z == z_in
    near = core == half
    other = 1 - core
    here = me % side
    x_part = part + 1 - 2 * (part % 2)
    y_part = lax.rem(part + 2, PARTS)
    d_part = PARTS - 1 - part
    chip_width = features // CHIPS
    tiles = features // 256
    ends = [tiles * (CHUNKS - k) // CHUNKS * 256 for k in range(CHUNKS)]
    chunks = [(features - end, end - after) for end, after in zip(ends, ends[1:] + [0])]
    cut = held // 128 * 128
    spare = held - cut
    wide = chip_width - cut
    step = quarter // 7
    last = per_half - 1
    whole = per_half - 2
    pieces = ((0, step), (step, 2 * step), (3 * step, 2 * step), (5 * step, 2 * step))
    count = len(pieces)
    direct = pieces[DIRECT][0]

    def copy(src, dst, send, recv, chip, c, q=None):
        return pltpu.make_async_remote_copy(
            src, dst, send, recv,
            device_id=(part if q is None else q, chip * CORES + c), device_id_type=MESH,
        )

    def arrived(dst, recv):
        copy(dst, dst, m_sems.at[0], recv, z_far, core).wait_recv()

    def departed(src, send):
        copy(src, src, send, m_sems.at[1], z_far, core).wait_send()

    m_copy = pltpu.make_async_copy(m_hbm, m_ref, m_sems.at[2])
    m_copy.start()
    others = [lax.rem(me + d, group) for d in range(1, group)]
    barrier = pltpu.get_barrier_semaphore()
    for peer in others:
        pl.semaphore_signal(barrier, inc=1, device_id=(part, peer), device_id_type=MESH)
    for q in (x_part, y_part):
        pl.semaphore_signal(barrier, inc=1, device_id=(q, me), device_id_type=MESH)

    def mask_copy(d):
        return pltpu.make_async_remote_copy(
            mine, mbuf.at[me], m_sems.at[0], m_sems.at[1],
            device_id=(part, others[d]), device_id_type=MESH,
        )

    def chip_cols(chip):
        return pl.ds(pl.multiple_of(chip * chip_width, 128), chip_width)

    def cut_cols(chip, h):
        return pl.ds(pl.multiple_of(chip * chip_width + h * wide, 128), cut)

    def weights(h, within, v):
        size = features - (chip_width if within else 0) - (cut if v else 0)
        block = 2 * ((1 - h) if within else h) + ((1 - h) if v else h)
        return block, pl.ds(pl.multiple_of((1 - h) * (features - size), 128), size)

    outer_set = tuple(weights(core, False, v) for v in range(2))
    inner_set = tuple(weights(core, True, v) for v in range(2))
    first = 2 * half
    every = pl.ds(0, features)

    def span_rows(q, i):
        at, size = pieces[i]
        return pl.ds(pl.multiple_of(q * quarter + at, 16), size)

    def outer_w(i, v):
        block, cols = weights(half, False, v)
        at = span_rows(part, i)
        dst = wbuf.at[block, at, cols]
        return copy(w_ref.at[at, cols] if v else dst, dst, o_send.at[0], a_recv.at[block, i], z_in, half)

    def outer_diag(v):
        block, cols = weights(half, False, v)
        at = pl.ds(pl.multiple_of(d_part * quarter, 16), direct)
        dst = wbuf.at[block, at, cols]
        return copy(w_ref.at[at, cols] if v else dst, dst, o_send.at[1], d_recv.at[block], z_in, half)

    def far_w(i, v):
        block, cols = weights(half, True, v)
        at = span_rows(part, i)
        dst = wbuf.at[block, at, cols]
        return copy(w_ref.at[at, cols] if v else dst, dst, o_send.at[0], a_recv.at[block, i], z_far, half)

    def near_w():
        block, cols = weights(half, True, 1)
        return copy(w_ref.at[:, cols], wbuf.at[block, :, cols], g_send.at[0], g_recv.at[2], z_in, half)

    def near_g():
        return copy(w_ref.at[:, chip_cols(z_out)], gbuf.at[core], g_send.at[1], g_recv.at[0], z_in, half)

    def near_c():
        at = pl.ds(pl.multiple_of((1 - half) * spare, 16), held)
        return copy(w_ref.at[:, cut_cols(z, half)], cbuf.at[at], g_send.at[2], g_recv.at[1], z, half)

    def own_w(within):
        block, cols = weights(half, within, 0)
        return pltpu.make_async_copy(w_ref.at[:, cols], wbuf.at[block, :, cols], l_sems.at[0])

    def own_g():
        return pltpu.make_async_copy(w_ref.at[:, chip_cols(z_out)], gbuf.at[core], l_sems.at[1])

    def fold_core():
        arrived(cbuf.at[pl.ds(0, held)], g_recv.at[1])
        row = lax.broadcasted_iota(jnp.int32, (held, cut), 0)
        col = lax.broadcasted_iota(jnp.int32, (held, cut), 1)
        pick = (row - half * spare == col).astype(jnp.bfloat16)
        turned = lax.dot_general(pick, cbuf[...], NT, preferred_element_type=jnp.float32)
        cols = pl.ds(pl.multiple_of(z * chip_width + (1 - half) * cut, 128), wide)
        wbuf[here, :, cols] = (wbuf[here, :, cols].astype(jnp.float32) - turned).astype(jnp.bfloat16)

    def fold(q, at, size):
        start = q * quarter + at
        row = lax.broadcasted_iota(jnp.int32, (2 * size, chip_width), 0)
        col = lax.broadcasted_iota(jnp.int32, (2 * size, chip_width), 1)
        pick = (start + jnp.where(row < size, row, row + held - size) == col).astype(jnp.bfloat16)
        turned = lax.dot_general(
            pick, gbuf[...].reshape(chip_width, chip_width), NT, preferred_element_type=jnp.float32
        ).reshape(2, size, chip_width)
        pair, where, cols = pl.ds(first, 2), pl.ds(pl.multiple_of(start, 16), size), chip_cols(z_in)
        wbuf[pair, where, cols] = (wbuf[pair, where, cols].astype(jnp.float32) - turned).astype(jnp.bfloat16)

    def got_mine(w, i):
        block, cols = w
        arrived(wbuf.at[block, span_rows(part, i), cols], a_recv.at[block, i])

    def got_sides(w, i):
        block, cols = w
        arrived(wbuf.at[block, pl.ds(0, 2 * pieces[i][1]), cols], b_recv.at[block, i])

    def got_diag(w):
        block, cols = w
        arrived(wbuf.at[block, pl.ds(0, quarter), cols], d_recv.at[block])

    def along(w, q, i, send, recv, chip, q_to):
        block, cols = w
        spot = wbuf.at[block, span_rows(q, i), cols]
        return copy(spot, spot, send, recv, chip, core, q_to)

    def spread(w, i):
        along(w, part, i, x_send.at[w[0]], b_recv.at[w[0], i], z_in, x_part).start()
        along(w, part, i, y_send.at[w[0]], b_recv.at[w[0], i], z_in, y_part).start()

    def to_far(w, i):
        along(w, part, i, u_send.at[w[0]], a_recv.at[w[0], i], z_far, part).start()

    def relay(w, v, i):
        got_sides(w, i)
        if (i < 2) == (v == 0):
            along(w, x_part, i, v_send.at[w[0]], d_recv.at[w[0]], z_in, y_part).start()
        else:
            along(w, y_part, i, v_send.at[w[0]], d_recv.at[w[0]], z_in, x_part).start()

    def sent_rows(w, send, many):
        block, cols = w
        departed(wbuf.at[block, pl.ds(0, many), cols], send.at[block])

    def chunk_cols(k):
        return pl.ds(*chunks[k])

    def e_part(j, block, k):
        if k is None:
            return ebuf.at[j, block]
        return ebuf.at[j, block, :, chunk_cols(k)]

    def e_mine(h, j, k):
        if k is None:
            return e_ref.at[h * per_half + j]
        return e_ref.at[h * per_half + j, :, chunk_cols(k)]

    def unit(j, k):
        return j if k is None else whole + (j - whole) * CHUNKS + k

    def e_far(j, k=None):
        recv = e_recv.at[unit(j, k), z]
        return copy(e_mine(1 - half, j, k), e_part(j, me, k), e_send.at[1], recv, z_far, core)

    def e_near(j, k=None):
        return copy(e_mine(half, j, k), e_part(j, me, k), e_send.at[0], e_recv.at[unit(j, k), z], z_in, core)

    def near_e(j):
        return copy(e_mine(half, j, None), ebuf.at[j, me], n_sems.at[0], n_sems.at[1], z_in, other)

    def own_e(j):
        return pltpu.make_async_copy(e_mine(half, j, None), ebuf.at[j, me], n_sems.at[2])

    away = (z_out, z_far, z_end)

    def three(j, k):
        if k is None:
            return ebuf.at[j, pl.ds(0, 3)]
        return ebuf.at[j, pl.ds(0, 3), :, chunk_cols(k)]

    def take_e(j, k=None):
        for chip in away:
            spot = e_part(j, chip * CORES + core, k)
            arrived(spot, e_recv.at[unit(j, k), chip])
            copy(spot, spot, h_send.at[0], h_recv.at[unit(j, k)], z_in, other).start()

    def have_e(j, k=None):
        arrived(three(j, k), h_recv.at[unit(j, k)])

    def have_own():
        pltpu.make_async_copy(ebuf.at[:, me], ebuf.at[:, me], n_sems.at[2]).wait()
        arrived(ebuf.at[:, z_in * CORES + other], n_sems.at[1])

    def all_units(act):
        for j in range(whole):
            act(j, None)
        for j in range(whole, per_half):
            for k in range(CHUNKS):
                act(j, k)

    def far_copy(j):
        return copy(zt.at[j], zfar.at[j], z_send.at[0], z_recv.at[j], z_in, other)

    def project(q, j):
        at = pl.ds(pl.multiple_of(q * quarter, 16), quarter)
        left = wbuf[:, at].reshape(side * quarter, features)
        right = ebuf[j].reshape(rows, features)
        zt[j, :, at] = lax.dot_general(
            left, right, NT, preferred_element_type=jnp.float32
        ).astype(jnp.bfloat16).reshape(side, quarter, rows)

    def project_pair(j, base):
        at = pl.ds(pl.multiple_of(d_part * quarter, 16), quarter)
        blocks = pl.ds(base, 2)
        left = wbuf[blocks, at].reshape(2 * quarter, features)
        right = ebuf[j].reshape(rows, features)
        zt[j, blocks, at] = lax.dot_general(
            left, right, NT, preferred_element_type=jnp.float32
        ).astype(jnp.bfloat16).reshape(2, quarter, rows)

    def project_part(j, q, k):
        at = pl.ds(pl.multiple_of(q * quarter, 16), quarter)
        cols, width = chunk_cols(k), chunks[k][1]
        left = wbuf[:, at, cols].reshape(side * quarter, width)
        right = ebuf[j, :, :, cols].reshape(rows, width)
        total = lax.dot_general(
            left, right, NT, preferred_element_type=jnp.float32
        ).reshape(side, quarter, rows)
        if k > 0:
            total = zsum[j - whole, :, at] + total
        if k < CHUNKS - 1:
            zsum[j - whole, :, at] = total
        else:
            zt[j, :, at] = total.astype(jnp.bfloat16)

    def raw_scores(j, c, held_zt):
        lanes = pl.ds(pl.multiple_of(c * span, 128), span)
        left = ebuf[j, :, :, lanes].reshape(rows, span)
        return jnp.dot(left, held_zt[j].reshape(span, rows), preferred_element_type=jnp.float32)

    def block_at(t):
        return pl.ds(pl.multiple_of(t * block_rows, block_rows), block_rows)

    def final_copy(src, dst, send, recv, t):
        return pltpu.make_async_remote_copy(
            src, dst, send, recv, device_id=(part, t), device_id_type=MESH
        )

    def score_all(j):
        arrived(zfar.at[j], z_recv.at[j])
        raw = held_raw[j] + raw_scores(j, other, zfar)
        fbuf[j] = (raw - jnp.transpose(raw)).astype(jnp.bfloat16)
        for d in range(group - 1):
            spot = rbuf.at[half * last + j]
            final_copy(fbuf.at[j, block_at(others[d])], spot, r_send.at[0], r_recv.at[half], others[d]).start()
        rbuf[half * last + j] = fbuf[j, block_at(me)]

    def score_last():
        raw = raw_scores(last, core, zt)
        tbuf[...] = (raw - jnp.transpose(raw)).astype(jnp.bfloat16)
        for d in range(group - 1):
            spot = lbuf.at[half, core]
            final_copy(tbuf.at[block_at(others[d])], spot, r_send.at[1], s_recv.at[half, core], others[d]).start()
        lbuf[half, core] = tbuf[block_at(me)]

    def each_mask():
        for d in range(group - 1):
            mask_copy(d).start()

    def loop(n, body):
        def run(j, carry):
            body(j)
            return carry
        lax.fori_loop(0, n, run, 0)

    def choose(index, values):
        picked = values[0]
        for n in range(1, len(values)):
            picked = jnp.where(index == n, values[n], picked)
        return picked

    quarters = (part, x_part, y_part, d_part)

    @pl.when(near)
    def _():
        @pl.when(inner)
        def _():
            own_w(True).start()
            own_g().start()

        @pl.when(jnp.logical_not(inner))
        def _():
            own_w(False).start()

    @pl.when(inner)
    def _():
        for j in range(per_half):
            own_e(j).start()

    wbuf[pl.ds(inner_set[0][0] // 2 * 2, 2), :, chip_cols(3 * core)] = jnp.zeros((2, held, chip_width), jnp.bfloat16)
    wbuf[inner_set[1][0], :, cut_cols(1 + core, core)] = jnp.zeros((held, cut), jnp.bfloat16)
    wbuf[outer_set[1][0], :, cut_cols(3 * core, core)] = jnp.zeros((held, cut), jnp.bfloat16)
    cbuf[pl.ds(pl.multiple_of(half * held, 16), spare)] = jnp.zeros((spare, cut), jnp.bfloat16)
    m_copy.wait()
    valid = m_ref[...].astype(jnp.float32)
    mine[...] = jnp.broadcast_to(jnp.sum(m_ref[...], axis=1, keepdims=True), mine.shape)
    pl.semaphore_wait(barrier, len(others) + 2)

    for v in range(2):
        @pl.when(jnp.logical_and(jnp.logical_not(inner), near == (v == 0)))
        def _():
            if v:
                near_c().start()
            else:
                own_w(False).wait()
                fold_core()
            for i in range(count):
                outer_w(i, v).start()
            outer_diag(v).start()

            def send(j, k):
                e_near(j, k).start()
                e_far(j, k).start()

            all_units(send)
            each_mask()

    @pl.when(jnp.logical_and(inner, near))
    def _():
        own_w(True).wait()
        fold_core()
        for i in range(count):
            far_w(i, 0).start()
        for j in range(per_half):
            near_e(j).start()
        own_g().wait()
        arrived(gbuf.at[other], g_recv.at[0])
        for i in range(count):
            for w in outer_set:
                got_mine(w, i)
            fold(part, *pieces[i])
            for w in outer_set:
                to_far(w, i)
                spread(w, i)
        all_units(lambda j, k: e_far(j, k).start())
        each_mask()
        block, cols = weights(half, True, 1)
        arrived(wbuf.at[block, :, cols], g_recv.at[2])
        have_own()
        for i in range(count):
            for v in range(2):
                if i < DIRECT:
                    got_sides(outer_set[v], i)
                else:
                    relay(outer_set[v], v, i)

        def turn(t):
            j = t // PARTS
            s = t % PARTS

            @pl.when(s == 0)
            def _():
                take_e(j)
                have_e(j)

            @pl.when(t == PARTS - 1)
            def _():
                for w in outer_set:
                    got_diag(w)
                fold(d_part, 0, direct)

            project(choose(s, quarters), j)

            @pl.when(s == PARTS - 1)
            def _():
                held_raw[j] = raw_scores(j, core, zt)

        loop(whole * PARTS, turn)
        take_e(whole, 0)
        have_e(whole, 0)

        def with_take(j, k, at):
            def run(s):
                @pl.when(s == at)
                def _():
                    take_e(whole + (k + 1) // CHUNKS, (k + 1) % CHUNKS)
                project_part(j, choose(s, quarters), k)

            loop(PARTS, run)

        with_take(whole, 0, 3)
        have_e(whole, 1)
        with_take(whole, 1, 2)
        held_raw[whole] = raw_scores(whole, core, zt)
        take_e(last, 1)
        for k in range(CHUNKS):
            have_e(last, k)
            loop(PARTS, lambda s: project_part(last, choose(s, quarters), k))
        score_last()
        loop(last, score_all)

    @pl.when(jnp.logical_and(inner, jnp.logical_not(near)))
    def _():
        near_c().start()
        near_g().start()
        for i in range(count):
            far_w(i, 1).start()
        near_w().start()
        for j in range(per_half):
            near_e(j).start()
        for pair in (inner_set, outer_set):
            for i in range(count):
                for w in pair:
                    got_mine(w, i)
                    spread(w, i)
        all_units(lambda j, k: e_far(j, k).start())
        each_mask()
        for i in range(count):
            for v in range(2):
                relay(inner_set[v], v, i)
        have_own()
        take_e(0)
        have_e(0)
        order = ((0, 0), (1, 0), (2, 0), (0, 1), (1, 1), (2, 1))

        def three_parts(j, k):
            loop(PARTS - 1, lambda s: project_part(j, choose(s, quarters), k))

        def turn(t):
            what = choose(t, [q * PARTS + j for q, j in order])

            @pl.when(t == 1)
            def _():
                for i in range(count):
                    if i == count - 1:
                        take_e(1)
                    for v in range(2):
                        relay(outer_set[v], v, i)

            @pl.when(t == 3)
            def _():
                have_e(1)

            @pl.when(t == 5)
            def _():
                take_e(whole, 0)

            project(choose(what // PARTS, quarters), what % PARTS)

        loop(len(order), turn)
        have_e(whole, 0)
        three_parts(whole, 0)
        take_e(whole, 1)
        for w in inner_set:
            got_diag(w)
        loop(whole, lambda j: project_pair(j, 2 * (1 - core)))
        have_e(whole, 1)
        three_parts(whole, 1)
        take_e(last, 0)
        have_e(last, 0)
        three_parts(last, 0)
        for w in outer_set:
            got_diag(w)
        take_e(last, 1)

        def diag_turn(j):
            project_pair(j, 2 * core)
            far_copy(j).start()

        loop(whole, diag_turn)
        for k in range(CHUNKS):
            project_part(whole, d_part, k)
        far_copy(whole).start()
        project_part(last, d_part, 0)
        have_e(last, 1)
        loop(PARTS, lambda s: project_part(last, choose(s, quarters), 1))
        score_last()

    arrived(mbuf.at[pl.ds(0, group - 1)], m_sems.at[1])
    mbuf[me] = mine[...]
    counts = mbuf[0]
    for g in range(1, group):
        counts = counts + mbuf[g]
    counts = counts[:, :1].astype(jnp.float32)
    slot = lax.broadcasted_iota(jnp.int32, (prompts, rows), 1).astype(jnp.float32)
    cols = (slot < counts).astype(jnp.float32)
    pairs = jnp.maximum(counts - 1.0, 1.0)
    same = lax.broadcasted_iota(jnp.int32, (block_rows, block_rows), 0)
    same = (same == lax.broadcasted_iota(jnp.int32, (block_rows, block_rows), 1)).astype(jnp.float32)
    down = lax.dot_general(same, valid, NT, preferred_element_type=jnp.float32)
    lane = lax.broadcasted_iota(jnp.int32, (block_rows, 128), 1)
    rates = jnp.zeros((block_rows, 128), jnp.float32)
    def settle(p, scores, rates):
        given = down[:, p:p + 1]
        prefs = jax.nn.sigmoid(scores) * given * cols[p:p + 1, :]
        o_ref[p] = prefs
        totals = jnp.sum(prefs, axis=1, keepdims=True) - 0.5 * given
        return jnp.where(lane == p, given * totals / pairs[p:p + 1, :], rates)

    for h in range(2):
        at_home = jnp.logical_and(inner, half == h)

        @pl.when(jnp.logical_not(jnp.logical_and(at_home, near)))
        def _():
            arrived(rbuf.at[pl.ds(h * last, last)], r_recv.at[h])
    for h in range(2):
        for j in range(last):
            rates = settle(h * per_half + j, rbuf[h * last + j].astype(jnp.float32), rates)
    for h in range(2):
        for c in range(CORES):
            at_home = jnp.logical_and(inner, half == h)

            @pl.when(jnp.logical_not(jnp.logical_and(at_home, core == c)))
            def _():
                arrived(lbuf.at[h, c], s_recv.at[h, c])
    for h in range(2):
        scores = lbuf[h, 0].astype(jnp.float32) + lbuf[h, 1].astype(jnp.float32)
        rates = settle(h * per_half + last, scores, rates)
    r_ref[...] = jnp.transpose(rates)[:prompts]

    departed(mbuf.at[pl.ds(0, group - 1)], m_sems.at[0])
    departed(ebuf.at[:, 0], e_send.at[1])
    for v in range(2):
        @pl.when(near == (v == 0))
        def _():
            @pl.when(inner)
            def _():
                block, cols = weights(half, True, v)
                departed(wbuf.at[block, pl.ds(0, quarter), cols], o_send.at[0])

            @pl.when(jnp.logical_not(inner))
            def _():
                block, cols = weights(half, False, v)
                departed(wbuf.at[block, pl.ds(0, quarter), cols], o_send.at[0])
                departed(wbuf.at[block, pl.ds(0, direct), cols], o_send.at[1])

    @pl.when(jnp.logical_not(near))
    def _():
        near_c().wait_send()

    @pl.when(jnp.logical_not(inner))
    def _():
        departed(ebuf.at[:, 0], e_send.at[0])

    @pl.when(inner)
    def _():
        departed(ebuf.at[:, 0], n_sems.at[0])
        departed(ebuf.at[:, pl.ds(0, 3)], h_send.at[0])

    @pl.when(jnp.logical_and(inner, near))
    def _():
        for w in outer_set:
            for sems in (x_send, y_send, u_send):
                sent_rows(w, sems, quarter)
            sent_rows(w, v_send, quarter - direct)
        departed(fbuf.at[:, pl.ds(0, rows - block_rows)], r_send.at[0])
        departed(tbuf.at[pl.ds(0, rows - block_rows)], r_send.at[1])

    @pl.when(jnp.logical_and(inner, jnp.logical_not(near)))
    def _():
        near_g().wait_send()
        near_w().wait_send()
        for w in inner_set + outer_set:
            for sems in (x_send, y_send, v_send):
                sent_rows(w, sems, quarter)
        departed(zt.at[pl.ds(0, last)], z_send.at[0])
        departed(tbuf.at[pl.ds(0, rows - block_rows)], r_send.at[1])


def line_scores(embeddings, head_weight, mask):
    prompts, block_rows, features = embeddings.shape
    held = head_weight.shape[0]
    group = CHIPS * CORES
    side = group // 2
    per_half = prompts // 2
    rows = group * block_rows
    units = per_half - 2 + 2 * CHUNKS
    chip_width = features // CHIPS
    cut = held // 128 * 128
    bf16, f32 = jnp.bfloat16, jnp.float32
    dma = pltpu.SemaphoreType.DMA
    held_in = pl.BlockSpec(memory_space=pltpu.HBM)
    vmem = pl.BlockSpec(memory_space=pltpu.VMEM)
    return pl.pallas_call(
        kernel,
        out_shape=(
            jax.ShapeDtypeStruct((prompts, block_rows, rows), f32),
            jax.ShapeDtypeStruct((prompts, block_rows), f32),
        ),
        in_specs=[held_in, held_in, held_in],
        out_specs=(vmem, vmem),
        scratch_shapes=[
            pltpu.VMEM((prompts, block_rows), jnp.int32),
            pltpu.VMEM((per_half, group, block_rows, features), bf16),
            pltpu.VMEM((side, held, features), bf16),
            pltpu.VMEM((CORES, held, chip_width), bf16),
            pltpu.VMEM((chip_width - cut, cut), bf16),
            pltpu.VMEM((per_half, side, held, rows), bf16),
            pltpu.VMEM((per_half - 1, side, held, rows), bf16),
            pltpu.VMEM((2, side, held, rows), f32),
            pltpu.VMEM((per_half - 1, rows, rows), f32),
            pltpu.VMEM((per_half - 1, rows, rows), bf16),
            pltpu.VMEM((rows, rows), bf16),
            pltpu.VMEM((prompts - 2, block_rows, rows), bf16),
            pltpu.VMEM((2, CORES, block_rows, rows), bf16),
            pltpu.VMEM((prompts, 128), jnp.int32),
            pltpu.VMEM((group, prompts, 128), jnp.int32),
            dma((3,)),
            dma((2,)),
            dma((units, CHIPS)),
            dma((units,)),
            dma((3,)),
            dma((1,)),
            dma((2,)),
            dma((2,)),
            dma((3,)),
            dma((3,)),
            dma((side,)),
            dma((side,)),
            dma((side,)),
            dma((side,)),
            dma((side, 4)),
            dma((side, 4)),
            dma((side,)),
            dma((1,)),
            dma((per_half - 1,)),
            dma((2,)),
            dma((2,)),
            dma((2, CORES)),
        ],
        compiler_params=pltpu.CompilerParams(
            collective_id=0, has_side_effects=True, vmem_limit_bytes=53 << 20
        ),
    )(embeddings, head_weight, pltpu.with_memory_space_constraint(mask, pltpu.HBM))


def shards(embeddings, head_weight, valid_mask):
    group_size = lax.axis_size("resp")
    slots = group_size * embeddings.shape[1]
    if (lax.axis_size("prompt"), group_size) == (PARTS, CHIPS * CORES):
        return line_scores(embeddings, head_weight, valid_mask)
    valid_rows = valid_mask.astype(jnp.float32)
    counts = lax.psum(jnp.sum(valid_rows, axis=1), "resp")
    scores = gathered_scores(embeddings, head_weight)
    column_ids = jnp.arange(slots, dtype=jnp.float32)
    valid_cols = (column_ids[None, :] < counts[:, None]).astype(jnp.float32)
    preferences = jax.nn.sigmoid(scores) * valid_rows[:, :, None] * valid_cols[:, None, :]
    totals = jnp.sum(preferences, axis=2) - 0.5 * valid_rows
    win_rates = valid_rows * totals / jnp.maximum(counts - 1.0, 1.0)[:, None]
    return (preferences, win_rates)


def solution(mesh):
    return jax.shard_map(
        shards,
        mesh=mesh,
        in_specs=(P("prompt", "resp", None), P("resp", None), P("prompt", "resp")),
        out_specs=(P("prompt", "resp", None), P("prompt", "resp")),
        check_vma=False,
    )
```

```python
import functools

import jax
import jax.numpy as jnp
from jax import lax
from jax.experimental import pallas as pl
from jax.experimental.pallas import tpu as pltpu
from jax.sharding import PartitionSpec as P

MESH = pl.DeviceIdType.MESH
CORES = 2
CHIPS = 4
PARTS = 4
CHUNKS = 2
DIRECT = 3
NT = (((1,), (1,)), ((), ()))


def gathered_halves(embeddings, head_weight, own_index, group_size):
    prompts, block_rows, features = embeddings.shape
    held = head_weight.shape[0]
    slots = group_size * block_rows
    everyone = lax.all_gather(embeddings, "resp", axis=0, tiled=True)
    flat = everyone.reshape(group_size * prompts * block_rows, features)
    through = lax.dot_general(flat, head_weight, NT, preferred_element_type=jnp.float32)
    through = through.astype(jnp.bfloat16).reshape(group_size, prompts, block_rows, held)
    mine = lax.dynamic_slice_in_dim(
        everyone.reshape(group_size, prompts, block_rows, features), own_index * held, held, 3
    )
    partial = jnp.einsum("gpid,hpjd->gpihj", mine, through, preferred_element_type=jnp.float32)
    flipped = jnp.einsum("gpid,hpjd->gpihj", through, mine, preferred_element_type=jnp.float32)
    partial = (partial - flipped).astype(jnp.bfloat16)
    return partial.reshape(group_size, prompts, block_rows, slots)


def gathered_scores(embeddings, head_weight):
    group_size = lax.axis_size("resp")
    own_index = lax.axis_index("resp")
    prompts, block_rows, features = embeddings.shape
    slots = group_size * block_rows
    at_once = max(1, min(prompts, (1 << 11) // slots))

    def scores_of(some):
        partial = gathered_halves(some, head_weight, own_index, group_size)
        swapped = lax.all_to_all(partial, "resp", split_axis=0, concat_axis=0, tiled=True)
        return jnp.sum(swapped.astype(jnp.float32), axis=0)

    pieces = embeddings.reshape(prompts // at_once, at_once, block_rows, features)
    return lax.map(scores_of, pieces).reshape(prompts, block_rows, slots)


def kernel(e_ref, w_ref, m_hbm, o_ref, r_ref,
           m_ref, ebuf, wbuf, gbuf, cbuf, zt, zfar, zsum, held_raw, fbuf, tbuf, rbuf, lbuf, mine, mbuf,
           m_sems, e_send, e_recv, h_recv, n_sems, h_send, o_send, l_sems, g_send, g_recv,
           w_send, a_recv, b_recv, d_recv, z_send, z_recv, r_send, r_recv, s_recv):
    part = lax.axis_index("prompt")
    me = lax.axis_index("resp")
    z = me // CORES
    core = me % CORES
    half = z // 2
    prompts, block_rows, features = e_ref.shape
    held = w_ref.shape[0]
    group = CHIPS * CORES
    per_half = prompts // 2
    side = group // 2
    span = held * side
    rows = group * block_rows
    quarter = held // PARTS
    z_in = 1 + half
    z_out = 3 * half
    z_far = 2 - half
    z_end = 3 - z_out
    inner = z == z_in
    near = core == half
    other = 1 - core
    here = me % side
    x_part = part + 1 - 2 * (part % 2)
    y_part = lax.rem(part + 2, PARTS)
    d_part = PARTS - 1 - part
    chip_width = features // CHIPS
    tiles = features // 256
    ends = [tiles * (CHUNKS - k) // CHUNKS * 256 for k in range(CHUNKS)]
    chunks = [(features - end, end - after) for end, after in zip(ends, ends[1:] + [0])]
    cut = held // 128 * 128
    spare = held - cut
    wide = chip_width - cut
    step = quarter // 7
    last = per_half - 1
    whole = per_half - 2
    pieces = ((0, step), (step, 2 * step), (3 * step, 2 * step), (5 * step, 2 * step))
    count = len(pieces)
    direct = pieces[DIRECT][0]

    def copy(src, dst, send, recv, chip, c, q=None):
        return pltpu.make_async_remote_copy(
            src, dst, send, recv,
            device_id=(part if q is None else q, chip * CORES + c), device_id_type=MESH,
        )

    def arrived(dst, recv):
        copy(dst, dst, m_sems.at[0], recv, z_far, core).wait_recv()

    def departed(src, send):
        copy(src, src, send, m_sems.at[1], z_far, core).wait_send()

    m_copy = pltpu.make_async_copy(m_hbm, m_ref, m_sems.at[2])
    m_copy.start()
    others = [lax.rem(me + d, group) for d in range(1, group)]
    barrier = pltpu.get_barrier_semaphore()
    for peer in others:
        pl.semaphore_signal(barrier, inc=1, device_id=(part, peer), device_id_type=MESH)
    for q in (x_part, y_part):
        pl.semaphore_signal(barrier, inc=1, device_id=(q, me), device_id_type=MESH)

    def mask_copy(d):
        return pltpu.make_async_remote_copy(
            mine, mbuf.at[me], m_sems.at[0], m_sems.at[1],
            device_id=(part, others[d]), device_id_type=MESH,
        )

    def chip_cols(chip):
        return pl.ds(pl.multiple_of(chip * chip_width, 128), chip_width)

    def cut_cols(chip, h):
        return pl.ds(pl.multiple_of(chip * chip_width + h * wide, 128), cut)

    def weights(h, within, v):
        size = features - (chip_width if within else 0) - (cut if v else 0)
        block = 2 * ((1 - h) if within else h) + ((1 - h) if v else h)
        return block, pl.ds(pl.multiple_of((1 - h) * (features - size), 128), size)

    outer_set = tuple(weights(core, False, v) for v in range(2))
    inner_set = tuple(weights(core, True, v) for v in range(2))
    first = 2 * half
    every = pl.ds(0, features)

    def span_rows(q, i):
        at, size = pieces[i]
        return pl.ds(pl.multiple_of(q * quarter + at, 16), size)

    def outer_w(i, v):
        block, cols = weights(half, False, v)
        at = span_rows(part, i)
        dst = wbuf.at[block, at, cols]
        return copy(w_ref.at[at, cols] if v else dst, dst, o_send.at[0], a_recv.at[block, i], z_in, half)

    def outer_diag(v):
        block, cols = weights(half, False, v)
        at = pl.ds(pl.multiple_of(d_part * quarter, 16), direct)
        dst = wbuf.at[block, at, cols]
        return copy(w_ref.at[at, cols] if v else dst, dst, o_send.at[1], d_recv.at[block], z_in, half)

    def far_w(i, v):
        block, cols = weights(half, True, v)
        at = span_rows(part, i)
        dst = wbuf.at[block, at, cols]
        return copy(w_ref.at[at, cols] if v else dst, dst, o_send.at[0], a_recv.at[block, i], z_far, half)

    def near_w():
        block, cols = weights(half, True, 1)
        return copy(w_ref.at[:, cols], wbuf.at[block, :, cols], g_send.at[0], g_recv.at[2], z_in, half)

    def near_g():
        return copy(w_ref.at[:, chip_cols(z_out)], gbuf.at[core], g_send.at[1], g_recv.at[0], z_in, half)

    def near_c():
        at = pl.ds(pl.multiple_of((1 - half) * spare, 16), held)
        return copy(w_ref.at[:, cut_cols(z, half)], cbuf.at[at], g_send.at[2], g_recv.at[1], z, half)

    def own_w(within):
        block, cols = weights(half, within, 0)
        return pltpu.make_async_copy(w_ref.at[:, cols], wbuf.at[block, :, cols], l_sems.at[0])

    def own_g():
        return pltpu.make_async_copy(w_ref.at[:, chip_cols(z_out)], gbuf.at[core], l_sems.at[1])

    def fold_core():
        arrived(cbuf.at[pl.ds(0, held)], g_recv.at[1])
        row = lax.broadcasted_iota(jnp.int32, (held, cut), 0)
        col = lax.broadcasted_iota(jnp.int32, (held, cut), 1)
        pick = (row - half * spare == col).astype(jnp.bfloat16)
        turned = lax.dot_general(pick, cbuf[...], NT, preferred_element_type=jnp.float32)
        cols = pl.ds(pl.multiple_of(z * chip_width + (1 - half) * cut, 128), wide)
        wbuf[here, :, cols] = (wbuf[here, :, cols].astype(jnp.float32) - turned).astype(jnp.bfloat16)

    def fold(q, at, size):
        start = q * quarter + at
        row = lax.broadcasted_iota(jnp.int32, (2 * size, chip_width), 0)
        col = lax.broadcasted_iota(jnp.int32, (2 * size, chip_width), 1)
        pick = (start + jnp.where(row < size, row, row + held - size) == col).astype(jnp.bfloat16)
        turned = lax.dot_general(
            pick, gbuf[...].reshape(chip_width, chip_width), NT, preferred_element_type=jnp.float32
        ).reshape(2, size, chip_width)
        pair, where, cols = pl.ds(first, 2), pl.ds(pl.multiple_of(start, 16), size), chip_cols(z_in)
        wbuf[pair, where, cols] = (wbuf[pair, where, cols].astype(jnp.float32) - turned).astype(jnp.bfloat16)

    def got_mine(w, i):
        block, cols = w
        arrived(wbuf.at[block, span_rows(part, i), cols], a_recv.at[block, i])

    def got_sides(w, i):
        block, cols = w
        arrived(wbuf.at[block, pl.ds(0, 2 * pieces[i][1]), cols], b_recv.at[block, i])

    def got_diag(w):
        block, cols = w
        arrived(wbuf.at[block, pl.ds(0, quarter), cols], d_recv.at[block])

    def along(w, q, i, send, recv, chip, q_to):
        block, cols = w
        spot = wbuf.at[block, span_rows(q, i), cols]
        return copy(spot, spot, send, recv, chip, core, q_to)

    def spread(w, i):
        along(w, part, i, w_send.at[w[0]], b_recv.at[w[0], i], z_in, x_part).start()
        along(w, part, i, w_send.at[w[0]], b_recv.at[w[0], i], z_in, y_part).start()

    def to_far(w, i):
        along(w, part, i, w_send.at[w[0]], a_recv.at[w[0], i], z_far, part).start()

    def relay(w, v, i):
        got_sides(w, i)
        if (i < 2) == (v == 0):
            along(w, x_part, i, w_send.at[w[0]], d_recv.at[w[0]], z_in, y_part).start()
        else:
            along(w, y_part, i, w_send.at[w[0]], d_recv.at[w[0]], z_in, x_part).start()

    def sent_rows(w, many):
        block, cols = w
        departed(wbuf.at[block, pl.ds(0, many), cols], w_send.at[block])

    def chunk_cols(k):
        return pl.ds(*chunks[k])

    def e_part(j, block, k):
        if k is None:
            return ebuf.at[j, block]
        return ebuf.at[j, block, :, chunk_cols(k)]

    def e_mine(h, j, k):
        if k is None:
            return e_ref.at[h * per_half + j]
        return e_ref.at[h * per_half + j, :, chunk_cols(k)]

    def unit(j, k):
        return j if k is None else whole + (j - whole) * CHUNKS + k

    def rank(chip, there):
        return jnp.where(chip > there, chip - 1, chip)

    def e_far(j, k=None):
        recv = e_recv.at[unit(j, k), rank(z, z_far)]
        return copy(e_mine(1 - half, j, k), e_part(j, me, k), e_send.at[1], recv, z_far, core)

    def e_near(j, k=None):
        return copy(e_mine(half, j, k), e_part(j, me, k), e_send.at[0], e_recv.at[unit(j, k), rank(z, z_in)], z_in, core)

    def near_e(j):
        return copy(e_mine(half, j, None), ebuf.at[j, me], n_sems.at[0], n_sems.at[1], z_in, other)

    def own_e(j):
        return pltpu.make_async_copy(e_mine(half, j, None), ebuf.at[j, me], n_sems.at[2])

    away = (z_out, z_far, z_end)

    def three(j, k):
        if k is None:
            return ebuf.at[j, pl.ds(0, 3)]
        return ebuf.at[j, pl.ds(0, 3), :, chunk_cols(k)]

    def take_e(j, k=None):
        for chip in away:
            spot = e_part(j, chip * CORES + core, k)
            arrived(spot, e_recv.at[unit(j, k), rank(chip, z_in)])
            copy(spot, spot, h_send.at[0], h_recv.at[unit(j, k)], z_in, other).start()

    def have_e(j, k=None):
        arrived(three(j, k), h_recv.at[unit(j, k)])

    def have_own():
        pltpu.make_async_copy(ebuf.at[:, me], ebuf.at[:, me], n_sems.at[2]).wait()
        arrived(ebuf.at[:, z_in * CORES + other], n_sems.at[1])

    def all_units(act):
        for j in range(whole):
            act(j, None)
        for j in range(whole, per_half):
            for k in range(CHUNKS):
                act(j, k)

    def far_copy(j):
        return copy(zt.at[j], zfar.at[j], z_send.at[0], z_recv.at[j], z_in, other)

    def project(q, j):
        at = pl.ds(pl.multiple_of(q * quarter, 16), quarter)
        left = wbuf[:, at].reshape(side * quarter, features)
        right = ebuf[j].reshape(rows, features)
        zt[j, :, at] = lax.dot_general(
            left, right, NT, preferred_element_type=jnp.float32
        ).astype(jnp.bfloat16).reshape(side, quarter, rows)

    def project_pair(j, base):
        at = pl.ds(pl.multiple_of(d_part * quarter, 16), quarter)
        blocks = pl.ds(base, 2)
        left = wbuf[blocks, at].reshape(2 * quarter, features)
        right = ebuf[j].reshape(rows, features)
        zt[j, blocks, at] = lax.dot_general(
            left, right, NT, preferred_element_type=jnp.float32
        ).astype(jnp.bfloat16).reshape(2, quarter, rows)

    def project_part(j, q, k):
        at = pl.ds(pl.multiple_of(q * quarter, 16), quarter)
        cols, width = chunk_cols(k), chunks[k][1]
        left = wbuf[:, at, cols].reshape(side * quarter, width)
        right = ebuf[j, :, :, cols].reshape(rows, width)
        total = lax.dot_general(
            left, right, NT, preferred_element_type=jnp.float32
        ).reshape(side, quarter, rows)
        if k > 0:
            total = zsum[j - whole, :, at] + total
        if k < CHUNKS - 1:
            zsum[j - whole, :, at] = total
        else:
            zt[j, :, at] = total.astype(jnp.bfloat16)

    def raw_scores(j, c, held_zt):
        lanes = pl.ds(pl.multiple_of(c * span, 128), span)
        left = ebuf[j, :, :, lanes].reshape(rows, span)
        return jnp.dot(left, held_zt[j].reshape(span, rows), preferred_element_type=jnp.float32)

    def block_at(t):
        return pl.ds(pl.multiple_of(t * block_rows, block_rows), block_rows)

    def final_copy(src, dst, send, recv, t):
        return pltpu.make_async_remote_copy(
            src, dst, send, recv, device_id=(part, t), device_id_type=MESH
        )

    def score_all(j):
        arrived(zfar.at[j], z_recv.at[j])
        raw = held_raw[j] + raw_scores(j, other, zfar)
        fbuf[j] = (raw - jnp.transpose(raw)).astype(jnp.bfloat16)
        for d in range(group - 1):
            spot = rbuf.at[half * last + j]
            final_copy(fbuf.at[j, block_at(others[d])], spot, r_send.at[0], r_recv.at[half], others[d]).start()
        rbuf[half * last + j] = fbuf[j, block_at(me)]

    def score_last():
        raw = raw_scores(last, core, zt)
        tbuf[...] = (raw - jnp.transpose(raw)).astype(jnp.bfloat16)
        for d in range(group - 1):
            spot = lbuf.at[half, core]
            final_copy(tbuf.at[block_at(others[d])], spot, r_send.at[1], s_recv.at[half, core], others[d]).start()
        lbuf[half, core] = tbuf[block_at(me)]

    def each_mask():
        for d in range(group - 1):
            mask_copy(d).start()

    def loop(n, body):
        def run(j, carry):
            body(j)
            return carry
        lax.fori_loop(0, n, run, 0)

    def choose(index, values):
        picked = values[0]
        for n in range(1, len(values)):
            picked = jnp.where(index == n, values[n], picked)
        return picked

    quarters = (part, x_part, y_part, d_part)

    @pl.when(near)
    def _():
        @pl.when(inner)
        def _():
            own_w(True).start()
            own_g().start()

        @pl.when(jnp.logical_not(inner))
        def _():
            own_w(False).start()

    @pl.when(inner)
    def _():
        for j in range(per_half):
            own_e(j).start()

    wbuf[pl.ds(inner_set[0][0] // 2 * 2, 2), :, chip_cols(3 * core)] = jnp.zeros((2, held, chip_width), jnp.bfloat16)
    wbuf[inner_set[1][0], :, cut_cols(1 + core, core)] = jnp.zeros((held, cut), jnp.bfloat16)
    wbuf[outer_set[1][0], :, cut_cols(3 * core, core)] = jnp.zeros((held, cut), jnp.bfloat16)
    cbuf[pl.ds(pl.multiple_of(half * held, 16), spare)] = jnp.zeros((spare, cut), jnp.bfloat16)
    m_copy.wait()
    valid = m_ref[...].astype(jnp.float32)
    mine[...] = jnp.broadcast_to(jnp.sum(m_ref[...], axis=1, keepdims=True), mine.shape)
    pl.semaphore_wait(barrier, len(others) + 2)

    for v in range(2):
        @pl.when(jnp.logical_and(jnp.logical_not(inner), near == (v == 0)))
        def _():
            if v:
                near_c().start()
            else:
                own_w(False).wait()
                fold_core()
            for i in range(count):
                outer_w(i, v).start()
            outer_diag(v).start()

            def send(j, k):
                e_near(j, k).start()
                e_far(j, k).start()

            all_units(send)
            each_mask()

    @pl.when(jnp.logical_and(inner, near))
    def _():
        own_w(True).wait()
        fold_core()
        for i in range(count):
            far_w(i, 0).start()
        for j in range(per_half):
            near_e(j).start()
        own_g().wait()
        arrived(gbuf.at[other], g_recv.at[0])
        for i in range(count):
            for w in outer_set:
                got_mine(w, i)
            fold(part, *pieces[i])
            for w in outer_set:
                to_far(w, i)
                spread(w, i)
        all_units(lambda j, k: e_far(j, k).start())
        each_mask()
        block, cols = weights(half, True, 1)
        arrived(wbuf.at[block, :, cols], g_recv.at[2])
        have_own()
        for i in range(count):
            for v in range(2):
                if i < DIRECT:
                    got_sides(outer_set[v], i)
                else:
                    relay(outer_set[v], v, i)

        def turn(t):
            j = t // PARTS
            s = t % PARTS

            @pl.when(s == 0)
            def _():
                take_e(j)
                have_e(j)

            @pl.when(t == PARTS - 1)
            def _():
                for w in outer_set:
                    got_diag(w)
                fold(d_part, 0, direct)

            project(choose(s, quarters), j)

            @pl.when(s == PARTS - 1)
            def _():
                held_raw[j] = raw_scores(j, core, zt)

        loop(whole * PARTS, turn)
        take_e(whole, 0)
        have_e(whole, 0)

        def with_take(j, k, at):
            def run(s):
                @pl.when(s == at)
                def _():
                    take_e(whole + (k + 1) // CHUNKS, (k + 1) % CHUNKS)
                project_part(j, choose(s, quarters), k)

            loop(PARTS, run)

        with_take(whole, 0, 3)
        have_e(whole, 1)
        with_take(whole, 1, 2)
        held_raw[whole] = raw_scores(whole, core, zt)
        take_e(last, 1)
        for k in range(CHUNKS):
            have_e(last, k)
            loop(PARTS, lambda s: project_part(last, choose(s, quarters), k))
        score_last()
        loop(last, score_all)

    @pl.when(jnp.logical_and(inner, jnp.logical_not(near)))
    def _():
        near_c().start()
        near_g().start()
        for i in range(count):
            far_w(i, 1).start()
        near_w().start()
        for j in range(per_half):
            near_e(j).start()
        for pair in (inner_set, outer_set):
            for i in range(count):
                for w in pair:
                    got_mine(w, i)
                    spread(w, i)
        all_units(lambda j, k: e_far(j, k).start())
        each_mask()
        for i in range(count):
            for v in range(2):
                relay(inner_set[v], v, i)
        have_own()
        take_e(0)
        have_e(0)
        order = ((0, 0), (1, 0), (2, 0), (0, 1), (1, 1), (2, 1))

        def three_parts(j, k):
            loop(PARTS - 1, lambda s: project_part(j, choose(s, quarters), k))

        def turn(t):
            what = choose(t, [q * PARTS + j for q, j in order])

            @pl.when(t == 1)
            def _():
                for i in range(count):
                    if i == count - 1:
                        take_e(1)
                    for v in range(2):
                        relay(outer_set[v], v, i)

            @pl.when(t == 3)
            def _():
                have_e(1)

            @pl.when(t == 5)
            def _():
                take_e(whole, 0)

            project(choose(what // PARTS, quarters), what % PARTS)

        loop(len(order), turn)
        have_e(whole, 0)
        three_parts(whole, 0)
        take_e(whole, 1)
        for w in inner_set:
            got_diag(w)
        loop(whole, lambda j: project_pair(j, 2 * (1 - core)))
        have_e(whole, 1)
        three_parts(whole, 1)
        take_e(last, 0)
        have_e(last, 0)
        three_parts(last, 0)
        for w in outer_set:
            got_diag(w)
        take_e(last, 1)

        def diag_turn(j):
            project_pair(j, 2 * core)
            far_copy(j).start()

        loop(whole, diag_turn)
        loop(2, lambda n: project_part(whole + n, d_part, 0))

        def final_turn(n):
            @pl.when(n == 1)
            def _():
                far_copy(whole).start()
                have_e(last, 1)
            project_part(jnp.where(n > 0, last, whole), choose(n, (d_part,) + quarters), 1)

        loop(1 + PARTS, final_turn)
        score_last()

    arrived(mbuf.at[pl.ds(0, group - 1)], m_sems.at[1])
    mbuf[me] = mine[...]
    counts = mbuf[0]
    for g in range(1, group):
        counts = counts + mbuf[g]
    counts = counts[:, :1].astype(jnp.float32)
    slot = lax.broadcasted_iota(jnp.int32, (prompts, rows), 1).astype(jnp.float32)
    cols = (slot < counts).astype(jnp.float32)
    pairs = jnp.maximum(counts - 1.0, 1.0)
    same = lax.broadcasted_iota(jnp.int32, (block_rows, block_rows), 0)
    same = (same == lax.broadcasted_iota(jnp.int32, (block_rows, block_rows), 1)).astype(jnp.float32)
    down = lax.dot_general(same, valid, NT, preferred_element_type=jnp.float32)
    lane = lax.broadcasted_iota(jnp.int32, (block_rows, 128), 1)
    rates = jnp.zeros((block_rows, 128), jnp.float32)
    def settle(p, scores, rates):
        given = down[:, p:p + 1]
        prefs = jax.nn.sigmoid(scores) * given * cols[p:p + 1, :]
        o_ref[p] = prefs
        totals = jnp.sum(prefs, axis=1, keepdims=True) - 0.5 * given
        return jnp.where(lane == p, given * totals / pairs[p:p + 1, :], rates)

    for h in range(2):
        at_home = jnp.logical_and(inner, half == h)

        @pl.when(jnp.logical_not(jnp.logical_and(at_home, near)))
        def _():
            arrived(rbuf.at[pl.ds(h * last, last)], r_recv.at[h])
    for h in range(2):
        for j in range(last):
            rates = settle(h * per_half + j, rbuf[h * last + j].astype(jnp.float32), rates)
    for h in range(2):
        for c in range(CORES):
            at_home = jnp.logical_and(inner, half == h)

            @pl.when(jnp.logical_not(jnp.logical_and(at_home, core == c)))
            def _():
                arrived(lbuf.at[h, c], s_recv.at[h, c])
    for h in range(2):
        scores = lbuf[h, 0].astype(jnp.float32) + lbuf[h, 1].astype(jnp.float32)
        rates = settle(h * per_half + last, scores, rates)
    r_ref[...] = jnp.transpose(rates)[:prompts]

    departed(mbuf.at[pl.ds(0, group - 1)], m_sems.at[0])
    departed(ebuf.at[:, 0], e_send.at[1])
    for v in range(2):
        @pl.when(near == (v == 0))
        def _():
            @pl.when(inner)
            def _():
                block, cols = weights(half, True, v)
                departed(wbuf.at[block, pl.ds(0, quarter), cols], o_send.at[0])

            @pl.when(jnp.logical_not(inner))
            def _():
                block, cols = weights(half, False, v)
                departed(wbuf.at[block, pl.ds(0, quarter), cols], o_send.at[0])
                departed(wbuf.at[block, pl.ds(0, direct), cols], o_send.at[1])

    @pl.when(jnp.logical_not(near))
    def _():
        near_c().wait_send()

    @pl.when(jnp.logical_not(inner))
    def _():
        departed(ebuf.at[:, 0], e_send.at[0])

    @pl.when(inner)
    def _():
        departed(ebuf.at[:, 0], n_sems.at[0])
        departed(ebuf.at[:, pl.ds(0, 3)], h_send.at[0])

    @pl.when(jnp.logical_and(inner, near))
    def _():
        for w in outer_set:
            sent_rows(w, 4 * quarter - direct)
        departed(fbuf.at[:, pl.ds(0, rows - block_rows)], r_send.at[0])
        departed(tbuf.at[pl.ds(0, rows - block_rows)], r_send.at[1])

    @pl.when(jnp.logical_and(inner, jnp.logical_not(near)))
    def _():
        near_g().wait_send()
        near_w().wait_send()
        for w in inner_set + outer_set:
            sent_rows(w, 3 * quarter)
        departed(zt.at[pl.ds(0, last)], z_send.at[0])
        departed(tbuf.at[pl.ds(0, rows - block_rows)], r_send.at[1])


def line_scores(embeddings, head_weight, mask):
    prompts, block_rows, features = embeddings.shape
    held = head_weight.shape[0]
    group = CHIPS * CORES
    side = group // 2
    per_half = prompts // 2
    rows = group * block_rows
    units = per_half - 2 + 2 * CHUNKS
    chip_width = features // CHIPS
    cut = held // 128 * 128
    bf16, f32 = jnp.bfloat16, jnp.float32
    dma = pltpu.SemaphoreType.DMA
    held_in = pl.BlockSpec(memory_space=pltpu.HBM)
    vmem = pl.BlockSpec(memory_space=pltpu.VMEM)
    return pl.pallas_call(
        kernel,
        out_shape=(
            jax.ShapeDtypeStruct((prompts, block_rows, rows), f32),
            jax.ShapeDtypeStruct((prompts, block_rows), f32),
        ),
        in_specs=[held_in, held_in, held_in],
        out_specs=(vmem, vmem),
        scratch_shapes=[
            pltpu.VMEM((prompts, block_rows), jnp.int32),
            pltpu.VMEM((per_half, group, block_rows, features), bf16),
            pltpu.VMEM((side, held, features), bf16),
            pltpu.VMEM((CORES, held, chip_width), bf16),
            pltpu.VMEM((chip_width - cut, cut), bf16),
            pltpu.VMEM((per_half, side, held, rows), bf16),
            pltpu.VMEM((per_half - 1, side, held, rows), bf16),
            pltpu.VMEM((2, side, held, rows), f32),
            pltpu.VMEM((per_half - 1, rows, rows), f32),
            pltpu.VMEM((per_half - 1, rows, rows), bf16),
            pltpu.VMEM((rows, rows), bf16),
            pltpu.VMEM((prompts - 2, block_rows, rows), bf16),
            pltpu.VMEM((2, CORES, block_rows, rows), bf16),
            pltpu.VMEM((prompts, 128), jnp.int32),
            pltpu.VMEM((group, prompts, 128), jnp.int32),
            dma((3,)),
            dma((2,)),
            dma((units, CHIPS - 1)),
            dma((units,)),
            dma((3,)),
            dma((1,)),
            dma((2,)),
            dma((2,)),
            dma((3,)),
            dma((3,)),
            dma((side,)),
            dma((side, 4)),
            dma((side, 4)),
            dma((side,)),
            dma((1,)),
            dma((per_half - 1,)),
            dma((2,)),
            dma((2,)),
            dma((2, CORES)),
        ],
        compiler_params=pltpu.CompilerParams(
            collective_id=0, has_side_effects=True, vmem_limit_bytes=53 << 20
        ),
    )(embeddings, head_weight, pltpu.with_memory_space_constraint(mask, pltpu.HBM))


def shards(embeddings, head_weight, valid_mask):
    group_size = lax.axis_size("resp")
    slots = group_size * embeddings.shape[1]
    if (lax.axis_size("prompt"), group_size) == (PARTS, CHIPS * CORES):
        return line_scores(embeddings, head_weight, valid_mask)
    valid_rows = valid_mask.astype(jnp.float32)
    counts = lax.psum(jnp.sum(valid_rows, axis=1), "resp")
    scores = gathered_scores(embeddings, head_weight)
    column_ids = jnp.arange(slots, dtype=jnp.float32)
    valid_cols = (column_ids[None, :] < counts[:, None]).astype(jnp.float32)
    preferences = jax.nn.sigmoid(scores) * valid_rows[:, :, None] * valid_cols[:, None, :]
    totals = jnp.sum(preferences, axis=2) - 0.5 * valid_rows
    win_rates = valid_rows * totals / jnp.maximum(counts - 1.0, 1.0)[:, None]
    return (preferences, win_rates)


def solution(mesh):
    return jax.shard_map(
        shards,
        mesh=mesh,
        in_specs=(P("prompt", "resp", None), P("resp", None), P("prompt", "resp")),
        out_specs=(P("prompt", "resp", None), P("prompt", "resp")),
        check_vma=False,
    )
```
